32 devices in a mesh: group: 2 (over x), patch: 16 (over z, y, core).
Axes of the slice: x: 2, y: 2, z: 4, core: 2. Of those that a mesh axis runs over, the one named last changes fastest.
Arguments:
- features: bfloat16 [32, 64, 4, 2304], P(('group', 'patch')), parts along dimension 0, may hold values from -6 to 6
- w_in: bfloat16 [28, 64], replicated, may hold values from -0.75 to 0.75
- w_plane: bfloat16 [9, 28, 28], replicated, may hold values from -0.375 to 0.375
- w_depth: bfloat16 [3, 28, 28], replicated, may hold values from -0.625 to 0.625
- w_head: bfloat16 [3, 28], replicated, may hold values from -1 to 1
- brick_owner: int32 [32], P(('group', 'patch')), parts along dimension 0, may hold values from 0 to 15, each once
- patch_anchor: int32 [32], P(('group', 'patch')), parts along dimension 0, may hold values from 0 to 3, as said below
- aug_code: int32 [32], P(('group', 'patch')), parts along dimension 0, may hold values from 0 to 7, as said below
Outputs:
- blended: float32 [32, 4, 2304], P(('group', 'patch')), parts along dimension 0
The draws below stay inside these ranges and needn't reach their ends.
There are 2 independent parts, one for each index of `group`. The reference program is written for one: setup_inputs(seed, part) draws one part's arguments, and reference() takes and returns one part's arrays. A program takes and returns all parts, laid end to end along the dimension named above; an argument that names none is the same for every part. Nothing has to cross between parts.
Inputs may be any that keep to these rules, and one draw needn't show every extreme that they name: `brick_owner`: every device owns exactly one brick of its region. `patch_anchor`: devices 8 k to 8 k + 7 share one anchor; different positions have different anchors. `aug_code`: devices 8 k to 8 k + 7 hold each code once.
All inputs are finite; a program needn't handle non-finite values.
Results may differ from the reference program's by a relative error of at most 0.00048.
Values sent between devices are 32-bit elements; how exact they have to be, the bound alone decides.
No kernel may reach another device: no remote copies, remote signals or barrier semaphores. Data moves between devices by JAX's collectives and lax.ppermute only.
A program may use at most 64 MiB of HBM per device.

```python
import math
import jax
import jax.numpy as jnp
from jax import lax

CIN = 64
CH = 28
PZ = 4
AUGS = 8
HALF = 48
POSITIONS = 2
NB_Y = 4
N_PATCH = 16


def draw_patch_anchor(key, part):
    row_order = jax.random.permutation(key, NB_Y)
    anchor_rows = row_order[:POSITIONS]
    return jnp.repeat(anchor_rows, AUGS).astype(jnp.int32)


def draw_aug_code(key, part):
    split_keys = jax.random.split(jax.random.fold_in(key, 7), POSITIONS)
    orderings = jax.vmap(lambda one_key: jax.random.permutation(one_key, AUGS))(split_keys)
    return orderings.reshape(-1).astype(jnp.int32)


def block_scale(own_key, extent, shards, low, top_value):
    def one(axis_at, parts):
        heights = jax.random.uniform(jax.random.fold_in(jax.random.fold_in(own_key, 6), axis_at), (parts,), jnp.float32, low / len(shards), top_value / len(shards))
        return jnp.repeat(jnp.exp(heights), extent[axis_at] // parts).reshape((-1,) + (1,) * (len(extent) - axis_at - 1))

    level = one(*shards[0])
    for cut in shards[1:]:
        level = level * one(*cut)
    return level


def scatter_about(rng, shape, width, bound, cuts=(), held_as=jnp.bfloat16):
    values = width * jax.random.normal(rng, shape, jnp.float32)
    if cuts:
        values = values * block_scale(rng, shape, cuts, -0.22, 0.18)
    return jnp.clip(values, -bound, bound).astype(held_as)


def setup_inputs(seed: int = 0, part: int = 0) -> dict:
    seeds = jax.random.split(jax.random.key(seed), 9)
    own_keys = jax.random.split(jax.random.fold_in(seeds[8], part), 9)
    features = scatter_about(own_keys[0], (N_PATCH, CIN, PZ, HALF * HALF), 1.0, 6.0, ((0, 16),))
    w_in = scatter_about(seeds[1], (CH, CIN), CIN ** -0.5, 0.75)
    w_plane = scatter_about(seeds[2], (9, CH, CH), (9 * CH) ** -0.5, 0.375)
    w_depth = scatter_about(seeds[3], (3, CH, CH), (3 * CH) ** -0.5, 0.625)
    w_head = scatter_about(seeds[4], (3, CH), CH ** -0.5, 1.0)
    brick_owner = jax.random.permutation(own_keys[5], N_PATCH).astype(jnp.int32)
    patch_anchor = draw_patch_anchor(jax.random.fold_in(jax.random.fold_in(seeds[8], part), 71), part)
    aug_code = draw_aug_code(jax.random.fold_in(jax.random.fold_in(seeds[8], part), 71), part)
    return {"features": features, "w_in": w_in, "w_plane": w_plane, "w_depth": w_depth, "w_head": w_head, "brick_owner": brick_owner, "patch_anchor": patch_anchor, "aug_code": aug_code}


def bump_curve(length):
    position = (jnp.arange(length, dtype=jnp.float32) + 0.5) / length
    return 0.1 + jnp.sin(jnp.pi * position) ** 2

def window_volume(patch_depth, plane_side):
    return bump_curve(patch_depth)[:, None, None] * bump_curve(plane_side)[None, :, None] * bump_curve(plane_side)[None, None, :]

def brick_partition(volume, brick_side):
    channels, patch_depth = (volume.shape[0], volume.shape[1])
    blocks = volume.reshape(channels, patch_depth, 4, brick_side, 4, brick_side).transpose(2, 4, 0, 1, 3, 5)
    return blocks.reshape(16, channels, patch_depth * brick_side * brick_side)

def mix_channels(weights, values):
    return jnp.einsum('oi,izyx->ozyx', weights.astype(jnp.float32), values.astype(jnp.float32), precision=lax.Precision.HIGHEST)

def patch_output(patch_feat, flip_code, w_in, w_plane, w_depth, w_head):
    channels, patch_depth, half_plane = patch_feat.shape
    half_side = math.isqrt(half_plane)
    plane_side = 2 * half_side
    brick_side = plane_side // 4
    hidden = w_in.shape[0]
    coarse = patch_feat.reshape(channels, patch_depth, half_side, half_side)
    projected = mix_channels(w_in, coarse).astype(jnp.bfloat16)
    upsampled = jnp.repeat(jnp.repeat(projected, 2, axis=2), 2, axis=3)
    padded = jnp.pad(upsampled, ((0, 0), (0, 0), (1, 1), (1, 1)))
    mix_total = jnp.zeros((hidden, patch_depth, plane_side, plane_side), jnp.float32)
    for row_tap in range(3):
        for col_tap in range(3):
            window_in = padded[:, :, row_tap:row_tap + plane_side, col_tap:col_tap + plane_side]
            mix_total = mix_total + mix_channels(w_plane[3 * row_tap + col_tap], window_in)
    first_out = (upsampled.astype(jnp.float32) + jax.nn.relu(mix_total)).astype(jnp.bfloat16)
    padded_depth = jnp.pad(first_out, ((0, 0), (1, 1), (0, 0), (0, 0)))
    mix_total = jnp.zeros((hidden, patch_depth, plane_side, plane_side), jnp.float32)
    for depth_tap in range(3):
        mix_total = mix_total + mix_channels(w_depth[depth_tap], padded_depth[:, depth_tap:depth_tap + patch_depth])
    second_out = (first_out.astype(jnp.float32) + jax.nn.relu(mix_total)).astype(jnp.bfloat16)
    affinity = jax.nn.sigmoid(mix_channels(w_head, second_out))
    affinity = jnp.where(flip_code % 2 == 1, affinity[:, ::-1], affinity)
    affinity = jnp.where(flip_code // 2 % 2 == 1, affinity[:, :, ::-1], affinity)
    affinity = jnp.where(flip_code // 4 % 2 == 1, affinity[:, :, :, ::-1], affinity)
    window = window_volume(patch_depth, plane_side)
    weighted = jnp.concatenate([affinity * window[None], window[None]], axis=0)
    return brick_partition(weighted, brick_side)

def reference(features, w_in, w_plane, w_depth, w_head, brick_owner, patch_anchor, aug_code):
    devices = features.shape[0]
    brick_rows = devices // 4
    cells = features.shape[2] * features.shape[3] // 4
    tile_index = jnp.arange(16, dtype=jnp.int32)

    def add_patch(running, patch_item):
        patch_feat, anchor_row, flip_code = patch_item
        volume_bricks = patch_output(patch_feat, flip_code, w_in, w_plane, w_depth, w_head)
        brick_id = ((anchor_row + tile_index // 4) % brick_rows * 4 + tile_index % 4).astype(jnp.int32)
        owners = brick_owner[brick_id]
        return (running.at[owners].add(volume_bricks), None)
    start = jnp.zeros((devices, 4, cells), jnp.float32)
    blended, _ = lax.scan(add_patch, start, (features, patch_anchor, aug_code))
    return blended
```

```python
import functools
import math

import numpy as np

import jax
import jax.numpy as jnp
from jax import lax
from jax.experimental import pallas as pl
from jax.experimental.pallas import tpu as pltpu
from jax.sharding import PartitionSpec as P

F32 = jnp.float32
BF16 = jnp.bfloat16
I32 = jnp.int32
PAD = 32
LANES = 128


def iota(shape, axis):
    return lax.broadcasted_iota(I32, shape, axis)


def vmem():
    return pl.BlockSpec(memory_space=pltpu.VMEM)


def smem():
    return pl.BlockSpec(memory_space=pltpu.SMEM)


def params():
    return pltpu.CompilerParams(vmem_limit_bytes=24 * 2**20)


def bump(length):
    position = (np.arange(length, dtype=np.float64) + 0.5) / length
    return 0.1 + np.sin(np.pi * position) ** 2


def weights_kernel(aug_ref, w_in_ref, w_plane_ref, w_depth_ref, w_head_ref, big_ref, plane_ref, depth_ref, head_ref, plane_scr, depth_scr):
    hidden, _ = w_in_ref.shape
    depth = depth_ref.shape[0] // PAD
    maps = w_head_ref.shape[0]
    aug = aug_ref[0]
    zf, yf, xf = aug & 1, (aug >> 1) & 1, (aug >> 2) & 1

    rows, cols = big_ref.shape
    spread = (iota((rows, hidden), 0) % PAD == iota((rows, hidden), 1)).astype(BF16)
    gather = (iota((w_in_ref.shape[1], cols), 1) // depth == iota((w_in_ref.shape[1], cols), 0)).astype(BF16)
    tall = jnp.dot(spread, w_in_ref[...], preferred_element_type=F32).astype(BF16)
    wide = jnp.dot(tall, gather, preferred_element_type=F32)
    same = iota((rows, cols), 1) % depth == iota((rows, cols), 0) // PAD
    big_ref[...] = jnp.where(same, wide, 0.0).astype(BF16)

    plane_scr[...] = jnp.zeros_like(plane_scr)
    taps = [w_plane_ref[t].astype(F32) for t in range(9)]
    near = (((0,), (1, 2), ()), ((), (0, 1), (2,)))
    for py in range(2):
        for px in range(2):
            for dy in range(2):
                for dx in range(3):
                    hit = [taps[3 * ty + tx] for ty in near[py][dy + py] for tx in near[px][dx]]
                    if not hit:
                        continue
                    total = functools.reduce(lambda a, b: a + b, hit)
                    high = total.astype(BF16).astype(F32)
                    col = (3 * dy + dx) * PAD
                    plane_scr[py, pl.ds(px * PAD, hidden), pl.ds(col, hidden)] = high
                    plane_scr[py, pl.ds((2 + px) * PAD, hidden), pl.ds(col, hidden)] = total - high
    plane_ref[...] = plane_scr[...].astype(BF16)

    depth_scr[...] = jnp.zeros_like(depth_scr)
    for t in range(3):
        tap = w_depth_ref[t].astype(F32)
        for z in range(depth):
            if 0 <= z + t - 1 < depth:
                depth_scr[pl.ds(z * PAD, hidden), pl.ds((z + t - 1) * PAD, hidden)] = tap
    depth_ref[...] = depth_scr[...].astype(BF16)

    rows, cols = head_ref.shape
    pick = (iota((rows, maps), 0) % maps == iota((rows, maps), 1)).astype(BF16)
    tall = jnp.dot(pick, w_head_ref[...], preferred_element_type=F32).astype(BF16)
    gather = (iota((hidden, cols), 1) % PAD == iota((hidden, cols), 0)).astype(BF16)
    wide = jnp.dot(tall, gather, preferred_element_type=F32)
    at = iota((rows, cols), 0) // maps
    came = iota((rows, cols), 1) // PAD
    flip = (2 * yf + xf) * depth + (depth - 1) * zf
    head_ref[...] = jnp.where(at == (came ^ flip), wide, 0.0).astype(BF16)


def pack_weights(aug_code, w_in, w_plane, w_depth, w_head, depth):
    hidden, channels = w_in.shape
    maps = w_head.shape[0]
    shapes = (
        (depth * PAD, channels * depth),
        (2, 4 * PAD, 6 * PAD),
        (depth * PAD, depth * PAD),
        (4 * depth * maps, 4 * depth * PAD),
    )
    return pl.pallas_call(
        weights_kernel,
        out_shape=[jax.ShapeDtypeStruct(s, BF16) for s in shapes],
        in_specs=[smem()] + [vmem()] * 4,
        out_specs=[vmem()] * 4,
        scratch_shapes=[pltpu.VMEM(shapes[1], F32), pltpu.VMEM(shapes[2], F32)],
        compiler_params=params(),
        name="weights",
    )(aug_code, w_in, w_plane, w_depth, w_head)


def patch_kernel(half, aug_ref, x_ref, big_ref, plane_ref, depth_ref, head_ref, out_ref, xs_ref, a_ref):
    channels, depth, cells = x_ref.shape
    rows = depth * PAD
    step = 2 * LANES
    margin = LANES
    aug = aug_ref[0]
    yf, xf = (aug >> 1) & 1, (aug >> 2) & 1

    x = x_ref[...].reshape(channels * depth, cells)
    projected = jnp.dot(big_ref[...], x, preferred_element_type=F32).astype(BF16)
    zeros = jnp.zeros((rows, margin), BF16)
    padded = jnp.concatenate([zeros, projected, zeros], axis=1)
    column = iota((rows, cells), 1) % half
    for d in range(3):
        shifted = projected if d == 1 else lax.slice_in_dim(padded, margin + d - 1, margin + d - 1 + cells, axis=1)
        if d == 0:
            shifted = jnp.where(column == 0, jnp.zeros_like(shifted), shifted)
        if d == 2:
            shifted = jnp.where(column == half - 1, jnp.zeros_like(shifted), shifted)
        xs_ref[d, :, pl.ds(0, margin)] = zeros
        xs_ref[d, :, pl.ds(margin, cells)] = shifted
        xs_ref[d, :, pl.ds(margin + cells, margin)] = zeros

    for t in range(cells // step):
        near = []
        for d in range(3):
            block = xs_ref[d, :, pl.ds(t * step, step + 2 * margin)]
            near.append([lax.slice_in_dim(block, margin + half * e, margin + half * e + step, axis=1) for e in (-1, 0, 1)])
        centre = near[1][1].astype(F32)
        first = [[None] * depth for _ in range(4)]
        for z in range(depth):
            cut = slice(z * PAD, (z + 1) * PAD)
            for py in range(2):
                around = jnp.concatenate([near[d][py + e][cut] for e in range(2) for d in range(3)], axis=0)
                mix = jnp.dot(plane_ref[py], around, preferred_element_type=F32)
                for px in range(2):
                    total = mix[px * PAD : (px + 1) * PAD] + mix[(2 + px) * PAD : (3 + px) * PAD]
                    first[2 * py + px][z] = (centre[cut] + jnp.maximum(total, 0.0)).astype(BF16)
        second = []
        for p in range(4):
            one = jnp.concatenate(first[p], axis=0)
            mix = jnp.dot(depth_ref[...], one, preferred_element_type=F32)
            second.append((one.astype(F32) + jnp.maximum(mix, 0.0)).astype(BF16))
        logits = jnp.zeros((head_ref.shape[0], step), F32)
        for q in range(2):
            pair = jnp.concatenate(second[2 * q : 2 * q + 2], axis=0)
            logits = logits + jnp.dot(head_ref[:, 2 * q * rows : 2 * (q + 1) * rows], pair, preferred_element_type=F32)
        affinity = jax.nn.sigmoid(logits)
        for u in range(step // LANES):
            a_ref[t * (step // LANES) + u] = affinity[:, u * LANES : (u + 1) * LANES]

    side = half // 4
    main, tail = LANES, side * side - LANES
    tiles = head_ref.shape[0] // 8
    lane = iota((8, LANES), 1)

    def source(cell, j, odd):
        yl = cell // side
        xl = cell - yl * side
        y = jnp.where(yf == 1, side - 1 - yl, yl)
        xx = side * j + xl
        xx = jnp.where(xf == 1, half - 1 - xx, xx)
        return y * half + xx + odd * (LANES // 2)

    span = -(-side * half // LANES)
    rest_base = jnp.where(yf == 1, 0, span - 2)
    group = lane // tail
    for odd in range(2):
        for j in range(4):
            src = source(lane, j, odd)
            tile_of, lane_of = src // LANES, src % LANES
            hits = [tile_of == k for k in range(span)]
            rest = source(LANES + lane % tail, j, odd)
            rest_hit = rest // LANES == rest_base
            rest_lane = rest % LANES
            for i in range(odd, 4, 2):
                base = side * half * i // LANES
                brick = (i ^ (3 * yf)) * 4 + j
                packed = jnp.zeros((8, LANES), F32)
                for r in range(tiles):
                    cut = pl.ds(8 * r, 8)
                    value = jnp.take_along_axis(a_ref[base, cut], lane_of, axis=1)
                    for k in range(1, span):
                        value = jnp.where(hits[k], jnp.take_along_axis(a_ref[base + k, cut], lane_of, axis=1), value)
                    out_ref[brick, cut] = value
                    low = jnp.take_along_axis(a_ref[base + rest_base, cut], rest_lane, axis=1)
                    high = jnp.take_along_axis(a_ref[base + rest_base + 1, cut], rest_lane, axis=1)
                    packed = jnp.where(group == r, jnp.where(rest_hit, low, high), packed)
                out_ref[brick, pl.ds(8 * tiles, 8)] = packed


def patch_bricks(aug_code, feat, packed):
    channels, depth, cells = feat.shape
    half = math.isqrt(cells)
    big, plane, depth_w, head = packed
    kept = head.shape[0]
    return pl.pallas_call(
        functools.partial(patch_kernel, half),
        out_shape=jax.ShapeDtypeStruct((16, kept + 8, LANES), F32),
        in_specs=[smem()] + [vmem()] * 5,
        out_specs=vmem(),
        scratch_shapes=[
            pltpu.VMEM((3, depth * PAD, cells + 2 * LANES), BF16),
            pltpu.VMEM((cells // LANES, kept, LANES), F32),
        ],
        compiler_params=params(),
        cost_estimate=pl.CostEstimate(flops=2 * 10**9, bytes_accessed=2 * 10**6, transcendentals=0),
        name="patch",
    )(aug_code, feat, big, plane, depth_w, head)


def seed_kernel(owner_ref, anchor_ref, out_ref):
    me = lax.axis_index("patch")
    kind = iota(out_ref.shape, 0)
    here = iota(out_ref.shape, 1) == me
    value = jnp.where(kind == 0, owner_ref[0], anchor_ref[0])
    out_ref[...] = jnp.where(here, value, 0)


def seed_table(owner, anchor, devices):
    width = -(-devices // LANES) * LANES
    return pl.pallas_call(
        seed_kernel,
        out_shape=jax.ShapeDtypeStruct((2, width), I32),
        in_specs=[smem(), smem()],
        out_specs=vmem(),
        compiler_params=params(),
        name="seed",
    )(owner, anchor)


def partner(devices, bit):
    return [(d, d ^ bit) for d in range(devices)]


def slots_kernel(devices, bits, table_ref, mine_ref, other_ref, window_ref, send_ref, keep_ref, place_ref):
    me = lax.axis_index("patch")
    brick_rows = devices // 4

    def note(b, _):
        place_ref[table_ref[0, b]] = b
        return 0

    lax.fori_loop(0, devices, note, 0)
    anchor = table_ref[1, me]
    count = 1 << len(bits)
    for s in range(count):
        mask = sum(bit for k, bit in enumerate(bits) if s >> (len(bits) - 1 - k) & 1)
        brick = place_ref[me ^ mask]
        row = lax.rem(brick // 4 - anchor + brick_rows, brick_rows)
        at = row * 4 + brick % 4
        if brick_rows > 4:
            at = jnp.where(row < 4, at, 0)
        value = (mine_ref[at] + other_ref[at]) * window_ref[at]
        if brick_rows > 4:
            value = jnp.where(row < 4, value, 0.0)
        if s < count // 2:
            keep_ref[s] = value
        else:
            send_ref[s - count // 2] = value


def fill_slots(devices, bits, table, mine, other, window):
    shape = jax.ShapeDtypeStruct((1 << (len(bits) - 1),) + mine.shape[1:], F32)
    return pl.pallas_call(
        functools.partial(slots_kernel, devices, bits),
        out_shape=[shape, shape],
        in_specs=[smem()] + [vmem()] * 3,
        out_specs=[vmem()] * 2,
        scratch_shapes=[pltpu.SMEM((devices,), I32)],
        compiler_params=params(),
        name="slots",
    )(table, mine, other, window)


def brick_kernel(devices, side, maps, depth_curve, table_ref, mine_ref, other_ref, rows_ref, cols_ref, out_ref):
    depth = len(depth_curve)
    wide = 2 * side
    plane = wide * wide
    tail = side * side - LANES
    per = depth * maps
    brick = mine_ref[0] + other_ref[0]
    kept = 4 * per
    main, packed = brick[:kept], brick[kept:]
    rest = jnp.concatenate([packed if k == 0 else pltpu.roll(packed, LANES - tail * k, 1) for k in range(kept // 8)], axis=0)
    fill = jnp.zeros((16 - per, LANES), F32)
    mains = [jnp.concatenate([main[per * p : per * (p + 1)], fill], axis=0) for p in range(4)]
    rests = [jnp.concatenate([rest[per * p : per * (p + 1)], fill], axis=0) for p in range(4)]
    columns = []
    for d in range(-(-plane // LANES)):
        n = iota((8, LANES), 1) + d * LANES
        y = n // wide
        x = n - y * wide
        cell = (y // 2) * side + x // 2
        quarter = 2 * (y % 2) + x % 2
        lane_of = cell % LANES
        top = min((d + 1) * LANES, plane) - 1
        tiles = []
        for r in range(2):
            cut = slice(8 * r, 8 * r + 8)
            value = None
            for p in range(4):
                one = jnp.take_along_axis(mains[p][cut], lane_of, axis=1)
                if (top // wide // 2 + 1) * side > LANES:
                    one = jnp.where(cell >= LANES, jnp.take_along_axis(rests[p][cut], lane_of, axis=1), one)
                value = one if value is None else jnp.where(quarter == p, one, value)
            tiles.append(value)
        columns.append(jnp.concatenate(tiles, axis=0))
    cells = jnp.concatenate(columns, axis=1)[:, :plane]
    for z in range(depth):
        out_ref[0, pl.ds(0, maps), pl.ds(z * plane, plane)] = cells[z * maps : (z + 1) * maps]

    me = lax.axis_index("patch")
    brick_rows = devices // 4
    owned = lax.fori_loop(0, devices, lambda b, at: jnp.where(table_ref[0, b] == me, b, at), 0)
    row, col = owned // 4, owned % 4

    def tally(d, counts):
        i = lax.rem(row - table_ref[1, d] + brick_rows, brick_rows)
        return tuple(c + jnp.where(i == k, 1, 0) for k, c in enumerate(counts))

    counts = lax.fori_loop(0, devices, tally, (0, 0, 0, 0))
    rows = sum(c.astype(F32) * rows_ref[pl.ds(k, 1), :] for k, c in enumerate(counts))
    window = (rows * cols_ref[pl.ds(col, 1), :])[:, :plane]
    for z in range(depth):
        out_ref[0, pl.ds(maps, 1), pl.ds(z * plane, plane)] = window * depth_curve[z]


def finish(devices, side, maps, depth, table, mine, other):
    plane = 4 * side * side
    width = -(-plane // LANES) * LANES
    curve = bump(8 * side)
    n = np.arange(width)
    y, x = np.minimum(n // (2 * side), 2 * side - 1), n % (2 * side)
    rows = np.stack([curve[2 * side * i + y] for i in range(4)]).astype(np.float32)
    cols = np.stack([curve[2 * side * i + x] for i in range(4)]).astype(np.float32)
    depth_curve = [float(np.float32(v)) for v in bump(depth)]
    return pl.pallas_call(
        functools.partial(brick_kernel, devices, side, maps, depth_curve),
        out_shape=jax.ShapeDtypeStruct((1, maps + 1, depth * plane), F32),
        in_specs=[smem()] + [vmem()] * 4,
        out_specs=vmem(),
        compiler_params=params(),
        name="brick",
    )(table, mine, other, rows, cols)


def wire_window(side, maps, depth):
    curve_y, curve_z = bump(8 * side), bump(depth)
    cell = np.arange(side * side)
    out = np.zeros((16, 4 * depth * maps, side * side))
    for i in range(4):
        for j in range(4):
            for p in range(4):
                y = curve_y[2 * side * i + 2 * (cell // side) + p // 2]
                x = curve_y[2 * side * j + 2 * (cell % side) + p % 2]
                for z in range(depth):
                    for m in range(maps):
                        out[4 * i + j, (p * depth + z) * maps + m] = curve_z[z] * y * x
    kept = out.shape[1]
    tail = side * side - LANES
    packed = np.zeros((16, 8, LANES))
    for k in range(kept // 8):
        packed[:, :, tail * k : tail * (k + 1)] = out[:, 8 * k : 8 * k + 8, LANES:]
    return np.concatenate([out[:, :, :LANES], packed], axis=1).astype(np.float32)


def on_device(features, w_in, w_plane, w_depth, w_head, brick_owner, patch_anchor, aug_code):
    devices = lax.axis_size("patch")
    _, _, depth, cells = features.shape
    side = math.isqrt(cells) // 4
    maps = w_head.shape[0]
    bits = [1 << k for k in range(devices.bit_length() - 1)]

    table = seed_table(brick_owner, patch_anchor, devices)
    for bit in bits:
        table = table + lax.ppermute(table, "patch", partner(devices, bit))
    packed = pack_weights(aug_code, w_in, w_plane, w_depth, w_head, depth)
    bricks = patch_bricks(aug_code, features[0], packed)
    other = lax.ppermute(bricks, "patch", partner(devices, 1))
    send, keep = fill_slots(devices, bits[1:], table, bricks, other, wire_window(side, maps, depth))
    for bit in bits[1:-1]:
        got = lax.ppermute(send, "patch", partner(devices, bit))
        half = send.shape[0] // 2
        keep, send = keep[:half] + got[:half], keep[half:] + got[half:]
    other = lax.ppermute(send, "patch", partner(devices, bits[-1]))
    return finish(devices, side, maps, depth, table, keep, other)


def solution(mesh):
    one = P(("group", "patch"))
    in_specs = (P(("group", "patch"), None, None, None), P(), P(), P(), P(), one, one, one)
    return jax.shard_map(
        on_device, mesh=mesh, in_specs=in_specs, out_specs=P(("group", "patch"), None, None), check_vma=False
    )
```

```python
import functools
import math

import numpy as np

import jax
import jax.numpy as jnp
from jax import lax
from jax.experimental import pallas as pl
from jax.experimental.pallas import tpu as pltpu
from jax.sharding import PartitionSpec as P


F32 = jnp.float32
BF16 = jnp.bfloat16
I32 = jnp.int32
PAD = 32
LANES = 128
SPARE = 96


def iota(shape, axis):
    return lax.broadcasted_iota(I32, shape, axis)


def vmem():
    return pl.BlockSpec(memory_space=pltpu.VMEM)


def smem():
    return pl.BlockSpec(memory_space=pltpu.SMEM)


def hbm():
    return pl.BlockSpec(memory_space=pltpu.HBM)


def stay(*arrays):
    return [pltpu.with_memory_space_constraint(a, pltpu.HBM) for a in arrays]


def params():
    return pltpu.CompilerParams(vmem_limit_bytes=16 * 2**20)


def cost(flops):
    return pl.CostEstimate(flops=flops, bytes_accessed=2**20, transcendentals=0)


def bump(length):
    position = (np.arange(length, dtype=np.float64) + 0.5) / length
    return 0.1 + np.sin(np.pi * position) ** 2


def front_kernel(half, aug_ref, w_in_hbm, w_plane_hbm, w_depth_hbm, w_head_hbm, x_hbm, plane_ref, depth_ref, head_ref, xs_ref, w_in_ref, w_plane_ref, w_depth_ref, w_head_ref, x_ref, big_ref, plane_scr, depth_scr, sems):
    pairs = ((w_plane_hbm, w_plane_ref), (w_in_hbm, w_in_ref), (w_depth_hbm, w_depth_ref), (w_head_hbm, w_head_ref), (x_hbm, x_ref))
    copies = [pltpu.make_async_copy(src, dst, sems.at[k]) for k, (src, dst) in enumerate(pairs)]
    for copy in copies:
        copy.start()
    for copy in copies[:-1]:
        copy.wait()
    hidden, _ = w_in_ref.shape
    depth = depth_ref.shape[0] // PAD
    maps = w_head_ref.shape[0]
    aug = aug_ref[0]
    zf, yf, xf = aug & 1, (aug >> 1) & 1, (aug >> 2) & 1

    rows, cols = big_ref.shape
    spread = (iota((rows, hidden), 0) % PAD == iota((rows, hidden), 1)).astype(BF16)
    gather = (iota((w_in_ref.shape[1], cols), 1) // depth == iota((w_in_ref.shape[1], cols), 0)).astype(BF16)
    tall = jnp.dot(spread, w_in_ref[...], preferred_element_type=F32).astype(BF16)
    wide = jnp.dot(tall, gather, preferred_element_type=F32)
    same = iota((rows, cols), 1) % depth == iota((rows, cols), 0) // PAD
    big_ref[...] = jnp.where(same, wide, 0.0).astype(BF16)

    plane_scr[...] = jnp.zeros_like(plane_scr)
    taps = [w_plane_ref[t].astype(F32) for t in range(9)]
    near = (((0,), (1, 2), ()), ((), (0, 1), (2,)))
    for py in range(2):
        for px in range(2):
            for dy in range(2):
                for dx in range(3):
                    hit = [taps[3 * ty + tx] for ty in near[py][dy + py] for tx in near[px][dx]]
                    if not hit:
                        continue
                    total = functools.reduce(lambda a, b: a + b, hit)
                    high = total.astype(BF16).astype(F32)
                    col = (3 * dy + dx) * PAD
                    plane_scr[py, pl.ds(px * PAD, hidden), pl.ds(col, hidden)] = high
                    plane_scr[py, pl.ds((2 + px) * PAD, hidden), pl.ds(col, hidden)] = total - high
    plane_ref[...] = plane_scr[...].astype(BF16)

    depth_scr[...] = jnp.zeros_like(depth_scr)
    for t in range(3):
        tap = w_depth_ref[t].astype(F32)
        for z in range(depth):
            if 0 <= z + t - 1 < depth:
                depth_scr[pl.ds(z * PAD, hidden), pl.ds((z + t - 1) * PAD, hidden)] = tap
    depth_ref[...] = depth_scr[...].astype(BF16)

    rows, cols = head_ref.shape
    pick = (iota((rows, maps), 0) % maps == iota((rows, maps), 1)).astype(BF16)
    tall = jnp.dot(pick, w_head_ref[...], preferred_element_type=F32).astype(BF16)
    gather = (iota((hidden, cols), 1) % PAD == iota((hidden, cols), 0)).astype(BF16)
    wide = jnp.dot(tall, gather, preferred_element_type=F32)
    at = iota((rows, cols), 0) // maps
    came = iota((rows, cols), 1) // PAD
    flip = (2 * yf + xf) * depth + (depth - 1) * zf
    head_ref[...] = jnp.where(at == (came ^ flip), wide, 0.0).astype(BF16)

    copies[-1].wait()
    channels, depth, cells = x_ref.shape
    rows = depth * PAD
    margin = LANES
    x = x_ref[...].reshape(channels * depth, cells)
    projected = jnp.dot(big_ref[...], x, preferred_element_type=F32).astype(BF16)
    zeros = jnp.zeros((rows, margin), BF16)
    padded = jnp.concatenate([zeros, projected, zeros], axis=1)
    column = iota((rows, cells), 1) % half
    for d in range(3):
        shifted = projected if d == 1 else lax.slice_in_dim(padded, margin + d - 1, margin + d - 1 + cells, axis=1)
        if d == 0:
            shifted = jnp.where(column == 0, jnp.zeros_like(shifted), shifted)
        if d == 2:
            shifted = jnp.where(column == half - 1, jnp.zeros_like(shifted), shifted)
        xs_ref[d, :, pl.ds(0, margin)] = zeros
        xs_ref[d, :, pl.ds(margin, cells)] = shifted
        xs_ref[d, :, pl.ds(margin + cells, margin)] = zeros


def front(aug_code, w_in, w_plane, w_depth, w_head, feat):
    _, channels = w_in.shape
    maps = w_head.shape[0]
    _, depth, cells = feat.shape
    plane = (2, 4 * PAD, 6 * PAD)
    depth_w = (depth * PAD, depth * PAD)
    head = (4 * depth * maps, 4 * depth * PAD)
    shifted = (3, depth * PAD, cells + 2 * LANES)
    return pl.pallas_call(
        functools.partial(front_kernel, math.isqrt(cells)),
        out_shape=[jax.ShapeDtypeStruct(s, BF16) for s in (plane, depth_w, head, shifted)],
        in_specs=[smem()] + [hbm()] * 5,
        out_specs=[vmem()] * 4,
        scratch_shapes=[
            pltpu.VMEM(w_in.shape, BF16),
            pltpu.VMEM(w_plane.shape, BF16),
            pltpu.VMEM(w_depth.shape, BF16),
            pltpu.VMEM(w_head.shape, BF16),
            pltpu.VMEM(feat.shape, BF16),
            pltpu.VMEM((depth * PAD, channels * depth), BF16),
            pltpu.VMEM(plane, F32),
            pltpu.VMEM(depth_w, F32),
            pltpu.SemaphoreType.DMA((5,)),
        ],
        compiler_params=params(),
        cost_estimate=cost(10**8),
        name="front",
    )(aug_code, *stay(w_in, w_plane, w_depth, w_head, feat))


def patch_kernel(half, tiles, brick_rows, last, aug_ref, xs_ref, plane_ref, depth_ref, head_ref, *refs):
    if last:
        carry_in, _, out_ref, a_ref = refs
    else:
        out_ref, carry_out, a_ref = refs
    _, rows, _ = xs_ref.shape
    depth = rows // PAD
    step = 2 * LANES
    margin = LANES
    first_tile = tiles[0] * (step // LANES) - (1 if last else 0)
    if last:
        a_ref[0] = carry_in[...]

    for t in tiles:
        near = []
        for d in range(3):
            block = xs_ref[d, :, pl.ds(t * step, step + 2 * margin)]
            near.append([lax.slice_in_dim(block, margin + half * e, margin + half * e + step, axis=1) for e in (-1, 0, 1)])
        centre = near[1][1].astype(F32)
        first = [[None] * depth for _ in range(4)]
        for z in range(depth):
            cut = slice(z * PAD, (z + 1) * PAD)
            for py in range(2):
                around = jnp.concatenate([near[d][py + e][cut] for e in range(2) for d in range(3)], axis=0)
                mix = jnp.dot(plane_ref[py], around, preferred_element_type=F32)
                for px in range(2):
                    total = mix[px * PAD : (px + 1) * PAD] + mix[(2 + px) * PAD : (3 + px) * PAD]
                    first[2 * py + px][z] = (centre[cut] + jnp.maximum(total, 0.0)).astype(BF16)
        second = []
        for p in range(4):
            one = jnp.concatenate(first[p], axis=0)
            mix = jnp.dot(depth_ref[...], one, preferred_element_type=F32)
            second.append((one.astype(F32) + jnp.maximum(mix, 0.0)).astype(BF16))
        logits = jnp.zeros((head_ref.shape[0], step), F32)
        for q in range(2):
            pair = jnp.concatenate(second[2 * q : 2 * q + 2], axis=0)
            logits = logits + jnp.dot(head_ref[:, 2 * q * rows : 2 * (q + 1) * rows], pair, preferred_element_type=F32)
        affinity = jax.nn.sigmoid(logits)
        for u in range(step // LANES):
            a_ref[t * (step // LANES) + u - first_tile] = affinity[:, u * LANES : (u + 1) * LANES]

    if not last:
        carry_out[...] = a_ref[(tiles[-1] + 1) * (step // LANES) - 1 - first_tile]

    aug = aug_ref[0]
    yf, xf = (aug >> 1) & 1, (aug >> 2) & 1

    side = half // 4
    tail = side * side - LANES
    row_tiles = head_ref.shape[0] // 8
    lane = iota((8, LANES), 1)

    def source(cell, j, odd):
        yl = cell // side
        xl = cell - yl * side
        y = jnp.where(yf == 1, side - 1 - yl, yl)
        xx = side * j + xl
        xx = jnp.where(xf == 1, half - 1 - xx, xx)
        return y * half + xx + odd * (LANES // 2)

    span = -(-side * half // LANES)
    rest_base = jnp.where(yf == 1, 0, span - 2)
    group = lane // tail
    for odd in range(2):
        for j in range(4):
            src = source(lane, j, odd)
            tile_of, lane_of = src // LANES, src % LANES
            hits = [tile_of == k for k in range(span)]
            rest = source(LANES + lane % tail, j, odd)
            rest_hit = rest // LANES == rest_base
            rest_lane = rest % LANES
            for i in [k for k in brick_rows if k % 2 == odd]:
                base = side * half * i // LANES - first_tile
                brick = (i ^ (3 * yf)) * 4 + j
                packed = jnp.zeros((8, LANES), F32)
                for r in range(row_tiles):
                    cut = pl.ds(8 * r, 8)
                    value = jnp.take_along_axis(a_ref[base, cut], lane_of, axis=1)
                    for k in range(1, span):
                        value = jnp.where(hits[k], jnp.take_along_axis(a_ref[base + k, cut], lane_of, axis=1), value)
                    out_ref[brick, cut] = value
                    low = jnp.take_along_axis(a_ref[base + rest_base, cut], rest_lane, axis=1)
                    high = jnp.take_along_axis(a_ref[base + rest_base + 1, cut], rest_lane, axis=1)
                    packed = jnp.where(group == r, jnp.where(rest_hit, low, high), packed)
                out_ref[brick, pl.ds(8 * row_tiles, 8)] = packed


def patch_half(half, tiles, brick_rows, last, aug_code, shifted, plane, depth_w, head, extra=()):
    kept = head.shape[0]
    bricks = jax.ShapeDtypeStruct((16, kept + 8, LANES), F32)
    carry = jax.ShapeDtypeStruct((kept, LANES), F32)
    return pl.pallas_call(
        functools.partial(patch_kernel, half, tiles, brick_rows, last),
        out_shape=[bricks] if last else [bricks, carry],
        in_specs=[smem()] + [vmem()] * (4 + len(extra)),
        out_specs=[vmem()] if last else [vmem()] * 2,
        scratch_shapes=[pltpu.VMEM((2 * len(tiles) + 1, kept, LANES), F32)],
        input_output_aliases={6: 0} if last else {},
        compiler_params=params(),
        cost_estimate=cost(10**9),
    )(aug_code, shifted, plane, depth_w, head, *extra)


def seed_kernel(owner_ref, out_ref):
    here = iota(out_ref.shape, 1) == lax.axis_index("patch")
    out_ref[...] = jnp.where(here, owner_ref[0], 0)


def seed_table(owner, devices):
    width = -(-devices // LANES) * LANES
    return pl.pallas_call(
        seed_kernel,
        out_shape=jax.ShapeDtypeStruct((1, width), I32),
        in_specs=[smem()],
        out_specs=vmem(),
        compiler_params=params(),
        name="seed",
    )(owner)


def partner(devices, bit):
    return [(d, d ^ bit) for d in range(devices)]


def slots_kernel(devices, bits, table_ref, anchor_ref, mine_ref, other_ref, window_ref, send_ref, keep_ref, place_ref):
    me = lax.axis_index("patch")
    brick_rows = devices // 4

    def note(b, _):
        place_ref[table_ref[0, b]] = b
        return 0

    lax.fori_loop(0, devices, note, 0)
    anchor = anchor_ref[0]
    count = 1 << len(bits)
    _, rows, lanes = mine_ref.shape
    spare = iota((rows, lanes), 1) - jnp.where(iota((rows, lanes), 0) == rows - 8, SPARE, lanes)
    for s in range(count):
        mask = functools.reduce(lambda a, b: a ^ b, [bit for k, bit in enumerate(bits) if s >> (len(bits) - 1 - k) & 1], 0)
        brick = place_ref[me ^ mask]
        row = lax.rem(brick // 4 - anchor + brick_rows, brick_rows)
        at = row * 4 + brick % 4
        if brick_rows > 4:
            at = jnp.where(row < 4, at, 0)
        value = (mine_ref[at] + other_ref[at]) * window_ref[at]
        value = jnp.where(spare == row, 2.0, value)
        value = jnp.where(spare == 4, 2.0 * (brick % 4).astype(F32), value)
        if brick_rows > 4:
            value = jnp.where(row < 4, value, 0.0)
        if s < count // 2:
            keep_ref[s] = value
        else:
            send_ref[s - count // 2] = value


def fill_slots(devices, bits, table, anchor, mine, other, window):
    shape = jax.ShapeDtypeStruct((1 << (len(bits) - 1),) + mine.shape[1:], F32)
    return pl.pallas_call(
        functools.partial(slots_kernel, devices, bits),
        out_shape=[shape, shape],
        in_specs=[smem()] * 2 + [vmem()] * 3,
        out_specs=[vmem()] * 2,
        scratch_shapes=[pltpu.SMEM((devices,), I32)],
        compiler_params=params(),
        name="slots",
    )(table, anchor, mine, other, window)


def brick_kernel(side, maps, depth_curve, mine_ref, other_ref, rows_ref, cols_ref, out_ref):
    depth = len(depth_curve)
    wide = 2 * side
    plane = wide * wide
    tail = side * side - LANES
    per = depth * maps
    brick = mine_ref[0] + other_ref[0]
    kept = 4 * per
    main, packed = brick[:kept], brick[kept:]
    rest = jnp.concatenate([packed if k == 0 else pltpu.roll(packed, LANES - tail * k, 1) for k in range(kept // 8)], axis=0)
    fill = jnp.zeros((16 - per, LANES), F32)
    mains = [jnp.concatenate([main[per * p : per * (p + 1)], fill], axis=0) for p in range(4)]
    rests = [jnp.concatenate([rest[per * p : per * (p + 1)], fill], axis=0) for p in range(4)]
    columns = []
    for d in range(-(-plane // LANES)):
        n = iota((8, LANES), 1) + d * LANES
        y = n // wide
        x = n - y * wide
        cell = (y // 2) * side + x // 2
        quarter = 2 * (y % 2) + x % 2
        lane_of = cell % LANES
        top = min((d + 1) * LANES, plane) - 1
        tiles = []
        for r in range(2):
            cut = slice(8 * r, 8 * r + 8)
            value = None
            for p in range(4):
                one = jnp.take_along_axis(mains[p][cut], lane_of, axis=1)
                if (top // wide // 2 + 1) * side > LANES:
                    one = jnp.where(cell >= LANES, jnp.take_along_axis(rests[p][cut], lane_of, axis=1), one)
                value = one if value is None else jnp.where(quarter == p, one, value)
            tiles.append(value)
        columns.append(jnp.concatenate(tiles, axis=0))
    cells = jnp.concatenate(columns, axis=1)[:, :plane]
    for z in range(depth):
        out_ref[0, pl.ds(0, maps), pl.ds(z * plane, plane)] = cells[z * maps : (z + 1) * maps]

    def noted(k):
        lane = jnp.take_along_axis(packed, jnp.full((8, LANES), SPARE + k, I32), axis=1)[0:1]
        return jnp.concatenate([lane] * (rows_ref.shape[1] // LANES), axis=1)

    counts = [noted(i) for i in range(4)]
    added = counts[0] + counts[1] + counts[2] + counts[3]
    column = noted(4)
    down = sum(counts[i] * rows_ref[pl.ds(i, 1), :] for i in range(4))
    across = sum(jnp.where(column == j * added, cols_ref[pl.ds(j, 1), :], 0.0) for j in range(4))
    window = (down * across)[:, :plane]
    for z in range(depth):
        out_ref[0, pl.ds(maps, 1), pl.ds(z * plane, plane)] = window * depth_curve[z]


def finish(side, maps, depth, mine, other):
    plane = 4 * side * side
    width = -(-plane // LANES) * LANES
    curve = bump(8 * side)
    n = np.arange(width)
    y, x = np.minimum(n // (2 * side), 2 * side - 1), n % (2 * side)
    rows = np.stack([curve[2 * side * i + y] for i in range(4)]).astype(np.float32)
    cols = np.stack([curve[2 * side * i + x] for i in range(4)]).astype(np.float32)
    depth_curve = [float(np.float32(v)) for v in bump(depth)]
    return pl.pallas_call(
        functools.partial(brick_kernel, side, maps, depth_curve),
        out_shape=jax.ShapeDtypeStruct((1, maps + 1, depth * plane), F32),
        in_specs=[vmem()] * 4,
        out_specs=vmem(),
        compiler_params=params(),
        name="brick",
    )(mine, other, rows, cols)


def wire_window(side, maps, depth):
    curve_y, curve_z = bump(8 * side), bump(depth)
    cell = np.arange(side * side)
    out = np.zeros((16, 4 * depth * maps, side * side))
    for i in range(4):
        for j in range(4):
            for p in range(4):
                y = curve_y[2 * side * i + 2 * (cell // side) + p // 2]
                x = curve_y[2 * side * j + 2 * (cell % side) + p % 2]
                for z in range(depth):
                    for m in range(maps):
                        out[4 * i + j, (p * depth + z) * maps + m] = curve_z[z] * y * x
    kept = out.shape[1]
    tail = side * side - LANES
    packed = np.zeros((16, 8, LANES))
    for k in range(kept // 8):
        packed[:, :, tail * k : tail * (k + 1)] = out[:, 8 * k : 8 * k + 8, LANES:]
    return np.concatenate([out[:, :, :LANES], packed], axis=1).astype(np.float32)


def on_device(features, w_in, w_plane, w_depth, w_head, brick_owner, patch_anchor, aug_code):
    devices = lax.axis_size("patch")
    _, _, depth, cells = features.shape
    side = math.isqrt(cells) // 4
    maps = w_head.shape[0]
    bits = [1] + [1 << k | 1 for k in range(1, devices.bit_length() - 1)]

    table = seed_table(brick_owner, devices)
    tables = [table]
    for bit in bits[1:] + bits[:1]:
        got = lax.ppermute(tables[-1], "patch", partner(devices, bit))
        tables.append(tables[-1] + got)
    table = tables[-1]
    plane, depth_w, head, shifted = front(aug_code, w_in, w_plane, w_depth, w_head, features[0])
    half = math.isqrt(cells)
    steps = cells // (2 * LANES)
    ready = -(-half * half // 2 // (2 * LANES))
    bricks, carry = patch_half(half, range(ready), (0, 1), False, aug_code, shifted, plane, depth_w, head)
    (bricks,) = patch_half(half, range(ready, steps), (2, 3), True, aug_code, shifted, plane, depth_w, head, (carry, bricks))
    other = lax.ppermute(bricks, "patch", partner(devices, 1))
    send, keep = fill_slots(devices, bits[1:], table, patch_anchor, bricks, other, wire_window(side, maps, depth))
    for bit in bits[1:-1]:
        got = lax.ppermute(send, "patch", partner(devices, bit))
        half = send.shape[0] // 2
        keep, send = keep[:half] + got[:half], keep[half:] + got[half:]
    other = lax.ppermute(send, "patch", partner(devices, bits[-1]))
    return finish(side, maps, depth, keep, other)


def solution(mesh):
    one = P(("group", "patch"))
    in_specs = (P(("group", "patch"), None, None, None), P(), P(), P(), P(), one, one, one)
    return jax.shard_map(
        on_device, mesh=mesh, in_specs=in_specs, out_specs=P(("group", "patch"), None, None), check_vma=False
    )
```

```python
import functools
import math

import numpy as np

import jax
import jax.numpy as jnp
from jax import lax
from jax.experimental import pallas as pl
from jax.experimental.pallas import tpu as pltpu
from jax.sharding import PartitionSpec as P


F32 = jnp.float32
BF16 = jnp.bfloat16
I32 = jnp.int32
PAD = 32
LANES = 128
CHUNKS = 3
SPARE = 96


def iota(shape, axis):
    return lax.broadcasted_iota(I32, shape, axis)


def vmem():
    return pl.BlockSpec(memory_space=pltpu.VMEM)


def smem():
    return pl.BlockSpec(memory_space=pltpu.SMEM)


def hbm():
    return pl.BlockSpec(memory_space=pltpu.HBM)


def stay(*arrays):
    return [pltpu.with_memory_space_constraint(a, pltpu.HBM) for a in arrays]


def params():
    return pltpu.CompilerParams(vmem_limit_bytes=16 * 2**20)


def cost(flops):
    return pl.CostEstimate(flops=flops, bytes_accessed=2**20, transcendentals=0)


def bump(length):
    position = (np.arange(length, dtype=np.float64) + 0.5) / length
    return 0.1 + np.sin(np.pi * position) ** 2


def front_kernel(half, aug_ref, w_in_hbm, w_plane_hbm, w_depth_hbm, w_head_hbm, x_hbm, plane_ref, depth_ref, head_ref, xs_ref, w_in_ref, w_plane_ref, w_depth_ref, w_head_ref, x_ref, big_ref, plane_scr, depth_scr, sems):
    size = x_hbm.shape[2] // CHUNKS
    feats = [
        pltpu.make_async_copy(x_hbm.at[:, :, pl.ds(c * size, size)], x_ref.at[:, :, pl.ds(c * size, size)], sems.at[4 + c])
        for c in range(CHUNKS)
    ]
    pairs = ((w_plane_hbm, w_plane_ref), (w_in_hbm, w_in_ref), (w_depth_hbm, w_depth_ref), (w_head_hbm, w_head_ref))
    copies = [pltpu.make_async_copy(src, dst, sems.at[k]) for k, (src, dst) in enumerate(pairs)]
    for copy in copies + feats:
        copy.start()
    for copy in copies:
        copy.wait()
    hidden, _ = w_in_ref.shape
    depth = depth_ref.shape[0] // PAD
    maps = w_head_ref.shape[0]
    aug = aug_ref[0]
    zf, yf, xf = aug & 1, (aug >> 1) & 1, (aug >> 2) & 1

    rows, cols = big_ref.shape
    spread = (iota((rows, hidden), 0) % PAD == iota((rows, hidden), 1)).astype(BF16)
    gather = (iota((w_in_ref.shape[1], cols), 1) // depth == iota((w_in_ref.shape[1], cols), 0)).astype(BF16)
    tall = jnp.dot(spread, w_in_ref[...], preferred_element_type=F32).astype(BF16)
    wide = jnp.dot(tall, gather, preferred_element_type=F32)
    same = iota((rows, cols), 1) % depth == iota((rows, cols), 0) // PAD
    big_ref[...] = jnp.where(same, wide, 0.0).astype(BF16)

    plane_scr[...] = jnp.zeros_like(plane_scr)
    taps = [w_plane_ref[t].astype(F32) for t in range(9)]
    near = (((0,), (1, 2), ()), ((), (0, 1), (2,)))
    for py in range(2):
        for px in range(2):
            for dy in range(2):
                for dx in range(3):
                    hit = [taps[3 * ty + tx] for ty in near[py][dy + py] for tx in near[px][dx]]
                    if not hit:
                        continue
                    total = functools.reduce(lambda a, b: a + b, hit)
                    high = total.astype(BF16).astype(F32)
                    col = (3 * dy + dx) * PAD
                    plane_scr[py, pl.ds(px * PAD, hidden), pl.ds(col, hidden)] = high
                    plane_scr[py, pl.ds((2 + px) * PAD, hidden), pl.ds(col, hidden)] = total - high
    plane_ref[...] = plane_scr[...].astype(BF16)

    depth_scr[...] = jnp.zeros_like(depth_scr)
    for t in range(3):
        tap = w_depth_ref[t].astype(F32)
        for z in range(depth):
            if 0 <= z + t - 1 < depth:
                depth_scr[pl.ds(z * PAD, hidden), pl.ds((z + t - 1) * PAD, hidden)] = tap
    depth_ref[...] = depth_scr[...].astype(BF16)

    rows, cols = head_ref.shape
    pick = (iota((rows, maps), 0) % maps == iota((rows, maps), 1)).astype(BF16)
    tall = jnp.dot(pick, w_head_ref[...], preferred_element_type=F32).astype(BF16)
    gather = (iota((hidden, cols), 1) % PAD == iota((hidden, cols), 0)).astype(BF16)
    wide = jnp.dot(tall, gather, preferred_element_type=F32)
    at = iota((rows, cols), 0) // maps
    came = iota((rows, cols), 1) // PAD
    flip = (2 * yf + xf) * depth + (depth - 1) * zf
    head_ref[...] = jnp.where(at == (came ^ flip), wide, 0.0).astype(BF16)

    channels, depth, cells = x_ref.shape
    rows = depth * PAD
    margin = LANES
    zeros = jnp.zeros((rows, margin), BF16)
    for d in range(3):
        xs_ref[d, :, pl.ds(0, margin)] = zeros
        xs_ref[d, :, pl.ds(margin + cells, margin)] = zeros
    size = cells // CHUNKS
    column = iota((rows, size), 1)

    def shift(c, d):
        at = c * size
        block = xs_ref[1, :, pl.ds(at, size + 2 * margin)]
        moved = lax.slice_in_dim(block, margin + d - 1, margin + d - 1 + size, axis=1)
        edge = (column + at) % half == (0 if d == 0 else half - 1)
        xs_ref[d, :, pl.ds(margin + at, size)] = jnp.where(edge, jnp.zeros_like(moved), moved)

    for c in range(CHUNKS):
        part = pl.ds(c * size, size)
        feats[c].wait()
        x = x_ref[:, :, part].reshape(channels * depth, size)
        xs_ref[1, :, pl.ds(margin + c * size, size)] = jnp.dot(big_ref[...], x, preferred_element_type=F32).astype(BF16)
        shift(c, 0)
        if c > 0:
            shift(c - 1, 2)
    shift(CHUNKS - 1, 2)


def front(aug_code, w_in, w_plane, w_depth, w_head, feat):
    _, channels = w_in.shape
    maps = w_head.shape[0]
    _, depth, cells = feat.shape
    plane = (2, 4 * PAD, 6 * PAD)
    depth_w = (depth * PAD, depth * PAD)
    head = (4 * depth * maps, 4 * depth * PAD)
    shifted = (3, depth * PAD, cells + 2 * LANES)
    return pl.pallas_call(
        functools.partial(front_kernel, math.isqrt(cells)),
        out_shape=[jax.ShapeDtypeStruct(s, BF16) for s in (plane, depth_w, head, shifted)],
        in_specs=[smem()] + [hbm()] * 5,
        out_specs=[vmem()] * 4,
        scratch_shapes=[
            pltpu.VMEM(w_in.shape, BF16),
            pltpu.VMEM(w_plane.shape, BF16),
            pltpu.VMEM(w_depth.shape, BF16),
            pltpu.VMEM(w_head.shape, BF16),
            pltpu.VMEM(feat.shape, BF16),
            pltpu.VMEM((depth * PAD, channels * depth), BF16),
            pltpu.VMEM(plane, F32),
            pltpu.VMEM(depth_w, F32),
            pltpu.SemaphoreType.DMA((4 + CHUNKS,)),
        ],
        compiler_params=params(),
        cost_estimate=cost(10**8),
        name="front",
    )(aug_code, *stay(w_in, w_plane, w_depth, w_head, feat))


def patch_kernel(half, tiles, brick_rows, keep_from, last, aug_ref, xs_ref, plane_ref, depth_ref, head_ref, *refs):
    if last:
        carry_in, _, anchor_ref, out_ref, anchor_out, a_ref = refs
        anchor_out[...] = jnp.full(anchor_out.shape, anchor_ref[0], I32)
    else:
        out_ref, carry_out, a_ref = refs
    _, rows, _ = xs_ref.shape
    depth = rows // PAD
    step = 2 * LANES
    margin = LANES
    carried = carry_in.shape[0] if last else 0
    first_tile = tiles[0] * (step // LANES) - carried
    if last:
        a_ref[pl.ds(0, carried)] = carry_in[...]

    def window_stage(t):
        near = []
        for d in range(3):
            block = xs_ref[d, :, pl.ds(t * step, step + 2 * margin)]
            near.append([lax.slice_in_dim(block, margin + half * e, margin + half * e + step, axis=1) for e in (-1, 0, 1)])
        return near

    def plane_stage(near, z):
        cut = slice(z * PAD, (z + 1) * PAD)
        centre = near[1][1][cut].astype(F32)
        first = []
        for py in range(2):
            around = jnp.concatenate([near[d][py + e][cut] for e in range(2) for d in range(3)], axis=0)
            mix = jnp.dot(plane_ref[py], around, preferred_element_type=F32)
            for px in range(2):
                total = mix[px * PAD : (px + 1) * PAD] + mix[(2 + px) * PAD : (3 + px) * PAD]
                first.append((centre + jnp.maximum(total, 0.0)).astype(BF16))
        return first

    def depth_stage(first, p):
        one = jnp.concatenate([first[z][p] for z in range(depth)], axis=0)
        mix = jnp.dot(depth_ref[...], one, preferred_element_type=F32)
        return (one.astype(F32) + jnp.maximum(mix, 0.0)).astype(BF16)

    def head_stage(t, second):
        logits = jnp.zeros((head_ref.shape[0], step), F32)
        for q in range(2):
            pair = jnp.concatenate(second[2 * q : 2 * q + 2], axis=0)
            logits = logits + jnp.dot(head_ref[:, 2 * q * rows : 2 * (q + 1) * rows], pair, preferred_element_type=F32)
        affinity = jax.nn.sigmoid(logits)
        for u in range(step // LANES):
            a_ref[t * (step // LANES) + u - first_tile] = affinity[:, u * LANES : (u + 1) * LANES]

    aug = aug_ref[0]
    yf, xf = (aug >> 1) & 1, (aug >> 2) & 1
    side = half // 4
    tail = side * side - LANES
    row_tiles = head_ref.shape[0] // 8
    lane = iota((8, LANES), 1)
    group = lane // tail
    span = -(-side * half // LANES)
    near_tiles = span - 2

    def source(cell, j, odd):
        y = cell // side
        x = cell - y * side
        y = jnp.where(yf == 1, side - 1 - y, y)
        x = jnp.where(xf == 1, side - 1 - x, x)
        return y * half + side * j + x + odd * (LANES // 2)

    def cut_stage(i, j):
        odd = i % 2
        owned = []
        for k in range(span):
            x = (lane + k * LANES + half - odd * (LANES // 2) % half) % half
            owned.append((x >= side * j) & (x < side * (j + 1)))
        src = source(lane, j, odd)
        main_lane, main_near = src % LANES, src < near_tiles * LANES
        rest_lane = source(LANES + lane % tail, j, odd) % LANES
        base = side * half * i // LANES - first_tile
        brick = (i ^ (3 * yf)) * 4 + (j ^ (3 * xf))
        packed = jnp.zeros((8, LANES), F32)
        for r in range(row_tiles):
            cut = pl.ds(8 * r, 8)
            merged = []
            for tiles_of in (range(near_tiles), range(near_tiles, span)):
                one = a_ref[base + tiles_of[0], cut]
                for k in tiles_of[1:]:
                    one = jnp.where(owned[k], a_ref[base + k, cut], one)
                merged.append(one)
            low = jnp.take_along_axis(merged[0], main_lane, axis=1)
            high = jnp.take_along_axis(merged[1], main_lane, axis=1)
            out_ref[brick, cut] = jnp.where(main_near, low, high)
            rest = jnp.take_along_axis(jnp.where(yf == 1, merged[0], merged[1]), rest_lane, axis=1)
            packed = jnp.where(group == r, rest, packed)
        out_ref[brick, pl.ds(8 * row_tiles, 8)] = packed

    first, second = {}, {}
    waiting = [(i, j) for i in brick_rows for j in range(4)]
    done = first_tile + carried
    for k in range(len(tiles) + 2):
        if k < len(tiles):
            near = window_stage(tiles[k])
            first[k] = []
        second[k - 1] = []
        for q in range(4):
            if k < len(tiles) and q < depth:
                first[k].append(plane_stage(near, q))
            if 0 <= k - 1 < len(tiles):
                second[k - 1].append(depth_stage(first[k - 1], q))
            if waiting and done >= side * half * waiting[0][0] // LANES + span:
                cut_stage(*waiting.pop(0))
        if 0 <= k - 2 < len(tiles):
            head_stage(tiles[k - 2], second[k - 2])
            done += step // LANES
    for left in waiting:
        cut_stage(*left)
    if not last:
        carry_out[...] = a_ref[pl.ds(keep_from - first_tile, done - keep_from)]


def patch_half(half, tiles, brick_rows, keep_from, last, aug_code, shifted, plane, depth_w, head, extra=()):
    kept = head.shape[0]
    carried = extra[0].shape[0] if last else 0
    bricks = jax.ShapeDtypeStruct((16, kept + 8, LANES), F32)
    beside = jax.ShapeDtypeStruct((1, LANES), I32) if last else jax.ShapeDtypeStruct((2 * len(tiles) - keep_from, kept, LANES), F32)
    spaces = [vmem(), vmem(), smem()] if last else []
    return pl.pallas_call(
        functools.partial(patch_kernel, half, tiles, brick_rows, keep_from, last),
        out_shape=[bricks, beside],
        in_specs=[smem()] + [vmem()] * 4 + spaces,
        out_specs=[vmem()] * 2,
        scratch_shapes=[pltpu.VMEM((2 * len(tiles) + carried, kept, LANES), F32)],
        input_output_aliases={6: 0} if last else {},
        compiler_params=params(),
        cost_estimate=cost(10**9),
    )(aug_code, shifted, plane, depth_w, head, *extra)


def seed_kernel(owner_ref, out_ref):
    here = iota(out_ref.shape, 1) == lax.axis_index("patch")
    out_ref[...] = jnp.where(here, owner_ref[0], 0)


def seed_table(owner, devices):
    width = -(-devices // LANES) * LANES
    return pl.pallas_call(
        seed_kernel,
        out_shape=jax.ShapeDtypeStruct((1, width), I32),
        in_specs=[smem()],
        out_specs=vmem(),
        compiler_params=params(),
        name="seed",
    )(owner)


def partner(devices, bit):
    return [(d, d ^ bit) for d in range(devices)]


def slots_kernel(devices, bits, table_ref, anchor_ref, mine_ref, other_ref, window_ref, send_ref, keep_ref, place_ref):
    me = lax.axis_index("patch")
    brick_rows = devices // 4

    def note(b, _):
        place_ref[table_ref[0, b]] = b
        return 0

    lax.fori_loop(0, devices, note, 0)
    anchor = anchor_ref[0, 0]
    count = 1 << len(bits)
    _, rows, lanes = mine_ref.shape
    spare = iota((rows, lanes), 1) - jnp.where(iota((rows, lanes), 0) == rows - 8, SPARE, lanes)
    for s in range(count):
        mask = functools.reduce(lambda a, b: a ^ b, [bit for k, bit in enumerate(bits) if s >> (len(bits) - 1 - k) & 1], 0)
        brick = place_ref[me ^ mask]
        row = lax.rem(brick // 4 - anchor + brick_rows, brick_rows)
        at = row * 4 + brick % 4
        if brick_rows > 4:
            at = jnp.where(row < 4, at, 0)
        value = (mine_ref[at] + other_ref[at]) * window_ref[at]
        value = jnp.where(spare == row, 2.0, value)
        value = jnp.where(spare == 4, 2.0 * (brick % 4).astype(F32), value)
        if brick_rows > 4:
            value = jnp.where(row < 4, value, 0.0)
        if s < count // 2:
            keep_ref[s] = value
        else:
            send_ref[s - count // 2] = value


def fill_slots(devices, bits, table, anchor, mine, other, window):
    shape = jax.ShapeDtypeStruct((1 << (len(bits) - 1),) + mine.shape[1:], F32)
    return pl.pallas_call(
        functools.partial(slots_kernel, devices, bits),
        out_shape=[shape, shape],
        in_specs=[smem()] * 2 + [vmem()] * 3,
        out_specs=[vmem()] * 2,
        scratch_shapes=[pltpu.SMEM((devices,), I32)],
        compiler_params=params(),
        name="slots",
    )(table, anchor, mine, other, window)


def brick_kernel(side, maps, depth_curve, mine_ref, a_ref, b_ref, c_ref, rows_ref, cols_ref, out_ref):
    depth = len(depth_curve)
    wide = 2 * side
    plane = wide * wide
    tail = side * side - LANES
    per = depth * maps
    brick = (mine_ref[0] + a_ref[0]) + (b_ref[0] + c_ref[0])
    kept = 4 * per
    main, packed = brick[:kept], brick[kept:]
    rest = jnp.concatenate([packed if k == 0 else pltpu.roll(packed, LANES - tail * k, 1) for k in range(kept // 8)], axis=0)
    fill = jnp.zeros((16 - per, LANES), F32)
    mains = [jnp.concatenate([main[per * p : per * (p + 1)], fill], axis=0) for p in range(4)]
    rests = [jnp.concatenate([rest[per * p : per * (p + 1)], fill], axis=0) for p in range(4)]
    columns = []
    for d in range(-(-plane // LANES)):
        n = iota((8, LANES), 1) + d * LANES
        y = n // wide
        x = n - y * wide
        cell = (y // 2) * side + x // 2
        quarter = 2 * (y % 2) + x % 2
        lane_of = cell % LANES
        top = min((d + 1) * LANES, plane) - 1
        tiles = []
        for r in range(2):
            cut = slice(8 * r, 8 * r + 8)
            value = None
            for p in range(4):
                one = jnp.take_along_axis(mains[p][cut], lane_of, axis=1)
                if (top // wide // 2 + 1) * side > LANES:
                    one = jnp.where(cell >= LANES, jnp.take_along_axis(rests[p][cut], lane_of, axis=1), one)
                value = one if value is None else jnp.where(quarter == p, one, value)
            tiles.append(value)
        columns.append(jnp.concatenate(tiles, axis=0))
    cells = jnp.concatenate(columns, axis=1)[:, :plane]
    for z in range(depth):
        out_ref[0, pl.ds(0, maps), pl.ds(z * plane, plane)] = cells[z * maps : (z + 1) * maps]

    def noted(k):
        lane = jnp.take_along_axis(packed, jnp.full((8, LANES), SPARE + k, I32), axis=1)[0:1]
        return jnp.concatenate([lane] * (rows_ref.shape[1] // LANES), axis=1)

    counts = [noted(i) for i in range(4)]
    added = counts[0] + counts[1] + counts[2] + counts[3]
    column = noted(4)
    down = sum(counts[i] * rows_ref[pl.ds(i, 1), :] for i in range(4))
    across = sum(jnp.where(column == j * added, cols_ref[pl.ds(j, 1), :], 0.0) for j in range(4))
    window = (down * across)[:, :plane]
    for z in range(depth):
        out_ref[0, pl.ds(maps, 1), pl.ds(z * plane, plane)] = window * depth_curve[z]


def finish(side, maps, depth, mine, others):
    plane = 4 * side * side
    width = -(-plane // LANES) * LANES
    curve = bump(8 * side)
    n = np.arange(width)
    y, x = np.minimum(n // (2 * side), 2 * side - 1), n % (2 * side)
    rows = np.stack([curve[2 * side * i + y] for i in range(4)]).astype(np.float32)
    cols = np.stack([curve[2 * side * i + x] for i in range(4)]).astype(np.float32)
    depth_curve = [float(np.float32(v)) for v in bump(depth)]
    return pl.pallas_call(
        functools.partial(brick_kernel, side, maps, depth_curve),
        out_shape=jax.ShapeDtypeStruct((1, maps + 1, depth * plane), F32),
        in_specs=[vmem()] * 6,
        out_specs=vmem(),
        compiler_params=params(),
        name="brick",
    )(mine, *others, rows, cols)


def wire_window(side, maps, depth):
    curve_y, curve_z = bump(8 * side), bump(depth)
    cell = np.arange(side * side)
    out = np.zeros((16, 4 * depth * maps, side * side))
    for i in range(4):
        for j in range(4):
            for p in range(4):
                y = curve_y[2 * side * i + 2 * (cell // side) + p // 2]
                x = curve_y[2 * side * j + 2 * (cell % side) + p % 2]
                for z in range(depth):
                    for m in range(maps):
                        out[4 * i + j, (p * depth + z) * maps + m] = curve_z[z] * y * x
    kept = out.shape[1]
    tail = side * side - LANES
    packed = np.zeros((16, 8, LANES))
    for k in range(kept // 8):
        packed[:, :, tail * k : tail * (k + 1)] = out[:, 8 * k : 8 * k + 8, LANES:]
    return np.concatenate([out[:, :, :LANES], packed], axis=1).astype(np.float32)


def on_device(features, w_in, w_plane, w_depth, w_head, brick_owner, patch_anchor, aug_code):
    devices = lax.axis_size("patch")
    _, _, depth, cells = features.shape
    side = math.isqrt(cells) // 4
    maps = w_head.shape[0]
    levels = [1 << k for k in range(devices.bit_length() - 1)]
    paired = levels[:1] + [bit | 1 for bit in levels[1:]]
    bits = paired[1:-2] + [levels[-2], paired[-1]]

    table = seed_table(brick_owner, devices)
    tables = [table]
    for bit in paired[1:] + paired[:1]:
        got = lax.ppermute(tables[-1], "patch", partner(devices, bit))
        tables.append(tables[-1] + got)
    table = tables[-1]
    plane, depth_w, head, shifted = front(aug_code, w_in, w_plane, w_depth, w_head, features[0])
    half = math.isqrt(cells)
    steps = cells // (2 * LANES)
    ready = -(-half * half // 2 // (2 * LANES))
    quarter = half * half // 4 // LANES
    bricks, carry = patch_half(half, range(ready), (0,), quarter, False, aug_code, shifted, plane, depth_w, head)
    bricks, anchor = patch_half(
        half, range(ready, steps), (1, 2, 3), 0, True, aug_code, shifted, plane, depth_w, head, (carry, bricks, patch_anchor)
    )
    other = lax.ppermute(bricks, "patch", partner(devices, 1))
    send, keep = fill_slots(devices, bits, table, anchor, bricks, other, wire_window(side, maps, depth))
    for bit in bits[:-2]:
        got = lax.ppermute(send, "patch", partner(devices, bit))
        half = send.shape[0] // 2
        last = half == 2
        cuts = [slice(k, k + 1) for k in range(4)] if last else [slice(0, half), slice(half, 2 * half)]
        parts = [keep[c] + got[c] for c in cuts]
        if not last:
            keep, send = parts
    far = [bits[-1], bits[-2], bits[-1] ^ bits[-2]]
    others = [lax.ppermute(part, "patch", partner(devices, bit)) for part, bit in zip(parts[1:], far)]
    return finish(side, maps, depth, parts[0], others)


def solution(mesh):
    one = P(("group", "patch"))
    in_specs = (P(("group", "patch"), None, None, None), P(), P(), P(), P(), one, one, one)
    return jax.shard_map(
        on_device, mesh=mesh, in_specs=in_specs, out_specs=P(("group", "patch"), None, None), check_vma=False
    )
```

```python
import functools
import math

import numpy as np

import jax
import jax.numpy as jnp
from jax import lax
from jax.experimental import pallas as pl
from jax.experimental.pallas import tpu as pltpu
from jax.sharding import PartitionSpec as P


F32 = jnp.float32
BF16 = jnp.bfloat16
I32 = jnp.int32
PAD = 32
LANES = 128
CHUNKS = 2
LEAD = -1
SPARE = 96


def iota(shape, axis):
    return lax.broadcasted_iota(I32, shape, axis)


def vmem():
    return pl.BlockSpec(memory_space=pltpu.VMEM)


def smem():
    return pl.BlockSpec(memory_space=pltpu.SMEM)


def hbm():
    return pl.BlockSpec(memory_space=pltpu.HBM)


def stay(*arrays):
    return [pltpu.with_memory_space_constraint(a, pltpu.HBM) for a in arrays]


def params():
    return pltpu.CompilerParams(vmem_limit_bytes=16 * 2**20)


def cost(flops):
    return pl.CostEstimate(flops=flops, bytes_accessed=2**20, transcendentals=0)


def bump(length):
    position = (np.arange(length, dtype=np.float64) + 0.5) / length
    return 0.1 + np.sin(np.pi * position) ** 2


def front_kernel(aug_ref, w_in_hbm, w_plane_hbm, w_depth_hbm, w_head_hbm, x_hbm, plane_ref, depth_ref, head_ref, xs_ref, w_in_ref, w_plane_ref, w_depth_ref, w_head_ref, x_ref, big_ref, plane_scr, depth_scr, sems):
    size = x_hbm.shape[2] // CHUNKS
    feats = [
        pltpu.make_async_copy(x_hbm.at[:, :, pl.ds(c * size, size)], x_ref.at[:, :, pl.ds(c * size, size)], sems.at[4 + c])
        for c in range(CHUNKS)
    ]
    pairs = ((w_plane_hbm, w_plane_ref), (w_in_hbm, w_in_ref), (w_depth_hbm, w_depth_ref), (w_head_hbm, w_head_ref))
    copies = [pltpu.make_async_copy(src, dst, sems.at[k]) for k, (src, dst) in enumerate(pairs)]
    for copy in copies + feats:
        copy.start()
    for copy in copies:
        copy.wait()
    hidden, _ = w_in_ref.shape
    depth = depth_ref.shape[0] // PAD
    maps = w_head_ref.shape[0]
    aug = aug_ref[0]
    zf, yf, xf = aug & 1, (aug >> 1) & 1, (aug >> 2) & 1

    rows, cols = big_ref.shape
    spread = (iota((rows, hidden), 0) % PAD == iota((rows, hidden), 1)).astype(BF16)
    gather = (iota((w_in_ref.shape[1], cols), 1) // depth == iota((w_in_ref.shape[1], cols), 0)).astype(BF16)
    tall = jnp.dot(spread, w_in_ref[...], preferred_element_type=F32).astype(BF16)
    wide = jnp.dot(tall, gather, preferred_element_type=F32)
    same = iota((rows, cols), 1) % depth == iota((rows, cols), 0) // PAD
    big_ref[...] = jnp.where(same, wide, 0.0).astype(BF16)

    plane_scr[...] = jnp.zeros_like(plane_scr)
    taps = [w_plane_ref[t].astype(F32) for t in range(9)]
    near = (((0,), (1, 2), ()), ((), (0, 1), (2,)))
    for py in range(2):
        for px in range(2):
            for dy in range(2):
                for dx in range(3):
                    hit = [taps[3 * ty + tx] for ty in near[py][dy + py] for tx in near[px][dx]]
                    if not hit:
                        continue
                    total = functools.reduce(lambda a, b: a + b, hit)
                    high = total.astype(BF16).astype(F32)
                    col = (3 * dy + dx) * PAD
                    plane_scr[py, pl.ds(px * PAD, hidden), pl.ds(col, hidden)] = high
                    plane_scr[py, pl.ds((2 + px) * PAD, hidden), pl.ds(col, hidden)] = total - high
    plane_ref[...] = plane_scr[...].astype(BF16)

    depth_scr[...] = jnp.zeros_like(depth_scr)
    for t in range(3):
        tap = w_depth_ref[t].astype(F32)
        for z in range(depth):
            if 0 <= z + t - 1 < depth:
                depth_scr[pl.ds(z * PAD, hidden), pl.ds((z + t - 1) * PAD, hidden)] = tap
    depth_ref[...] = depth_scr[...].astype(BF16)

    rows, cols = head_ref.shape
    pick = (iota((rows, maps), 0) % maps == iota((rows, maps), 1)).astype(BF16)
    tall = jnp.dot(pick, w_head_ref[...], preferred_element_type=F32).astype(BF16)
    gather = (iota((hidden, cols), 1) % PAD == iota((hidden, cols), 0)).astype(BF16)
    wide = jnp.dot(tall, gather, preferred_element_type=F32)
    at = iota((rows, cols), 0) // maps
    came = iota((rows, cols), 1) // PAD
    flip = (2 * yf + xf) * depth + (depth - 1) * zf
    head_ref[...] = jnp.where(at == (came ^ flip), wide, 0.0).astype(BF16)

    channels, depth, cells = x_ref.shape
    zeros = jnp.zeros((depth * PAD, LANES), BF16)
    xs_ref[:, pl.ds(0, LANES)] = zeros
    xs_ref[:, pl.ds(LANES + cells, LANES)] = zeros
    for c, copy in enumerate(feats):
        part = pl.ds(c * size, size)
        copy.wait()
        x = x_ref[:, :, part].reshape(channels * depth, size)
        xs_ref[:, pl.ds(LANES + c * size, size)] = jnp.dot(big_ref[...], x, preferred_element_type=F32).astype(BF16)


def front(aug_code, w_in, w_plane, w_depth, w_head, feat):
    _, channels = w_in.shape
    maps = w_head.shape[0]
    _, depth, cells = feat.shape
    plane = (2, 4 * PAD, 6 * PAD)
    depth_w = (depth * PAD, depth * PAD)
    head = (4 * depth * maps, 4 * depth * PAD)
    padded = (depth * PAD, cells + 2 * LANES)
    return pl.pallas_call(
        front_kernel,
        out_shape=[jax.ShapeDtypeStruct(s, BF16) for s in (plane, depth_w, head, padded)],
        in_specs=[smem()] + [hbm()] * 5,
        out_specs=[vmem()] * 4,
        scratch_shapes=[
            pltpu.VMEM(w_in.shape, BF16),
            pltpu.VMEM(w_plane.shape, BF16),
            pltpu.VMEM(w_depth.shape, BF16),
            pltpu.VMEM(w_head.shape, BF16),
            pltpu.VMEM(feat.shape, BF16),
            pltpu.VMEM((depth * PAD, channels * depth), BF16),
            pltpu.VMEM(plane, F32),
            pltpu.VMEM(depth_w, F32),
            pltpu.SemaphoreType.DMA((4 + CHUNKS,)),
        ],
        compiler_params=params(),
        cost_estimate=cost(10**8),
        name="front",
    )(aug_code, *stay(w_in, w_plane, w_depth, w_head, feat))


def patch_kernel(half, tiles, brick_rows, keep_from, last, aug_ref, xs_ref, plane_ref, depth_ref, head_ref, *refs):
    if last:
        carry_in, _, anchor_ref, out_ref, anchor_out, a_ref = refs
        anchor_out[...] = jnp.full(anchor_out.shape, anchor_ref[0], I32)
    else:
        out_ref, carry_out, a_ref = refs
    rows, _ = xs_ref.shape
    depth = rows // PAD
    step = 2 * LANES
    margin = LANES
    carried = carry_in.shape[0] if last else 0
    first_tile = tiles[0] * (step // LANES) - carried
    if last:
        a_ref[pl.ds(0, carried)] = carry_in[...]

    def window_stage(t):
        column = (iota((rows, step), 1) + t * step) % half
        block = xs_ref[:, pl.ds(t * step, step + 2 * margin)]
        near = []
        for d in (-1, 0, 1):
            near.append([])
            for e in (-1, 0, 1):
                at = margin + half * e + d
                one = lax.slice_in_dim(block, at, at + step, axis=1)
                if d:
                    one = jnp.where(column == (0 if d < 0 else half - 1), jnp.zeros_like(one), one)
                near[-1].append(one)
        return near

    def plane_stage(near, z):
        cut = slice(z * PAD, (z + 1) * PAD)
        centre = near[1][1][cut].astype(F32)
        first = []
        for py in range(2):
            around = jnp.concatenate([near[d][py + e][cut] for e in range(2) for d in range(3)], axis=0)
            mix = jnp.dot(plane_ref[py], around, preferred_element_type=F32)
            for px in range(2):
                total = mix[px * PAD : (px + 1) * PAD] + mix[(2 + px) * PAD : (3 + px) * PAD]
                first.append((centre + jnp.maximum(total, 0.0)).astype(BF16))
        return first

    def depth_stage(first, p):
        one = jnp.concatenate([first[z][p] for z in range(depth)], axis=0)
        mix = jnp.dot(depth_ref[...], one, preferred_element_type=F32)
        return (one.astype(F32) + jnp.maximum(mix, 0.0)).astype(BF16)

    def head_stage(t, second):
        logits = jnp.zeros((head_ref.shape[0], step), F32)
        for q in range(2):
            pair = jnp.concatenate(second[2 * q : 2 * q + 2], axis=0)
            logits = logits + jnp.dot(head_ref[:, 2 * q * rows : 2 * (q + 1) * rows], pair, preferred_element_type=F32)
        affinity = jax.nn.sigmoid(logits)
        for u in range(step // LANES):
            a_ref[t * (step // LANES) + u - first_tile] = affinity[:, u * LANES : (u + 1) * LANES]

    aug = aug_ref[0]
    yf, xf = (aug >> 1) & 1, (aug >> 2) & 1
    side = half // 4
    tail = side * side - LANES
    row_tiles = head_ref.shape[0] // 8
    lane = iota((8, LANES), 1)
    group = lane // tail
    span = -(-side * half // LANES)
    near_tiles = span - 2

    def source(cell, j, odd):
        y = cell // side
        x = cell - y * side
        y = jnp.where(yf == 1, side - 1 - y, y)
        x = jnp.where(xf == 1, side - 1 - x, x)
        return y * half + side * j + x + odd * (LANES // 2)

    def cut_stage(i, j):
        odd = i % 2
        owned = []
        for k in range(span):
            x = (lane + k * LANES + half - odd * (LANES // 2) % half) % half
            owned.append((x >= side * j) & (x < side * (j + 1)))
        src = source(lane, j, odd)
        main_lane, main_near = src % LANES, src < near_tiles * LANES
        rest_lane = source(LANES + lane % tail, j, odd) % LANES
        base = side * half * i // LANES - first_tile
        brick = (i ^ (3 * yf)) * 4 + (j ^ (3 * xf))
        packed = jnp.zeros((8, LANES), F32)
        for r in range(row_tiles):
            cut = pl.ds(8 * r, 8)
            merged = []
            for tiles_of in (range(near_tiles), range(near_tiles, span)):
                one = a_ref[base + tiles_of[0], cut]
                for k in tiles_of[1:]:
                    one = jnp.where(owned[k], a_ref[base + k, cut], one)
                merged.append(one)
            low = jnp.take_along_axis(merged[0], main_lane, axis=1)
            high = jnp.take_along_axis(merged[1], main_lane, axis=1)
            out_ref[brick, cut] = jnp.where(main_near, low, high)
            rest = jnp.take_along_axis(jnp.where(yf == 1, merged[0], merged[1]), rest_lane, axis=1)
            packed = jnp.where(group == r, rest, packed)
        out_ref[brick, pl.ds(8 * row_tiles, 8)] = packed

    first, second = {}, {}
    waiting = [(i, j) for i in brick_rows for j in range(4)]
    done = first_tile + carried
    for k in range(len(tiles) + 2):
        if k < len(tiles):
            near = window_stage(tiles[k])
            first[k] = []
        second[k - 1] = []
        for q in range(4):
            if k < len(tiles) and q < depth:
                first[k].append(plane_stage(near, q))
            if 0 <= k - 1 < len(tiles):
                second[k - 1].append(depth_stage(first[k - 1], q))
            if waiting and done >= side * half * waiting[0][0] // LANES + span:
                cut_stage(*waiting.pop(0))
        if 0 <= k - 2 < len(tiles):
            head_stage(tiles[k - 2], second[k - 2])
            done += step // LANES
    for left in waiting:
        cut_stage(*left)
    if not last:
        carry_out[...] = a_ref[pl.ds(keep_from - first_tile, done - keep_from)]


def patch_half(half, tiles, brick_rows, keep_from, last, aug_code, shifted, plane, depth_w, head, extra=()):
    kept = head.shape[0]
    carried = extra[0].shape[0] if last else 0
    bricks = jax.ShapeDtypeStruct((16, kept + 8, LANES), F32)
    beside = jax.ShapeDtypeStruct((1, LANES), I32) if last else jax.ShapeDtypeStruct((2 * len(tiles) - keep_from, kept, LANES), F32)
    spaces = [vmem(), vmem(), smem()] if last else []
    return pl.pallas_call(
        functools.partial(patch_kernel, half, tiles, brick_rows, keep_from, last),
        out_shape=[bricks, beside],
        in_specs=[smem()] + [vmem()] * 4 + spaces,
        out_specs=[vmem()] * 2,
        scratch_shapes=[pltpu.VMEM((2 * len(tiles) + carried, kept, LANES), F32)],
        input_output_aliases={6: 0} if last else {},
        compiler_params=params(),
        cost_estimate=cost(10**9),
    )(aug_code, shifted, plane, depth_w, head, *extra)


def seed_kernel(owner_ref, out_ref):
    here = iota(out_ref.shape, 1) == lax.axis_index("patch")
    out_ref[...] = jnp.where(here, owner_ref[0], 0)


def seed_table(owner, devices):
    width = -(-devices // LANES) * LANES
    return pl.pallas_call(
        seed_kernel,
        out_shape=jax.ShapeDtypeStruct((1, width), I32),
        in_specs=[smem()],
        out_specs=vmem(),
        compiler_params=params(),
        name="seed",
    )(owner)


def partner(devices, bit):
    return [(d, d ^ bit) for d in range(devices)]


def slots_kernel(devices, bits, table_ref, anchor_ref, mine_ref, other_ref, window_ref, send_ref, keep_ref):
    me = lax.axis_index("patch")
    brick_rows = devices // 4
    brick = iota(table_ref.shape, 1)
    row = lax.rem(brick // 4 - anchor_ref[:, :1] + brick_rows, jnp.full_like(brick, brick_rows))
    place = row * 4 + brick % 4
    owner = jnp.where(brick < devices, table_ref[...], -1)
    count = 1 << len(bits)
    _, rows, lanes = mine_ref.shape
    spare = iota((rows, lanes), 1) - jnp.where(iota((rows, lanes), 0) == rows - 8, SPARE, lanes)
    places = []
    for s in range(count):
        mask = functools.reduce(lambda a, b: a ^ b, [bit for k, bit in enumerate(bits) if s >> (len(bits) - 1 - k) & 1], 0)
        places.append(jnp.sum(jnp.where(owner == (me ^ mask), place, 0)))
    for s, at in enumerate(places):
        covered = at < 16
        slot = at if brick_rows <= 4 else jnp.where(covered, at, 0)
        value = (mine_ref[slot] + other_ref[slot]) * window_ref[slot]
        value = jnp.where(spare == at // 4, 2.0, value)
        value = jnp.where(spare == 4, 2.0 * (at % 4).astype(F32), value)
        if brick_rows > 4:
            value = jnp.where(covered, value, 0.0)
        if s < count // 2:
            keep_ref[s] = value
        else:
            send_ref[s - count // 2] = value


def fill_slots(devices, bits, table, anchor, mine, other, window):
    shape = jax.ShapeDtypeStruct((1 << (len(bits) - 1),) + mine.shape[1:], F32)
    return pl.pallas_call(
        functools.partial(slots_kernel, devices, bits),
        out_shape=[shape, shape],
        in_specs=[vmem()] * 5,
        out_specs=[vmem()] * 2,
        compiler_params=params(),
        name="slots",
    )(table, anchor, mine, other, window)


def brick_kernel(side, maps, depth_curve, mine_ref, a_ref, b_ref, c_ref, rows_ref, cols_ref, out_ref):
    depth = len(depth_curve)
    wide = 2 * side
    plane = wide * wide
    tail = side * side - LANES
    per = depth * maps
    brick = (mine_ref[0] + a_ref[0]) + (b_ref[0] + c_ref[0])
    kept = 4 * per
    main, packed = brick[:kept], brick[kept:]
    rest = jnp.concatenate([packed if k == 0 else pltpu.roll(packed, LANES - tail * k, 1) for k in range(kept // 8)], axis=0)
    fill = jnp.zeros((16 - per, LANES), F32)
    mains = [jnp.concatenate([main[per * p : per * (p + 1)], fill], axis=0) for p in range(4)]
    rests = [jnp.concatenate([rest[per * p : per * (p + 1)], fill], axis=0) for p in range(4)]
    columns = []
    for d in range(-(-plane // LANES)):
        n = iota((8, LANES), 1) + d * LANES
        y = n // wide
        x = n - y * wide
        cell = (y // 2) * side + x // 2
        quarter = 2 * (y % 2) + x % 2
        lane_of = cell % LANES
        top = min((d + 1) * LANES, plane) - 1
        tiles = []
        for r in range(2):
            cut = slice(8 * r, 8 * r + 8)
            value = None
            for p in range(4):
                one = jnp.take_along_axis(mains[p][cut], lane_of, axis=1)
                if (top // wide // 2 + 1) * side > LANES:
                    one = jnp.where(cell >= LANES, jnp.take_along_axis(rests[p][cut], lane_of, axis=1), one)
                value = one if value is None else jnp.where(quarter == p, one, value)
            tiles.append(value)
        columns.append(jnp.concatenate(tiles, axis=0))
    cells = jnp.concatenate(columns, axis=1)[:, :plane]
    for z in range(depth):
        out_ref[0, pl.ds(0, maps), pl.ds(z * plane, plane)] = cells[z * maps : (z + 1) * maps]

    def noted(k):
        lane = jnp.take_along_axis(packed, jnp.full((8, LANES), SPARE + k, I32), axis=1)[0:1]
        return jnp.concatenate([lane] * (rows_ref.shape[1] // LANES), axis=1)

    counts = [noted(i) for i in range(4)]
    added = counts[0] + counts[1] + counts[2] + counts[3]
    column = noted(4)
    down = sum(counts[i] * rows_ref[pl.ds(i, 1), :] for i in range(4))
    across = sum(jnp.where(column == j * added, cols_ref[pl.ds(j, 1), :], 0.0) for j in range(4))
    window = (down * across)[:, :plane]
    for z in range(depth):
        out_ref[0, pl.ds(maps, 1), pl.ds(z * plane, plane)] = window * depth_curve[z]


def finish(side, maps, depth, mine, others):
    plane = 4 * side * side
    width = -(-plane // LANES) * LANES
    curve = bump(8 * side)
    n = np.arange(width)
    y, x = np.minimum(n // (2 * side), 2 * side - 1), n % (2 * side)
    rows = np.stack([curve[2 * side * i + y] for i in range(4)]).astype(np.float32)
    cols = np.stack([curve[2 * side * i + x] for i in range(4)]).astype(np.float32)
    depth_curve = [float(np.float32(v)) for v in bump(depth)]
    return pl.pallas_call(
        functools.partial(brick_kernel, side, maps, depth_curve),
        out_shape=jax.ShapeDtypeStruct((1, maps + 1, depth * plane), F32),
        in_specs=[vmem()] * 6,
        out_specs=vmem(),
        compiler_params=params(),
        name="brick",
    )(mine, *others, rows, cols)


def wire_window(side, maps, depth):
    curve_y, curve_z = bump(8 * side), bump(depth)
    cell = np.arange(side * side)
    out = np.zeros((16, 4 * depth * maps, side * side))
    for i in range(4):
        for j in range(4):
            for p in range(4):
                y = curve_y[2 * side * i + 2 * (cell // side) + p // 2]
                x = curve_y[2 * side * j + 2 * (cell % side) + p % 2]
                for z in range(depth):
                    for m in range(maps):
                        out[4 * i + j, (p * depth + z) * maps + m] = curve_z[z] * y * x
    kept = out.shape[1]
    tail = side * side - LANES
    packed = np.zeros((16, 8, LANES))
    for k in range(kept // 8):
        packed[:, :, tail * k : tail * (k + 1)] = out[:, 8 * k : 8 * k + 8, LANES:]
    return np.concatenate([out[:, :, :LANES], packed], axis=1).astype(np.float32)


def on_device(features, w_in, w_plane, w_depth, w_head, brick_owner, patch_anchor, aug_code):
    devices = lax.axis_size("patch")
    _, _, depth, cells = features.shape
    side = math.isqrt(cells) // 4
    maps = w_head.shape[0]
    levels = [1 << k for k in range(devices.bit_length() - 1)]
    paired = levels[:1] + [bit | 1 for bit in levels[1:]]
    bits = paired[1:-1] + [levels[-1]]

    def table_round(k, table):
        return table + lax.ppermute(table, "patch", partner(devices, rounds[k]))

    rounds = paired[1:] + paired[:1]
    table = table_round(0, seed_table(brick_owner, devices))
    plane, depth_w, head, shifted = front(aug_code, w_in, w_plane, w_depth, w_head, features[0])
    half = math.isqrt(cells)
    steps = cells // (2 * LANES)
    ready = -(-half * half // 2 // (2 * LANES)) + LEAD
    quarter = half * half // 4 // LANES
    table = table_round(1, table)
    bricks, carry = patch_half(half, range(ready), (0,), quarter, False, aug_code, shifted, plane, depth_w, head)
    patch_anchor, table = lax.optimization_barrier((patch_anchor, table))
    for k in range(2, len(rounds)):
        table = table_round(k, table)
    bricks, anchor = patch_half(
        half, range(ready, steps), (1, 2, 3), 0, True, aug_code, shifted, plane, depth_w, head, (carry, bricks, patch_anchor)
    )
    other = lax.ppermute(bricks, "patch", partner(devices, 1))
    send, keep = fill_slots(devices, bits, table, anchor, bricks, other, wire_window(side, maps, depth))
    for bit in bits[:-2]:
        got = lax.ppermute(send, "patch", partner(devices, bit))
        half = send.shape[0] // 2
        last = half == 2
        cuts = [slice(k, k + 1) for k in range(4)] if last else [slice(0, half), slice(half, 2 * half)]
        parts = [keep[c] + got[c] for c in cuts]
        if not last:
            keep, send = parts
    far = [(3, bits[-1] ^ bits[-2]), (1, bits[-1]), (2, bits[-2])]
    others = [lax.ppermute(parts[k], "patch", partner(devices, bit)) for k, bit in far]
    return finish(side, maps, depth, parts[0], others)


def solution(mesh):
    one = P(("group", "patch"))
    in_specs = (P(("group", "patch"), None, None, None), P(), P(), P(), P(), one, one, one)
    return jax.shard_map(
        on_device, mesh=mesh, in_specs=in_specs, out_specs=P(("group", "patch"), None, None), check_vma=False
    )
```

```python
import functools
import math

import numpy as np

import jax
import jax.numpy as jnp
from jax import lax
from jax.experimental import pallas as pl
from jax.experimental.pallas import tpu as pltpu
from jax.sharding import PartitionSpec as P


F32 = jnp.float32
BF16 = jnp.bfloat16
I32 = jnp.int32
PAD = 32
LANES = 128
CHUNKS = 2
LEAD = 1
SPARE = 96


def iota(shape, axis):
    return lax.broadcasted_iota(I32, shape, axis)


def vmem():
    return pl.BlockSpec(memory_space=pltpu.VMEM)


def smem():
    return pl.BlockSpec(memory_space=pltpu.SMEM)


def hbm():
    return pl.BlockSpec(memory_space=pltpu.HBM)


def stay(*arrays):
    return [pltpu.with_memory_space_constraint(a, pltpu.HBM) for a in arrays]


def params():
    return pltpu.CompilerParams(vmem_limit_bytes=16 * 2**20)


def cost(flops):
    return pl.CostEstimate(flops=flops, bytes_accessed=2**20, transcendentals=0)


def bump(length):
    position = (np.arange(length, dtype=np.float64) + 0.5) / length
    return 0.1 + np.sin(np.pi * position) ** 2


def front_kernel(aug_ref, w_in_hbm, w_plane_hbm, w_depth_hbm, w_head_hbm, x_hbm, plane_ref, depth_ref, head_ref, xs_ref, w_in_ref, w_plane_ref, w_depth_ref, w_head_ref, x_ref, big_ref, plane_scr, depth_scr, sems):
    size = x_hbm.shape[2] // CHUNKS
    feats = [
        pltpu.make_async_copy(x_hbm.at[:, :, pl.ds(c * size, size)], x_ref.at[:, :, pl.ds(c * size, size)], sems.at[4 + c])
        for c in range(CHUNKS)
    ]
    pairs = ((w_plane_hbm, w_plane_ref), (w_in_hbm, w_in_ref), (w_depth_hbm, w_depth_ref), (w_head_hbm, w_head_ref))
    copies = [pltpu.make_async_copy(src, dst, sems.at[k]) for k, (src, dst) in enumerate(pairs)]
    for copy in copies + feats:
        copy.start()
    for copy in copies:
        copy.wait()
    hidden, _ = w_in_ref.shape
    depth = depth_ref.shape[0] // PAD
    maps = w_head_ref.shape[0]
    aug = aug_ref[0]
    zf, yf, xf = aug & 1, (aug >> 1) & 1, (aug >> 2) & 1

    rows, cols = big_ref.shape
    spread = (iota((rows, hidden), 0) % PAD == iota((rows, hidden), 1)).astype(BF16)
    gather = (iota((w_in_ref.shape[1], cols), 1) // depth == iota((w_in_ref.shape[1], cols), 0)).astype(BF16)
    tall = jnp.dot(spread, w_in_ref[...], preferred_element_type=F32).astype(BF16)
    wide = jnp.dot(tall, gather, preferred_element_type=F32)
    same = iota((rows, cols), 1) % depth == iota((rows, cols), 0) // PAD
    big_ref[...] = jnp.where(same, wide, 0.0).astype(BF16)

    plane_scr[...] = jnp.zeros_like(plane_scr)
    taps = [w_plane_ref[t].astype(F32) for t in range(9)]
    near = (((0,), (1, 2), ()), ((), (0, 1), (2,)))
    for py in range(2):
        for px in range(2):
            for dy in range(2):
                for dx in range(3):
                    hit = [taps[3 * ty + tx] for ty in near[py][dy + py] for tx in near[px][dx]]
                    if not hit:
                        continue
                    total = functools.reduce(lambda a, b: a + b, hit)
                    high = total.astype(BF16).astype(F32)
                    col = (3 * dy + dx) * PAD
                    plane_scr[py, pl.ds(px * PAD, hidden), pl.ds(col, hidden)] = high
                    plane_scr[py, pl.ds((2 + px) * PAD, hidden), pl.ds(col, hidden)] = total - high
    plane_ref[...] = plane_scr[...].astype(BF16)

    depth_scr[...] = jnp.zeros_like(depth_scr)
    for t in range(3):
        tap = w_depth_ref[t].astype(F32)
        for z in range(depth):
            if 0 <= z + t - 1 < depth:
                depth_scr[pl.ds(z * PAD, hidden), pl.ds((z + t - 1) * PAD, hidden)] = tap
    depth_ref[...] = depth_scr[...].astype(BF16)

    rows, cols = head_ref.shape
    pick = (iota((rows, maps), 0) % maps == iota((rows, maps), 1)).astype(BF16)
    tall = jnp.dot(pick, w_head_ref[...], preferred_element_type=F32).astype(BF16)
    gather = (iota((hidden, cols), 1) % PAD == iota((hidden, cols), 0)).astype(BF16)
    wide = jnp.dot(tall, gather, preferred_element_type=F32)
    at = iota((rows, cols), 0) // maps
    came = iota((rows, cols), 1) // PAD
    flip = (2 * yf + xf) * depth + (depth - 1) * zf
    head_ref[...] = jnp.where(at == (came ^ flip), wide, 0.0).astype(BF16)

    channels, depth, cells = x_ref.shape
    zeros = jnp.zeros((depth * PAD, LANES), BF16)
    xs_ref[:, pl.ds(0, LANES)] = zeros
    xs_ref[:, pl.ds(LANES + cells, LANES)] = zeros
    for c, copy in enumerate(feats):
        part = pl.ds(c * size, size)
        copy.wait()
        x = x_ref[:, :, part].reshape(channels * depth, size)
        xs_ref[:, pl.ds(LANES + c * size, size)] = jnp.dot(big_ref[...], x, preferred_element_type=F32).astype(BF16)


def front(aug_code, w_in, w_plane, w_depth, w_head, feat):
    _, channels = w_in.shape
    maps = w_head.shape[0]
    _, depth, cells = feat.shape
    plane = (2, 4 * PAD, 6 * PAD)
    depth_w = (depth * PAD, depth * PAD)
    head = (4 * depth * maps, 4 * depth * PAD)
    padded = (depth * PAD, cells + 2 * LANES)
    return pl.pallas_call(
        front_kernel,
        out_shape=[jax.ShapeDtypeStruct(s, BF16) for s in (plane, depth_w, head, padded)],
        in_specs=[smem()] + [hbm()] * 5,
        out_specs=[vmem()] * 4,
        scratch_shapes=[
            pltpu.VMEM(w_in.shape, BF16),
            pltpu.VMEM(w_plane.shape, BF16),
            pltpu.VMEM(w_depth.shape, BF16),
            pltpu.VMEM(w_head.shape, BF16),
            pltpu.VMEM(feat.shape, BF16),
            pltpu.VMEM((depth * PAD, channels * depth), BF16),
            pltpu.VMEM(plane, F32),
            pltpu.VMEM(depth_w, F32),
            pltpu.SemaphoreType.DMA((4 + CHUNKS,)),
        ],
        compiler_params=params(),
        cost_estimate=cost(10**8),
        name="front",
    )(aug_code, *stay(w_in, w_plane, w_depth, w_head, feat))


def patch_kernel(half, tiles, brick_rows, keep_from, last, aug_ref, xs_ref, plane_ref, depth_ref, head_ref, *refs):
    if last:
        carry_in, _, anchor_ref, out_ref, anchor_out, a_ref = refs
        anchor_out[...] = jnp.full(anchor_out.shape, anchor_ref[0], I32)
    else:
        out_ref, carry_out, a_ref = refs
    rows, _ = xs_ref.shape
    depth = rows // PAD
    step = 2 * LANES
    margin = LANES
    carried = carry_in.shape[0] if last else 0
    first_tile = tiles[0] * (step // LANES) - carried
    if last:
        a_ref[pl.ds(0, carried)] = carry_in[...]

    def window_stage(t):
        column = (iota((rows, step), 1) + t * step) % half
        block = xs_ref[:, pl.ds(t * step, step + 2 * margin)]
        near = []
        for d in (-1, 0, 1):
            near.append([])
            for e in (-1, 0, 1):
                at = margin + half * e + d
                one = lax.slice_in_dim(block, at, at + step, axis=1)
                if d:
                    one = jnp.where(column == (0 if d < 0 else half - 1), jnp.zeros_like(one), one)
                near[-1].append(one)
        return near

    def plane_stage(near, z):
        cut = slice(z * PAD, (z + 1) * PAD)
        centre = near[1][1][cut].astype(F32)
        first = []
        for py in range(2):
            around = jnp.concatenate([near[d][py + e][cut] for e in range(2) for d in range(3)], axis=0)
            mix = jnp.dot(plane_ref[py], around, preferred_element_type=F32)
            for px in range(2):
                total = mix[px * PAD : (px + 1) * PAD] + mix[(2 + px) * PAD : (3 + px) * PAD]
                first.append((centre + jnp.maximum(total, 0.0)).astype(BF16))
        return first

    def depth_stage(first, p):
        one = jnp.concatenate([first[z][p] for z in range(depth)], axis=0)
        mix = jnp.dot(depth_ref[...], one, preferred_element_type=F32)
        return (one.astype(F32) + jnp.maximum(mix, 0.0)).astype(BF16)

    def head_stage(t, second):
        logits = jnp.zeros((head_ref.shape[0], step), F32)
        for q in range(2):
            pair = jnp.concatenate(second[2 * q : 2 * q + 2], axis=0)
            logits = logits + jnp.dot(head_ref[:, 2 * q * rows : 2 * (q + 1) * rows], pair, preferred_element_type=F32)
        affinity = jax.nn.sigmoid(logits)
        for u in range(step // LANES):
            a_ref[t * (step // LANES) + u - first_tile] = affinity[:, u * LANES : (u + 1) * LANES]

    aug = aug_ref[0]
    yf, xf = (aug >> 1) & 1, (aug >> 2) & 1
    side = half // 4
    tail = side * side - LANES
    row_tiles = head_ref.shape[0] // 8
    lane = iota((8, LANES), 1)
    group = lane // tail
    span = -(-side * half // LANES)
    near_tiles = span - 2

    def source(cell, j, odd):
        y = cell // side
        x = cell - y * side
        y = jnp.where(yf == 1, side - 1 - y, y)
        x = jnp.where(xf == 1, side - 1 - x, x)
        return y * half + side * j + x + odd * (LANES // 2)

    def cut_stage(i, j):
        odd = i % 2
        owned = []
        for k in range(span):
            x = (lane + k * LANES + half - odd * (LANES // 2) % half) % half
            owned.append((x >= side * j) & (x < side * (j + 1)))
        src = source(lane, j, odd)
        main_lane, main_near = src % LANES, src < near_tiles * LANES
        rest_lane = source(LANES + lane % tail, j, odd) % LANES
        base = side * half * i // LANES - first_tile
        brick = (i ^ (3 * yf)) * 4 + (j ^ (3 * xf))
        packed = jnp.zeros((8, LANES), F32)
        for r in range(row_tiles):
            cut = pl.ds(8 * r, 8)
            merged = []
            for tiles_of in (range(near_tiles), range(near_tiles, span)):
                one = a_ref[base + tiles_of[0], cut]
                for k in tiles_of[1:]:
                    one = jnp.where(owned[k], a_ref[base + k, cut], one)
                merged.append(one)
            low = jnp.take_along_axis(merged[0], main_lane, axis=1)
            high = jnp.take_along_axis(merged[1], main_lane, axis=1)
            out_ref[brick, cut] = jnp.where(main_near, low, high)
            rest = jnp.take_along_axis(jnp.where(yf == 1, merged[0], merged[1]), rest_lane, axis=1)
            packed = jnp.where(group == r, rest, packed)
        out_ref[brick, pl.ds(8 * row_tiles, 8)] = packed

    first, second = {}, {}
    waiting = [(i, j) for i in brick_rows for j in range(4)]
    done = first_tile + carried
    for k in range(len(tiles) + 2):
        if k < len(tiles):
            near = window_stage(tiles[k])
            first[k] = []
        second[k - 1] = []
        for q in range(4):
            if k < len(tiles) and q < depth:
                first[k].append(plane_stage(near, q))
            if 0 <= k - 1 < len(tiles):
                second[k - 1].append(depth_stage(first[k - 1], q))
            if waiting and done >= side * half * waiting[0][0] // LANES + span:
                cut_stage(*waiting.pop(0))
        if 0 <= k - 2 < len(tiles):
            head_stage(tiles[k - 2], second[k - 2])
            done += step // LANES
    for left in waiting:
        cut_stage(*left)
    if not last:
        carry_out[...] = a_ref[pl.ds(keep_from - first_tile, done - keep_from)]


def patch_half(half, tiles, brick_rows, keep_from, last, aug_code, shifted, plane, depth_w, head, extra=()):
    kept = head.shape[0]
    carried = extra[0].shape[0] if last else 0
    bricks = jax.ShapeDtypeStruct((16, kept + 8, LANES), F32)
    beside = jax.ShapeDtypeStruct((1, LANES), I32) if last else jax.ShapeDtypeStruct((2 * len(tiles) - keep_from, kept, LANES), F32)
    spaces = [vmem(), vmem(), smem()] if last else []
    return pl.pallas_call(
        functools.partial(patch_kernel, half, tiles, brick_rows, keep_from, last),
        out_shape=[bricks, beside],
        in_specs=[smem()] + [vmem()] * 4 + spaces,
        out_specs=[vmem()] * 2,
        scratch_shapes=[pltpu.VMEM((2 * len(tiles) + carried, kept, LANES), F32)],
        input_output_aliases={6: 0} if last else {},
        compiler_params=params(),
        cost_estimate=cost(10**9),
    )(aug_code, shifted, plane, depth_w, head, *extra)


def seed_kernel(owner_ref, out_ref):
    here = iota(out_ref.shape, 1) == lax.axis_index("patch")
    out_ref[...] = jnp.where(here, owner_ref[0], 0)


def seed_table(owner, devices):
    width = -(-devices // LANES) * LANES
    return pl.pallas_call(
        seed_kernel,
        out_shape=jax.ShapeDtypeStruct((1, width), I32),
        in_specs=[smem()],
        out_specs=vmem(),
        compiler_params=params(),
        name="seed",
    )(owner)


def partner(devices, bit):
    return [(d, d ^ bit) for d in range(devices)]


def slots_kernel(devices, bits, table_ref, anchor_ref, mine_ref, other_ref, window_ref, send_ref, keep_ref):
    me = lax.axis_index("patch")
    brick_rows = devices // 4
    brick = iota(table_ref.shape, 1)
    row = lax.rem(brick // 4 - anchor_ref[:, :1] + brick_rows, jnp.full_like(brick, brick_rows))
    place = row * 4 + brick % 4
    owner = jnp.where(brick < devices, table_ref[...], -1)
    count = 1 << len(bits)
    _, rows, lanes = mine_ref.shape
    spare = iota((rows, lanes), 1) - jnp.where(iota((rows, lanes), 0) == rows - 8, SPARE, lanes)
    places = []
    for s in range(count):
        mask = functools.reduce(lambda a, b: a ^ b, [bit for k, bit in enumerate(bits) if s >> (len(bits) - 1 - k) & 1], 0)
        places.append(jnp.sum(jnp.where(owner == (me ^ mask), place, 0)))
    for s, at in enumerate(places):
        covered = at < 16
        slot = at if brick_rows <= 4 else jnp.where(covered, at, 0)
        value = (mine_ref[slot] + other_ref[slot]) * window_ref[slot]
        value = jnp.where(spare == at // 4, 2.0, value)
        value = jnp.where(spare == 4, 2.0 * (at % 4).astype(F32), value)
        if brick_rows > 4:
            value = jnp.where(covered, value, 0.0)
        if s < count // 2:
            keep_ref[s] = value
        else:
            send_ref[s - count // 2] = value


def fill_slots(devices, bits, table, anchor, mine, other, window):
    shape = jax.ShapeDtypeStruct((1 << (len(bits) - 1),) + mine.shape[1:], F32)
    return pl.pallas_call(
        functools.partial(slots_kernel, devices, bits),
        out_shape=[shape, shape],
        in_specs=[vmem()] * 5,
        out_specs=[vmem()] * 2,
        compiler_params=params(),
        name="slots",
    )(table, anchor, mine, other, window)


def brick_kernel(side, maps, depth_curve, mine_ref, a_ref, b_ref, c_ref, rows_ref, cols_ref, out_ref):
    depth = len(depth_curve)
    wide = 2 * side
    plane = wide * wide
    tail = side * side - LANES
    per = depth * maps
    brick = (mine_ref[0] + a_ref[0]) + (b_ref[0] + c_ref[0])
    kept = 4 * per
    main, packed = brick[:kept], brick[kept:]
    rest = jnp.concatenate([packed if k == 0 else pltpu.roll(packed, LANES - tail * k, 1) for k in range(kept // 8)], axis=0)
    fill = jnp.zeros((16 - per, LANES), F32)
    mains = [jnp.concatenate([main[per * p : per * (p + 1)], fill], axis=0) for p in range(4)]
    rests = [jnp.concatenate([rest[per * p : per * (p + 1)], fill], axis=0) for p in range(4)]
    columns = []
    for d in range(-(-plane // LANES)):
        n = iota((8, LANES), 1) + d * LANES
        y = n // wide
        x = n - y * wide
        cell = (y // 2) * side + x // 2
        quarter = 2 * (y % 2) + x % 2
        lane_of = cell % LANES
        top = min((d + 1) * LANES, plane) - 1
        tiles = []
        for r in range(2):
            cut = slice(8 * r, 8 * r + 8)
            value = None
            for p in range(4):
                one = jnp.take_along_axis(mains[p][cut], lane_of, axis=1)
                if (top // wide // 2 + 1) * side > LANES:
                    one = jnp.where(cell >= LANES, jnp.take_along_axis(rests[p][cut], lane_of, axis=1), one)
                value = one if value is None else jnp.where(quarter == p, one, value)
            tiles.append(value)
        columns.append(jnp.concatenate(tiles, axis=0))
    cells = jnp.concatenate(columns, axis=1)[:, :plane]
    for z in range(depth):
        out_ref[0, pl.ds(0, maps), pl.ds(z * plane, plane)] = cells[z * maps : (z + 1) * maps]

    def noted(k):
        lane = jnp.take_along_axis(packed, jnp.full((8, LANES), SPARE + k, I32), axis=1)[0:1]
        return jnp.concatenate([lane] * (rows_ref.shape[1] // LANES), axis=1)

    counts = [noted(i) for i in range(4)]
    added = counts[0] + counts[1] + counts[2] + counts[3]
    column = noted(4)
    down = sum(counts[i] * rows_ref[pl.ds(i, 1), :] for i in range(4))
    across = sum(jnp.where(column == j * added, cols_ref[pl.ds(j, 1), :], 0.0) for j in range(4))
    window = (down * across)[:, :plane]
    for z in range(depth):
        out_ref[0, pl.ds(maps, 1), pl.ds(z * plane, plane)] = window * depth_curve[z]


def finish(side, maps, depth, mine, others):
    plane = 4 * side * side
    width = -(-plane // LANES) * LANES
    curve = bump(8 * side)
    n = np.arange(width)
    y, x = np.minimum(n // (2 * side), 2 * side - 1), n % (2 * side)
    rows = np.stack([curve[2 * side * i + y] for i in range(4)]).astype(np.float32)
    cols = np.stack([curve[2 * side * i + x] for i in range(4)]).astype(np.float32)
    depth_curve = [float(np.float32(v)) for v in bump(depth)]
    return pl.pallas_call(
        functools.partial(brick_kernel, side, maps, depth_curve),
        out_shape=jax.ShapeDtypeStruct((1, maps + 1, depth * plane), F32),
        in_specs=[vmem()] * 6,
        out_specs=vmem(),
        compiler_params=params(),
        name="brick",
    )(mine, *others, rows, cols)


def wire_window(side, maps, depth):
    curve_y, curve_z = bump(8 * side), bump(depth)
    cell = np.arange(side * side)
    out = np.zeros((16, 4 * depth * maps, side * side))
    for i in range(4):
        for j in range(4):
            for p in range(4):
                y = curve_y[2 * side * i + 2 * (cell // side) + p // 2]
                x = curve_y[2 * side * j + 2 * (cell % side) + p % 2]
                for z in range(depth):
                    for m in range(maps):
                        out[4 * i + j, (p * depth + z) * maps + m] = curve_z[z] * y * x
    kept = out.shape[1]
    tail = side * side - LANES
    packed = np.zeros((16, 8, LANES))
    for k in range(kept // 8):
        packed[:, :, tail * k : tail * (k + 1)] = out[:, 8 * k : 8 * k + 8, LANES:]
    return np.concatenate([out[:, :, :LANES], packed], axis=1).astype(np.float32)


def on_device(features, w_in, w_plane, w_depth, w_head, brick_owner, patch_anchor, aug_code):
    devices = lax.axis_size("patch")
    _, _, depth, cells = features.shape
    side = math.isqrt(cells) // 4
    maps = w_head.shape[0]
    levels = [1 << k for k in range(devices.bit_length() - 1)]
    paired = levels[:1] + [bit | 1 for bit in levels[1:]]
    bits = paired[1:-1] + [levels[-1]]

    def table_round(k, table):
        return table + lax.ppermute(table, "patch", partner(devices, rounds[k]))

    rounds = paired
    table = seed_table(brick_owner, devices)
    for k in range(len(rounds)):
        table = table_round(k, table)
    plane, depth_w, head, shifted = front(aug_code, w_in, w_plane, w_depth, w_head, features[0])
    half = math.isqrt(cells)
    steps = cells // (2 * LANES)
    ready = -(-half * half // 2 // (2 * LANES)) + LEAD
    starts = [half * half * i // 4 // LANES for i in range(4)]
    span = -(-half * half // 4 // LANES)
    early = [i for i in range(4) if starts[i] + span < 2 * ready]
    late = [i for i in range(4) if i not in early]
    bricks, carry = patch_half(half, range(ready), early, starts[late[0]], False, aug_code, shifted, plane, depth_w, head)
    bricks, anchor = patch_half(
        half, range(ready, steps), late, 0, True, aug_code, shifted, plane, depth_w, head, (carry, bricks, patch_anchor)
    )
    other = lax.ppermute(bricks, "patch", partner(devices, 1))
    send, keep = fill_slots(devices, bits, table, anchor, bricks, other, wire_window(side, maps, depth))
    for bit in bits[:-2]:
        got = lax.ppermute(send, "patch", partner(devices, bit))
        half = send.shape[0] // 2
        last = half == 2
        cuts = [slice(k, k + 1) for k in range(4)] if last else [slice(0, half), slice(half, 2 * half)]
        parts = [keep[c] + got[c] for c in cuts]
        if not last:
            keep, send = parts
    far = [(3, bits[-1] ^ bits[-2]), (1, bits[-1]), (2, bits[-2])]
    others = [lax.ppermute(parts[k], "patch", partner(devices, bit)) for k, bit in far]
    return finish(side, maps, depth, parts[0], others)


def solution(mesh):
    one = P(("group", "patch"))
    in_specs = (P(("group", "patch"), None, None, None), P(), P(), P(), P(), one, one, one)
    return jax.shard_map(
        on_device, mesh=mesh, in_specs=in_specs, out_specs=P(("group", "patch"), None, None), check_vma=False
    )
```

```python
import functools
import math

import numpy as np

import jax
import jax.numpy as jnp
from jax import lax
from jax.experimental import pallas as pl
from jax.experimental.pallas import tpu as pltpu
from jax.sharding import PartitionSpec as P


F32 = jnp.float32
BF16 = jnp.bfloat16
I32 = jnp.int32
PAD = 32
LANES = 128
CHUNKS = 2
FAR_FIRST = (3, 2, 1)
DIRECT = 2
LEAD = 1
SPARE = 96


def iota(shape, axis):
    return lax.broadcasted_iota(I32, shape, axis)


def vmem():
    return pl.BlockSpec(memory_space=pltpu.VMEM)


def smem():
    return pl.BlockSpec(memory_space=pltpu.SMEM)


def hbm():
    return pl.BlockSpec(memory_space=pltpu.HBM)


def stay(*arrays):
    return [pltpu.with_memory_space_constraint(a, pltpu.HBM) for a in arrays]


def params():
    return pltpu.CompilerParams(vmem_limit_bytes=16 * 2**20)


def cost(flops):
    return pl.CostEstimate(flops=flops, bytes_accessed=2**20, transcendentals=0)


def bump(length):
    position = (np.arange(length, dtype=np.float64) + 0.5) / length
    return 0.1 + np.sin(np.pi * position) ** 2


def front_kernel(aug_ref, w_in_hbm, w_plane_hbm, w_depth_hbm, w_head_hbm, x_hbm, plane_ref, depth_ref, head_ref, xs_ref, w_in_ref, w_plane_ref, w_depth_ref, w_head_ref, x_ref, big_ref, plane_scr, depth_scr, sems):
    size = x_hbm.shape[2] // CHUNKS
    feats = [
        pltpu.make_async_copy(x_hbm.at[:, :, pl.ds(c * size, size)], x_ref.at[:, :, pl.ds(c * size, size)], sems.at[4 + c])
        for c in range(CHUNKS)
    ]
    pairs = ((w_plane_hbm, w_plane_ref), (w_in_hbm, w_in_ref), (w_depth_hbm, w_depth_ref), (w_head_hbm, w_head_ref))
    copies = [pltpu.make_async_copy(src, dst, sems.at[k]) for k, (src, dst) in enumerate(pairs)]
    for copy in copies + feats:
        copy.start()
    for copy in copies:
        copy.wait()
    hidden, _ = w_in_ref.shape
    depth = depth_ref.shape[0] // PAD
    maps = w_head_ref.shape[0]
    aug = aug_ref[0]
    zf, yf, xf = aug & 1, (aug >> 1) & 1, (aug >> 2) & 1

    rows, cols = big_ref.shape
    spread = (iota((rows, hidden), 0) % PAD == iota((rows, hidden), 1)).astype(BF16)
    gather = (iota((w_in_ref.shape[1], cols), 1) // depth == iota((w_in_ref.shape[1], cols), 0)).astype(BF16)
    tall = jnp.dot(spread, w_in_ref[...], preferred_element_type=F32).astype(BF16)
    wide = jnp.dot(tall, gather, preferred_element_type=F32)
    same = iota((rows, cols), 1) % depth == iota((rows, cols), 0) // PAD
    big_ref[...] = jnp.where(same, wide, 0.0).astype(BF16)

    plane_scr[...] = jnp.zeros_like(plane_scr)
    taps = [w_plane_ref[t].astype(F32) for t in range(9)]
    near = (((0,), (1, 2), ()), ((), (0, 1), (2,)))
    for py in range(2):
        for px in range(2):
            for dy in range(2):
                for dx in range(3):
                    hit = [taps[3 * ty + tx] for ty in near[py][dy + py] for tx in near[px][dx]]
                    if not hit:
                        continue
                    total = functools.reduce(lambda a, b: a + b, hit)
                    high = total.astype(BF16).astype(F32)
                    col = (3 * dy + dx) * PAD
                    plane_scr[py, pl.ds(px * PAD, hidden), pl.ds(col, hidden)] = high
                    plane_scr[py, pl.ds((2 + px) * PAD, hidden), pl.ds(col, hidden)] = total - high
    plane_ref[...] = plane_scr[...].astype(BF16)

    depth_scr[...] = jnp.zeros_like(depth_scr)
    for t in range(3):
        tap = w_depth_ref[t].astype(F32)
        for z in range(depth):
            if 0 <= z + t - 1 < depth:
                depth_scr[pl.ds(z * PAD, hidden), pl.ds((z + t - 1) * PAD, hidden)] = tap
    depth_ref[...] = depth_scr[...].astype(BF16)

    rows, cols = head_ref.shape
    pick = (iota((rows, maps), 0) % maps == iota((rows, maps), 1)).astype(BF16)
    tall = jnp.dot(pick, w_head_ref[...], preferred_element_type=F32).astype(BF16)
    gather = (iota((hidden, cols), 1) % PAD == iota((hidden, cols), 0)).astype(BF16)
    wide = jnp.dot(tall, gather, preferred_element_type=F32)
    at = iota((rows, cols), 0) // maps
    came = iota((rows, cols), 1) // PAD
    flip = (2 * yf + xf) * depth + (depth - 1) * zf
    head_ref[...] = jnp.where(at == (came ^ flip), wide, 0.0).astype(BF16)

    channels, depth, cells = x_ref.shape
    zeros = jnp.zeros((depth * PAD, LANES), BF16)
    xs_ref[:, pl.ds(0, LANES)] = zeros
    xs_ref[:, pl.ds(LANES + cells, LANES)] = zeros
    for c, copy in enumerate(feats):
        part = pl.ds(c * size, size)
        copy.wait()
        x = x_ref[:, :, part].reshape(channels * depth, size)
        xs_ref[:, pl.ds(LANES + c * size, size)] = jnp.dot(big_ref[...], x, preferred_element_type=F32).astype(BF16)


def front(aug_code, w_in, w_plane, w_depth, w_head, feat):
    _, channels = w_in.shape
    maps = w_head.shape[0]
    _, depth, cells = feat.shape
    plane = (2, 4 * PAD, 6 * PAD)
    depth_w = (depth * PAD, depth * PAD)
    head = (4 * depth * maps, 4 * depth * PAD)
    padded = (depth * PAD, cells + 2 * LANES)
    return pl.pallas_call(
        front_kernel,
        out_shape=[jax.ShapeDtypeStruct(s, BF16) for s in (plane, depth_w, head, padded)],
        in_specs=[smem()] + [hbm()] * 5,
        out_specs=[vmem()] * 4,
        scratch_shapes=[
            pltpu.VMEM(w_in.shape, BF16),
            pltpu.VMEM(w_plane.shape, BF16),
            pltpu.VMEM(w_depth.shape, BF16),
            pltpu.VMEM(w_head.shape, BF16),
            pltpu.VMEM(feat.shape, BF16),
            pltpu.VMEM((depth * PAD, channels * depth), BF16),
            pltpu.VMEM(plane, F32),
            pltpu.VMEM(depth_w, F32),
            pltpu.SemaphoreType.DMA((4 + CHUNKS,)),
        ],
        compiler_params=params(),
        cost_estimate=cost(10**8),
        name="front",
    )(aug_code, *stay(w_in, w_plane, w_depth, w_head, feat))


def patch_kernel(half, tiles, brick_rows, keep_from, last, aug_ref, xs_ref, plane_ref, depth_ref, head_ref, *refs):
    if last:
        carry_in, _, anchor_ref, out_ref, anchor_out, a_ref = refs
        anchor_out[...] = jnp.full(anchor_out.shape, anchor_ref[0], I32)
    else:
        out_ref, carry_out, a_ref = refs
    rows, _ = xs_ref.shape
    depth = rows // PAD
    step = 2 * LANES
    margin = LANES
    carried = carry_in.shape[0] if last else 0
    first_tile = tiles[0] * (step // LANES) - carried
    if last:
        a_ref[pl.ds(0, carried)] = carry_in[...]

    def window_stage(t):
        column = (iota((rows, step), 1) + t * step) % half
        block = xs_ref[:, pl.ds(t * step, step + 2 * margin)]
        near = []
        for d in (-1, 0, 1):
            near.append([])
            for e in (-1, 0, 1):
                at = margin + half * e + d
                one = lax.slice_in_dim(block, at, at + step, axis=1)
                if d:
                    one = jnp.where(column == (0 if d < 0 else half - 1), jnp.zeros_like(one), one)
                near[-1].append(one)
        return near

    def plane_stage(near, z):
        cut = slice(z * PAD, (z + 1) * PAD)
        centre = near[1][1][cut].astype(F32)
        first = []
        for py in range(2):
            around = jnp.concatenate([near[d][py + e][cut] for e in range(2) for d in range(3)], axis=0)
            mix = jnp.dot(plane_ref[py], around, preferred_element_type=F32)
            for px in range(2):
                total = mix[px * PAD : (px + 1) * PAD] + mix[(2 + px) * PAD : (3 + px) * PAD]
                first.append((centre + jnp.maximum(total, 0.0)).astype(BF16))
        return first

    def depth_stage(first, p):
        one = jnp.concatenate([first[z][p] for z in range(depth)], axis=0)
        mix = jnp.dot(depth_ref[...], one, preferred_element_type=F32)
        return (one.astype(F32) + jnp.maximum(mix, 0.0)).astype(BF16)

    def head_stage(t, second):
        logits = jnp.zeros((head_ref.shape[0], step), F32)
        for q in range(2):
            pair = jnp.concatenate(second[2 * q : 2 * q + 2], axis=0)
            logits = logits + jnp.dot(head_ref[:, 2 * q * rows : 2 * (q + 1) * rows], pair, preferred_element_type=F32)
        affinity = jax.nn.sigmoid(logits)
        for u in range(step // LANES):
            a_ref[t * (step // LANES) + u - first_tile] = affinity[:, u * LANES : (u + 1) * LANES]

    aug = aug_ref[0]
    yf, xf = (aug >> 1) & 1, (aug >> 2) & 1
    side = half // 4
    tail = side * side - LANES
    row_tiles = head_ref.shape[0] // 8
    lane = iota((8, LANES), 1)
    group = lane // tail
    span = -(-side * half // LANES)
    near_tiles = span - 2

    def source(cell, j, odd):
        y = cell // side
        x = cell - y * side
        y = jnp.where(yf == 1, side - 1 - y, y)
        x = jnp.where(xf == 1, side - 1 - x, x)
        return y * half + side * j + x + odd * (LANES // 2)

    def cut_stage(i, j):
        odd = i % 2
        owned = []
        for k in range(span):
            x = (lane + k * LANES + half - odd * (LANES // 2) % half) % half
            owned.append((x >= side * j) & (x < side * (j + 1)))
        src = source(lane, j, odd)
        main_lane, main_near = src % LANES, src < near_tiles * LANES
        rest_lane = source(LANES + lane % tail, j, odd) % LANES
        base = side * half * i // LANES - first_tile
        brick = (i ^ (3 * yf)) * 4 + (j ^ (3 * xf))
        packed = jnp.zeros((8, LANES), F32)
        for r in range(row_tiles):
            cut = pl.ds(8 * r, 8)
            merged = []
            for tiles_of in (range(near_tiles), range(near_tiles, span)):
                one = a_ref[base + tiles_of[0], cut]
                for k in tiles_of[1:]:
                    one = jnp.where(owned[k], a_ref[base + k, cut], one)
                merged.append(one)
            low = jnp.take_along_axis(merged[0], main_lane, axis=1)
            high = jnp.take_along_axis(merged[1], main_lane, axis=1)
            out_ref[brick, cut] = jnp.where(main_near, low, high)
            rest = jnp.take_along_axis(jnp.where(yf == 1, merged[0], merged[1]), rest_lane, axis=1)
            packed = jnp.where(group == r, rest, packed)
        out_ref[brick, pl.ds(8 * row_tiles, 8)] = packed

    first, second = {}, {}
    waiting = [(i, j) for i in brick_rows for j in range(4)]
    done = first_tile + carried
    for k in range(len(tiles) + 2):
        if k < len(tiles):
            near = window_stage(tiles[k])
            first[k] = []
        second[k - 1] = []
        for q in range(4):
            if k < len(tiles) and q < depth:
                first[k].append(plane_stage(near, q))
            if 0 <= k - 1 < len(tiles):
                second[k - 1].append(depth_stage(first[k - 1], q))
            if waiting and done >= side * half * waiting[0][0] // LANES + span:
                cut_stage(*waiting.pop(0))
        if 0 <= k - 2 < len(tiles):
            head_stage(tiles[k - 2], second[k - 2])
            done += step // LANES
    for left in waiting:
        cut_stage(*left)
    if not last:
        carry_out[...] = a_ref[pl.ds(keep_from - first_tile, done - keep_from)]


def patch_half(half, tiles, brick_rows, keep_from, last, aug_code, shifted, plane, depth_w, head, extra=()):
    kept = head.shape[0]
    carried = extra[0].shape[0] if last else 0
    bricks = jax.ShapeDtypeStruct((16, kept + 8, LANES), F32)
    beside = jax.ShapeDtypeStruct((1, LANES), I32) if last else jax.ShapeDtypeStruct((2 * len(tiles) - keep_from, kept, LANES), F32)
    spaces = [vmem(), vmem(), smem()] if last else []
    return pl.pallas_call(
        functools.partial(patch_kernel, half, tiles, brick_rows, keep_from, last),
        out_shape=[bricks, beside],
        in_specs=[smem()] + [vmem()] * 4 + spaces,
        out_specs=[vmem()] * 2,
        scratch_shapes=[pltpu.VMEM((2 * len(tiles) + carried, kept, LANES), F32)],
        input_output_aliases={6: 0} if last else {},
        compiler_params=params(),
        cost_estimate=cost(10**9),
    )(aug_code, shifted, plane, depth_w, head, *extra)


def seed_kernel(owner_ref, out_ref):
    here = iota(out_ref.shape, 1) == lax.axis_index("patch")
    out_ref[...] = jnp.where(here, owner_ref[0], 0)


def seed_table(owner, devices):
    width = -(-devices // LANES) * LANES
    return pl.pallas_call(
        seed_kernel,
        out_shape=jax.ShapeDtypeStruct((1, width), I32),
        in_specs=[smem()],
        out_specs=vmem(),
        compiler_params=params(),
        name="seed",
    )(owner)


def partner(devices, bit):
    return [(d, d ^ bit) for d in range(devices)]


def slots_kernel(devices, masks, table_ref, anchor_ref, mine_ref, other_ref, window_ref, *outs):
    me = lax.axis_index("patch")
    brick_rows = devices // 4
    brick = iota(table_ref.shape, 1)
    row = lax.rem(brick // 4 - anchor_ref[:, :1] + brick_rows, jnp.full_like(brick, brick_rows))
    place = row * 4 + brick % 4
    owner = jnp.where(brick < devices, table_ref[...], -1)
    _, rows, lanes = mine_ref.shape
    spare = iota((rows, lanes), 1) - jnp.where(iota((rows, lanes), 0) == rows - 8, SPARE, lanes)
    places = [jnp.sum(jnp.where(owner == (me ^ mask), place, 0)) for mask in masks]
    size = outs[0].shape[0]
    for s, at in enumerate(places):
        covered = at < 16
        slot = at if brick_rows <= 4 else jnp.where(covered, at, 0)
        value = (mine_ref[slot] + other_ref[slot]) * window_ref[slot]
        value = jnp.where(spare == at // 4, 2.0, value)
        value = jnp.where(spare == 4, 2.0 * (at % 4).astype(F32), value)
        if brick_rows > 4:
            value = jnp.where(covered, value, 0.0)
        outs[s // size][s % size] = value


def fill_slots(devices, masks, pieces, table, anchor, mine, other, window):
    shape = jax.ShapeDtypeStruct((len(masks) // pieces,) + mine.shape[1:], F32)
    return pl.pallas_call(
        functools.partial(slots_kernel, devices, masks),
        out_shape=[shape] * pieces,
        in_specs=[vmem()] * 5,
        out_specs=[vmem()] * pieces,
        compiler_params=params(),
        name="slots",
    )(table, anchor, mine, other, window)


def brick_kernel(side, maps, depth_curve, mine_ref, *refs):
    *others, rows_ref, cols_ref, out_ref = refs
    depth = len(depth_curve)
    wide = 2 * side
    plane = wide * wide
    tail = side * side - LANES
    per = depth * maps
    brick = mine_ref[0]
    for other in others:
        brick = brick + other[0]
    kept = 4 * per
    main, packed = brick[:kept], brick[kept:]
    rest = jnp.concatenate([packed if k == 0 else pltpu.roll(packed, LANES - tail * k, 1) for k in range(kept // 8)], axis=0)
    fill = jnp.zeros((16 - per, LANES), F32)
    mains = [jnp.concatenate([main[per * p : per * (p + 1)], fill], axis=0) for p in range(4)]
    rests = [jnp.concatenate([rest[per * p : per * (p + 1)], fill], axis=0) for p in range(4)]
    columns = []
    for d in range(-(-plane // LANES)):
        n = iota((8, LANES), 1) + d * LANES
        y = n // wide
        x = n - y * wide
        cell = (y // 2) * side + x // 2
        quarter = 2 * (y % 2) + x % 2
        lane_of = cell % LANES
        top = min((d + 1) * LANES, plane) - 1
        tiles = []
        for r in range(2):
            cut = slice(8 * r, 8 * r + 8)
            value = None
            for p in range(4):
                one = jnp.take_along_axis(mains[p][cut], lane_of, axis=1)
                if (top // wide // 2 + 1) * side > LANES:
                    one = jnp.where(cell >= LANES, jnp.take_along_axis(rests[p][cut], lane_of, axis=1), one)
                value = one if value is None else jnp.where(quarter == p, one, value)
            tiles.append(value)
        columns.append(jnp.concatenate(tiles, axis=0))
    cells = jnp.concatenate(columns, axis=1)[:, :plane]
    for z in range(depth):
        out_ref[0, pl.ds(0, maps), pl.ds(z * plane, plane)] = cells[z * maps : (z + 1) * maps]

    def noted(k):
        lane = jnp.take_along_axis(packed, jnp.full((8, LANES), SPARE + k, I32), axis=1)[0:1]
        return jnp.concatenate([lane] * (rows_ref.shape[1] // LANES), axis=1)

    counts = [noted(i) for i in range(4)]
    added = counts[0] + counts[1] + counts[2] + counts[3]
    column = noted(4)
    down = sum(counts[i] * rows_ref[pl.ds(i, 1), :] for i in range(4))
    across = sum(jnp.where(column == j * added, cols_ref[pl.ds(j, 1), :], 0.0) for j in range(4))
    window = (down * across)[:, :plane]
    for z in range(depth):
        out_ref[0, pl.ds(maps, 1), pl.ds(z * plane, plane)] = window * depth_curve[z]


def finish(side, maps, depth, mine, others):
    plane = 4 * side * side
    width = -(-plane // LANES) * LANES
    curve = bump(8 * side)
    n = np.arange(width)
    y, x = np.minimum(n // (2 * side), 2 * side - 1), n % (2 * side)
    rows = np.stack([curve[2 * side * i + y] for i in range(4)]).astype(np.float32)
    cols = np.stack([curve[2 * side * i + x] for i in range(4)]).astype(np.float32)
    depth_curve = [float(np.float32(v)) for v in bump(depth)]
    return pl.pallas_call(
        functools.partial(brick_kernel, side, maps, depth_curve),
        out_shape=jax.ShapeDtypeStruct((1, maps + 1, depth * plane), F32),
        in_specs=[vmem()] * (len(others) + 3),
        out_specs=vmem(),
        compiler_params=params(),
        name="brick",
    )(mine, *others, rows, cols)


def wire_window(side, maps, depth):
    curve_y, curve_z = bump(8 * side), bump(depth)
    cell = np.arange(side * side)
    out = np.zeros((16, 4 * depth * maps, side * side))
    for i in range(4):
        for j in range(4):
            for p in range(4):
                y = curve_y[2 * side * i + 2 * (cell // side) + p // 2]
                x = curve_y[2 * side * j + 2 * (cell % side) + p % 2]
                for z in range(depth):
                    for m in range(maps):
                        out[4 * i + j, (p * depth + z) * maps + m] = curve_z[z] * y * x
    kept = out.shape[1]
    tail = side * side - LANES
    packed = np.zeros((16, 8, LANES))
    for k in range(kept // 8):
        packed[:, :, tail * k : tail * (k + 1)] = out[:, 8 * k : 8 * k + 8, LANES:]
    return np.concatenate([out[:, :, :LANES], packed], axis=1).astype(np.float32)


def on_device(features, w_in, w_plane, w_depth, w_head, brick_owner, patch_anchor, aug_code):
    devices = lax.axis_size("patch")
    _, _, depth, cells = features.shape
    side = math.isqrt(cells) // 4
    maps = w_head.shape[0]
    levels = [1 << k for k in range(devices.bit_length() - 1)]
    paired = levels[:1] + [bit | 1 for bit in levels[1:]]
    halved = paired[1:-DIRECT]
    direct = [sum(bit for k, bit in enumerate(levels[-DIRECT:]) if q >> k & 1) | min(q, 1) for q in range(1 << DIRECT)]
    masks = [0]
    for bit in reversed(halved):
        masks = masks + [bit ^ mask for mask in masks]
    masks = [mask ^ last for mask in masks for last in direct]

    def table_round(k, table):
        return table + lax.ppermute(table, "patch", partner(devices, rounds[k]))

    rounds = paired
    table = seed_table(brick_owner, devices)
    for k in range(len(rounds)):
        table = table_round(k, table)
    plane, depth_w, head, shifted = front(aug_code, w_in, w_plane, w_depth, w_head, features[0])
    half = math.isqrt(cells)
    steps = cells // (2 * LANES)
    ready = -(-half * half // 2 // (2 * LANES)) + LEAD
    starts = [half * half * i // 4 // LANES for i in range(4)]
    span = -(-half * half // 4 // LANES)
    early = [i for i in range(4) if starts[i] + span < 2 * ready]
    late = [i for i in range(4) if i not in early]
    bricks, carry = patch_half(half, range(ready), early, starts[late[0]], False, aug_code, shifted, plane, depth_w, head)
    bricks, anchor = patch_half(
        half, range(ready, steps), late, 0, True, aug_code, shifted, plane, depth_w, head, (carry, bricks, patch_anchor)
    )
    other = lax.ppermute(bricks, "patch", partner(devices, 1))
    pieces = 2 if halved else len(direct)
    parts = fill_slots(devices, masks, pieces, table, anchor, bricks, other, wire_window(side, maps, depth))
    for k, bit in enumerate(halved):
        keep, send = parts
        got = lax.ppermute(send, "patch", partner(devices, bit))
        size = send.shape[0] // 2 if k + 1 < len(halved) else 1
        parts = [keep[i : i + size] + got[i : i + size] for i in range(0, send.shape[0], size)]
    others = [lax.ppermute(parts[q], "patch", partner(devices, direct[q])) for q in FAR_FIRST]
    return finish(side, maps, depth, parts[0], others)


def solution(mesh):
    one = P(("group", "patch"))
    in_specs = (P(("group", "patch"), None, None, None), P(), P(), P(), P(), one, one, one)
    return jax.shard_map(
        on_device, mesh=mesh, in_specs=in_specs, out_specs=P(("group", "patch"), None, None), check_vma=False
    )
```

```python
import functools
import math

import numpy as np

import jax
import jax.numpy as jnp
from jax import lax
from jax.experimental import pallas as pl
from jax.experimental.pallas import tpu as pltpu
from jax.sharding import PartitionSpec as P


F32 = jnp.float32
BF16 = jnp.bfloat16
I32 = jnp.int32
PAD = 32
LANES = 128
CHUNKS = 2
FAR_FIRST = (3, 2, 1)
DIRECT = 2
LEAD = 1
SPARE = 96


def iota(shape, axis):
    return lax.broadcasted_iota(I32, shape, axis)


def vmem():
    return pl.BlockSpec(memory_space=pltpu.VMEM)


def smem():
    return pl.BlockSpec(memory_space=pltpu.SMEM)


def hbm():
    return pl.BlockSpec(memory_space=pltpu.HBM)


def stay(*arrays):
    return [pltpu.with_memory_space_constraint(a, pltpu.HBM) for a in arrays]


def params():
    return pltpu.CompilerParams(vmem_limit_bytes=16 * 2**20)


def cost(flops):
    return pl.CostEstimate(flops=flops, bytes_accessed=2**20, transcendentals=0)


def bump(length):
    position = (np.arange(length, dtype=np.float64) + 0.5) / length
    return 0.1 + np.sin(np.pi * position) ** 2


def front_kernel(aug_ref, w_in_hbm, w_plane_hbm, w_depth_hbm, w_head_hbm, x_hbm, plane_ref, depth_ref, head_ref, xs_ref, w_in_ref, w_plane_ref, w_depth_ref, w_head_ref, x_ref, big_ref, plane_scr, depth_scr, sems):
    size = x_hbm.shape[2] // CHUNKS
    feats = [
        pltpu.make_async_copy(x_hbm.at[:, :, pl.ds(c * size, size)], x_ref.at[:, :, pl.ds(c * size, size)], sems.at[4 + c])
        for c in range(CHUNKS)
    ]
    pairs = ((w_plane_hbm, w_plane_ref), (w_in_hbm, w_in_ref), (w_depth_hbm, w_depth_ref), (w_head_hbm, w_head_ref))
    copies = [pltpu.make_async_copy(src, dst, sems.at[k]) for k, (src, dst) in enumerate(pairs)]
    for copy in copies + feats:
        copy.start()
    for copy in copies:
        copy.wait()
    hidden, _ = w_in_ref.shape
    depth = depth_ref.shape[0] // PAD
    maps = w_head_ref.shape[0]
    aug = aug_ref[0]
    zf, yf, xf = aug & 1, (aug >> 1) & 1, (aug >> 2) & 1

    rows, cols = big_ref.shape
    spread = (iota((rows, hidden), 0) % PAD == iota((rows, hidden), 1)).astype(BF16)
    gather = (iota((w_in_ref.shape[1], cols), 1) // depth == iota((w_in_ref.shape[1], cols), 0)).astype(BF16)
    tall = jnp.dot(spread, w_in_ref[...], preferred_element_type=F32).astype(BF16)
    wide = jnp.dot(tall, gather, preferred_element_type=F32)
    same = iota((rows, cols), 1) % depth == iota((rows, cols), 0) // PAD
    big_ref[...] = jnp.where(same, wide, 0.0).astype(BF16)

    plane_scr[...] = jnp.zeros_like(plane_scr)
    taps = [w_plane_ref[t].astype(F32) for t in range(9)]
    near = (((0,), (1, 2), ()), ((), (0, 1), (2,)))
    for py in range(2):
        for px in range(2):
            for dy in range(2):
                for dx in range(3):
                    hit = [taps[3 * ty + tx] for ty in near[py][dy + py] for tx in near[px][dx]]
                    if not hit:
                        continue
                    total = functools.reduce(lambda a, b: a + b, hit)
                    high = total.astype(BF16).astype(F32)
                    col = (3 * dy + dx) * PAD
                    plane_scr[py, pl.ds(px * PAD, hidden), pl.ds(col, hidden)] = high
                    plane_scr[py, pl.ds((2 + px) * PAD, hidden), pl.ds(col, hidden)] = total - high
    plane_ref[...] = plane_scr[...].astype(BF16)

    depth_scr[...] = jnp.zeros_like(depth_scr)
    for t in range(3):
        tap = w_depth_ref[t].astype(F32)
        for z in range(depth):
            if 0 <= z + t - 1 < depth:
                depth_scr[pl.ds(z * PAD, hidden), pl.ds((z + t - 1) * PAD, hidden)] = tap
    depth_ref[...] = depth_scr[...].astype(BF16)

    rows, cols = head_ref.shape
    pick = (iota((rows, maps), 0) % maps == iota((rows, maps), 1)).astype(BF16)
    tall = jnp.dot(pick, w_head_ref[...], preferred_element_type=F32).astype(BF16)
    gather = (iota((hidden, cols), 1) % PAD == iota((hidden, cols), 0)).astype(BF16)
    wide = jnp.dot(tall, gather, preferred_element_type=F32)
    at = iota((rows, cols), 0) // maps
    came = iota((rows, cols), 1) // PAD
    flip = (2 * yf + xf) * depth + (depth - 1) * zf
    head_ref[...] = jnp.where(at == (came ^ flip), wide, 0.0).astype(BF16)

    channels, depth, cells = x_ref.shape
    zeros = jnp.zeros((depth * PAD, LANES), BF16)
    xs_ref[:, pl.ds(0, LANES)] = zeros
    xs_ref[:, pl.ds(LANES + cells, LANES)] = zeros
    for c, copy in enumerate(feats):
        part = pl.ds(c * size, size)
        copy.wait()
        x = x_ref[:, :, part].reshape(channels * depth, size)
        xs_ref[:, pl.ds(LANES + c * size, size)] = jnp.dot(big_ref[...], x, preferred_element_type=F32).astype(BF16)


def front(aug_code, w_in, w_plane, w_depth, w_head, feat):
    _, channels = w_in.shape
    maps = w_head.shape[0]
    _, depth, cells = feat.shape
    plane = (2, 4 * PAD, 6 * PAD)
    depth_w = (depth * PAD, depth * PAD)
    head = (4 * depth * maps, 4 * depth * PAD)
    padded = (depth * PAD, cells + 2 * LANES)
    return pl.pallas_call(
        front_kernel,
        out_shape=[jax.ShapeDtypeStruct(s, BF16) for s in (plane, depth_w, head, padded)],
        in_specs=[smem()] + [hbm()] * 5,
        out_specs=[vmem()] * 4,
        scratch_shapes=[
            pltpu.VMEM(w_in.shape, BF16),
            pltpu.VMEM(w_plane.shape, BF16),
            pltpu.VMEM(w_depth.shape, BF16),
            pltpu.VMEM(w_head.shape, BF16),
            pltpu.VMEM(feat.shape, BF16),
            pltpu.VMEM((depth * PAD, channels * depth), BF16),
            pltpu.VMEM(plane, F32),
            pltpu.VMEM(depth_w, F32),
            pltpu.SemaphoreType.DMA((4 + CHUNKS,)),
        ],
        compiler_params=params(),
        cost_estimate=cost(10**8),
        name="front",
    )(aug_code, *stay(w_in, w_plane, w_depth, w_head, feat))


def patch_kernel(half, tiles, brick_rows, keep_from, last, aug_ref, xs_ref, plane_ref, depth_ref, head_ref, *refs):
    if last:
        carry_in, _, anchor_ref, out_ref, anchor_out, a_ref = refs
        anchor_out[...] = jnp.full(anchor_out.shape, anchor_ref[0], I32)
    else:
        out_ref, carry_out, a_ref = refs
    rows, _ = xs_ref.shape
    depth = rows // PAD
    step = 2 * LANES
    margin = LANES
    carried = carry_in.shape[0] if last else 0
    first_tile = tiles[0] * (step // LANES) - carried
    if last:
        a_ref[pl.ds(0, carried)] = carry_in[...]

    def window_stage(t):
        column = (iota((rows, step), 1) + t * step) % half
        block = xs_ref[:, pl.ds(t * step, step + 2 * margin)]
        near = []
        for d in (-1, 0, 1):
            near.append([])
            for e in (-1, 0, 1):
                at = margin + half * e + d
                one = lax.slice_in_dim(block, at, at + step, axis=1)
                if d:
                    one = jnp.where(column == (0 if d < 0 else half - 1), jnp.zeros_like(one), one)
                near[-1].append(one)
        return near

    def plane_stage(near, z):
        cut = slice(z * PAD, (z + 1) * PAD)
        centre = near[1][1][cut].astype(F32)
        first = []
        for py in range(2):
            around = jnp.concatenate([near[d][py + e][cut] for e in range(2) for d in range(3)], axis=0)
            mix = jnp.dot(plane_ref[py], around, preferred_element_type=F32)
            for px in range(2):
                total = mix[px * PAD : (px + 1) * PAD] + mix[(2 + px) * PAD : (3 + px) * PAD]
                first.append((centre + jnp.maximum(total, 0.0)).astype(BF16))
        return first

    def depth_stage(first, p):
        one = jnp.concatenate([first[z][p] for z in range(depth)], axis=0)
        mix = jnp.dot(depth_ref[...], one, preferred_element_type=F32)
        return (one.astype(F32) + jnp.maximum(mix, 0.0)).astype(BF16)

    def head_stage(t, second):
        logits = jnp.zeros((head_ref.shape[0], step), F32)
        for q in range(2):
            pair = jnp.concatenate(second[2 * q : 2 * q + 2], axis=0)
            logits = logits + jnp.dot(head_ref[:, 2 * q * rows : 2 * (q + 1) * rows], pair, preferred_element_type=F32)
        affinity = jax.nn.sigmoid(logits)
        for u in range(step // LANES):
            a_ref[t * (step // LANES) + u - first_tile] = affinity[:, u * LANES : (u + 1) * LANES]

    aug = aug_ref[0]
    yf, xf = (aug >> 1) & 1, (aug >> 2) & 1
    side = half // 4
    tail = side * side - LANES
    row_tiles = head_ref.shape[0] // 8
    lane = iota((8, LANES), 1)
    group = lane // tail
    span = -(-side * half // LANES)
    near_tiles = span - 2

    def source(cell, j, odd):
        y = cell // side
        x = cell - y * side
        y = jnp.where(yf == 1, side - 1 - y, y)
        x = jnp.where(xf == 1, side - 1 - x, x)
        return y * half + side * j + x + odd * (LANES // 2)

    def cut_stage(i, j):
        odd = i % 2
        owned = []
        for k in range(span):
            x = (lane + k * LANES + half - odd * (LANES // 2) % half) % half
            owned.append((x >= side * j) & (x < side * (j + 1)))
        src = source(lane, j, odd)
        main_lane, main_near = src % LANES, src < near_tiles * LANES
        rest_lane = source(LANES + lane % tail, j, odd) % LANES
        base = side * half * i // LANES - first_tile
        brick = (i ^ (3 * yf)) * 4 + (j ^ (3 * xf))
        packed = jnp.zeros((8, LANES), F32)
        for r in range(row_tiles):
            cut = pl.ds(8 * r, 8)
            merged = []
            for tiles_of in (range(near_tiles), range(near_tiles, span)):
                one = a_ref[base + tiles_of[0], cut]
                for k in tiles_of[1:]:
                    one = jnp.where(owned[k], a_ref[base + k, cut], one)
                merged.append(one)
            low = jnp.take_along_axis(merged[0], main_lane, axis=1)
            high = jnp.take_along_axis(merged[1], main_lane, axis=1)
            out_ref[brick, cut] = jnp.where(main_near, low, high)
            rest = jnp.take_along_axis(jnp.where(yf == 1, merged[0], merged[1]), rest_lane, axis=1)
            packed = jnp.where(group == r, rest, packed)
        out_ref[brick, pl.ds(8 * row_tiles, 8)] = packed

    first, second = {}, {}
    waiting = [(i, j) for i in brick_rows for j in range(4)]
    done = first_tile + carried
    for k in range(len(tiles) + 2):
        if k < len(tiles):
            near = window_stage(tiles[k])
            first[k] = []
        second[k - 1] = []
        for q in range(4):
            if k < len(tiles) and q < depth:
                first[k].append(plane_stage(near, q))
            if 0 <= k - 1 < len(tiles):
                second[k - 1].append(depth_stage(first[k - 1], q))
            if waiting and done >= side * half * waiting[0][0] // LANES + span:
                cut_stage(*waiting.pop(0))
        if 0 <= k - 2 < len(tiles):
            head_stage(tiles[k - 2], second[k - 2])
            done += step // LANES
    for left in waiting:
        cut_stage(*left)
    if not last:
        carry_out[...] = a_ref[pl.ds(keep_from - first_tile, done - keep_from)]


def patch_half(half, tiles, brick_rows, keep_from, last, aug_code, shifted, plane, depth_w, head, extra=()):
    kept = head.shape[0]
    carried = extra[0].shape[0] if last else 0
    bricks = jax.ShapeDtypeStruct((16, kept + 8, LANES), F32)
    beside = jax.ShapeDtypeStruct((1, LANES), I32) if last else jax.ShapeDtypeStruct((2 * len(tiles) - keep_from, kept, LANES), F32)
    spaces = [vmem(), vmem(), smem()] if last else []
    return pl.pallas_call(
        functools.partial(patch_kernel, half, tiles, brick_rows, keep_from, last),
        out_shape=[bricks, beside],
        in_specs=[smem()] + [vmem()] * 4 + spaces,
        out_specs=[vmem()] * 2,
        scratch_shapes=[pltpu.VMEM((2 * len(tiles) + carried, kept, LANES), F32)],
        input_output_aliases={6: 0} if last else {},
        compiler_params=params(),
        cost_estimate=cost(10**9),
    )(aug_code, shifted, plane, depth_w, head, *extra)


def seed_kernel(owner_ref, out_ref):
    here = iota(out_ref.shape, 1) == lax.axis_index("patch")
    out_ref[...] = jnp.where(here, owner_ref[0], 0)


def seed_table(owner, devices):
    width = -(-devices // LANES) * LANES
    return pl.pallas_call(
        seed_kernel,
        out_shape=jax.ShapeDtypeStruct((1, width), I32),
        in_specs=[smem()],
        out_specs=vmem(),
        compiler_params=params(),
        name="seed",
    )(owner)


def partner(devices, bit):
    return [(d, d ^ bit) for d in range(devices)]


def slots_kernel(devices, masks, table_ref, anchor_ref, mine_ref, other_ref, window_ref, *outs):
    me = lax.axis_index("patch")
    brick_rows = devices // 4
    brick = iota(table_ref.shape, 1)
    row = lax.rem(brick // 4 - anchor_ref[:, :1] + brick_rows, jnp.full_like(brick, brick_rows))
    place = row * 4 + brick % 4
    owner = jnp.where(brick < devices, table_ref[...], -1)
    _, rows, lanes = mine_ref.shape
    spare = iota((rows, lanes), 1) - jnp.where(iota((rows, lanes), 0) == rows - 8, SPARE, lanes)
    places = [jnp.sum(jnp.where(owner == (me ^ mask), place, 0)) for mask in masks]
    size = outs[0].shape[0]
    for s, at in enumerate(places):
        covered = at < 16
        slot = at if brick_rows <= 4 else jnp.where(covered, at, 0)
        value = (mine_ref[slot] + other_ref[slot]) * window_ref[slot]
        value = jnp.where(spare == at // 4, 2.0, value)
        value = jnp.where(spare == 4, 2.0 * (at % 4).astype(F32), value)
        if brick_rows > 4:
            value = jnp.where(covered, value, 0.0)
        outs[s // size][s % size] = value


def fill_slots(devices, masks, pieces, table, anchor, mine, other, window):
    shape = jax.ShapeDtypeStruct((len(masks) // pieces,) + mine.shape[1:], F32)
    return pl.pallas_call(
        functools.partial(slots_kernel, devices, masks),
        out_shape=[shape] * pieces,
        in_specs=[vmem()] * 5,
        out_specs=[vmem()] * pieces,
        compiler_params=params(),
        name="slots",
    )(table, anchor, mine, other, window)


def brick_kernel(side, maps, depth_curve, mine_ref, *refs):
    *others, rows_ref, cols_ref, out_ref = refs
    depth = len(depth_curve)
    wide = 2 * side
    plane = wide * wide
    tail = side * side - LANES
    per = depth * maps
    brick = mine_ref[0]
    for other in others:
        brick = brick + other[0]
    kept = 4 * per
    main, packed = brick[:kept], brick[kept:]
    rest = jnp.concatenate([packed if k == 0 else pltpu.roll(packed, LANES - tail * k, 1) for k in range(kept // 8)], axis=0)
    fill = jnp.zeros((16 - per, LANES), F32)
    mains = [jnp.concatenate([main[per * p : per * (p + 1)], fill], axis=0) for p in range(4)]
    rests = [jnp.concatenate([rest[per * p : per * (p + 1)], fill], axis=0) for p in range(4)]
    columns = []
    for d in range(-(-plane // LANES)):
        n = iota((8, LANES), 1) + d * LANES
        y = n // wide
        x = n - y * wide
        cell = (y // 2) * side + x // 2
        quarter = 2 * (y % 2) + x % 2
        lane_of = cell % LANES
        top = min((d + 1) * LANES, plane) - 1
        tiles = []
        for r in range(2):
            cut = slice(8 * r, 8 * r + 8)
            value = None
            for p in range(4):
                one = jnp.take_along_axis(mains[p][cut], lane_of, axis=1)
                if (top // wide // 2 + 1) * side > LANES:
                    one = jnp.where(cell >= LANES, jnp.take_along_axis(rests[p][cut], lane_of, axis=1), one)
                value = one if value is None else jnp.where(quarter == p, one, value)
            tiles.append(value)
        columns.append(jnp.concatenate(tiles, axis=0))
    cells = jnp.concatenate(columns, axis=1)[:, :plane]
    for z in range(depth):
        out_ref[0, pl.ds(0, maps), pl.ds(z * plane, plane)] = cells[z * maps : (z + 1) * maps]

    def noted(k):
        lane = jnp.take_along_axis(packed, jnp.full((8, LANES), SPARE + k, I32), axis=1)[0:1]
        return jnp.concatenate([lane] * (rows_ref.shape[1] // LANES), axis=1)

    counts = [noted(i) for i in range(4)]
    added = counts[0] + counts[1] + counts[2] + counts[3]
    column = noted(4)
    down = sum(counts[i] * rows_ref[pl.ds(i, 1), :] for i in range(4))
    across = sum(jnp.where(column == j * added, cols_ref[pl.ds(j, 1), :], 0.0) for j in range(4))
    window = (down * across)[:, :plane]
    for z in range(depth):
        out_ref[0, pl.ds(maps, 1), pl.ds(z * plane, plane)] = window * depth_curve[z]


def finish(side, maps, depth, mine, others):
    plane = 4 * side * side
    width = -(-plane // LANES) * LANES
    curve = bump(8 * side)
    n = np.arange(width)
    y, x = np.minimum(n // (2 * side), 2 * side - 1), n % (2 * side)
    rows = np.stack([curve[2 * side * i + y] for i in range(4)]).astype(np.float32)
    cols = np.stack([curve[2 * side * i + x] for i in range(4)]).astype(np.float32)
    depth_curve = [float(np.float32(v)) for v in bump(depth)]
    return pl.pallas_call(
        functools.partial(brick_kernel, side, maps, depth_curve),
        out_shape=jax.ShapeDtypeStruct((1, maps + 1, depth * plane), F32),
        in_specs=[vmem()] * (len(others) + 3),
        out_specs=vmem(),
        compiler_params=params(),
        name="brick",
    )(mine, *others, rows, cols)


def wire_window(side, maps, depth):
    curve_y, curve_z = bump(8 * side), bump(depth)
    cell = np.arange(side * side)
    out = np.zeros((16, 4 * depth * maps, side * side))
    for i in range(4):
        for j in range(4):
            for p in range(4):
                y = curve_y[2 * side * i + 2 * (cell // side) + p // 2]
                x = curve_y[2 * side * j + 2 * (cell % side) + p % 2]
                for z in range(depth):
                    for m in range(maps):
                        out[4 * i + j, (p * depth + z) * maps + m] = curve_z[z] * y * x
    kept = out.shape[1]
    tail = side * side - LANES
    packed = np.zeros((16, 8, LANES))
    for k in range(kept // 8):
        packed[:, :, tail * k : tail * (k + 1)] = out[:, 8 * k : 8 * k + 8, LANES:]
    return np.concatenate([out[:, :, :LANES], packed], axis=1).astype(np.float32)


def on_device(features, w_in, w_plane, w_depth, w_head, brick_owner, patch_anchor, aug_code):
    devices = lax.axis_size("patch")
    _, _, depth, cells = features.shape
    side = math.isqrt(cells) // 4
    maps = w_head.shape[0]
    levels = [1 << k for k in range(devices.bit_length() - 1)]
    paired = levels[:1] + [bit | 1 for bit in levels[1:]]
    halved = paired[1:-DIRECT]
    direct = [sum(bit for k, bit in enumerate(levels[-DIRECT:]) if q >> k & 1) | min(q, 1) for q in range(1 << DIRECT)]
    masks = [0]
    for bit in reversed(halved):
        masks = masks + [bit ^ mask for mask in masks]
    masks = [mask ^ last for mask in masks for last in direct]

    table = seed_table(brick_owner, devices)
    for bit in halved:
        table = table + lax.ppermute(table, "patch", partner(devices, bit))
    reached = []
    for q in FAR_FIRST:
        reached.append(lax.ppermute(table, "patch", partner(devices, direct[q])))
    table = functools.reduce(lambda a, b: a + b, reached, table)
    table = table + lax.ppermute(table, "patch", partner(devices, 1))
    plane, depth_w, head, shifted = front(aug_code, w_in, w_plane, w_depth, w_head, features[0])
    half = math.isqrt(cells)
    steps = cells // (2 * LANES)
    ready = -(-half * half // 2 // (2 * LANES)) + LEAD
    starts = [half * half * i // 4 // LANES for i in range(4)]
    span = -(-half * half // 4 // LANES)
    early = [i for i in range(4) if starts[i] + span < 2 * ready]
    late = [i for i in range(4) if i not in early]
    bricks, carry = patch_half(half, range(ready), early, starts[late[0]], False, aug_code, shifted, plane, depth_w, head)
    bricks, anchor = patch_half(
        half, range(ready, steps), late, 0, True, aug_code, shifted, plane, depth_w, head, (carry, bricks, patch_anchor)
    )
    other = lax.ppermute(bricks, "patch", partner(devices, 1))
    pieces = 2 if halved else len(direct)
    parts = fill_slots(devices, masks, pieces, table, anchor, bricks, other, wire_window(side, maps, depth))
    for k, bit in enumerate(halved):
        keep, send = parts
        got = lax.ppermute(send, "patch", partner(devices, bit))
        size = send.shape[0] // 2 if k + 1 < len(halved) else 1
        parts = [keep[i : i + size] + got[i : i + size] for i in range(0, send.shape[0], size)]
    others = [lax.ppermute(parts[q], "patch", partner(devices, direct[q])) for q in FAR_FIRST]
    return finish(side, maps, depth, parts[0], others)


def solution(mesh):
    one = P(("group", "patch"))
    in_specs = (P(("group", "patch"), None, None, None), P(), P(), P(), P(), one, one, one)
    return jax.shard_map(
        on_device, mesh=mesh, in_specs=in_specs, out_specs=P(("group", "patch"), None, None), check_vma=False
    )
```

```python
import functools
import math

import numpy as np

import jax
import jax.numpy as jnp
from jax import lax
from jax.experimental import pallas as pl
from jax.experimental.pallas import tpu as pltpu
from jax.sharding import PartitionSpec as P


F32 = jnp.float32
BF16 = jnp.bfloat16
I32 = jnp.int32
PAD = 32
LANES = 128
CHUNKS = 2
FAR_FIRST = (3, 2, 1)
DIRECT = 2
LEAD = 1
SPARE = 96


def iota(shape, axis):
    return lax.broadcasted_iota(I32, shape, axis)


def vmem():
    return pl.BlockSpec(memory_space=pltpu.VMEM)


def smem():
    return pl.BlockSpec(memory_space=pltpu.SMEM)


def hbm():
    return pl.BlockSpec(memory_space=pltpu.HBM)


def stay(*arrays):
    return [pltpu.with_memory_space_constraint(a, pltpu.HBM) for a in arrays]


def params():
    return pltpu.CompilerParams(vmem_limit_bytes=16 * 2**20)


def cost(flops):
    return pl.CostEstimate(flops=flops, bytes_accessed=2**20, transcendentals=0)


def bump(length):
    position = (np.arange(length, dtype=np.float64) + 0.5) / length
    return 0.1 + np.sin(np.pi * position) ** 2


def front_kernel(aug_ref, w_in_hbm, w_plane_hbm, w_depth_hbm, w_head_hbm, x_hbm, plane_ref, depth_ref, head_ref, xs_ref, w_in_ref, w_plane_ref, w_depth_ref, w_head_ref, x_ref, big_ref, plane_scr, depth_scr, sems):
    size = x_hbm.shape[2] // CHUNKS
    feats = [
        pltpu.make_async_copy(x_hbm.at[:, :, pl.ds(c * size, size)], x_ref.at[:, :, pl.ds(c * size, size)], sems.at[4 + c])
        for c in range(CHUNKS)
    ]
    pairs = ((w_plane_hbm, w_plane_ref), (w_in_hbm, w_in_ref), (w_depth_hbm, w_depth_ref), (w_head_hbm, w_head_ref))
    copies = [pltpu.make_async_copy(src, dst, sems.at[k]) for k, (src, dst) in enumerate(pairs)]
    for copy in copies + feats:
        copy.start()
    for copy in copies:
        copy.wait()
    hidden, _ = w_in_ref.shape
    depth = depth_ref.shape[0] // PAD
    maps = w_head_ref.shape[0]
    aug = aug_ref[0]
    zf, yf, xf = aug & 1, (aug >> 1) & 1, (aug >> 2) & 1

    rows, cols = big_ref.shape
    spread = (iota((rows, hidden), 0) % PAD == iota((rows, hidden), 1)).astype(BF16)
    gather = (iota((w_in_ref.shape[1], cols), 1) // depth == iota((w_in_ref.shape[1], cols), 0)).astype(BF16)
    tall = jnp.dot(spread, w_in_ref[...], preferred_element_type=F32).astype(BF16)
    wide = jnp.dot(tall, gather, preferred_element_type=F32)
    same = iota((rows, cols), 1) % depth == iota((rows, cols), 0) // PAD
    big_ref[...] = jnp.where(same, wide, 0.0).astype(BF16)

    plane_scr[...] = jnp.zeros_like(plane_scr)
    taps = [w_plane_ref[t].astype(F32) for t in range(9)]
    near = (((0,), (1, 2), ()), ((), (0, 1), (2,)))
    for py in range(2):
        for px in range(2):
            for dy in range(2):
                for dx in range(3):
                    hit = [taps[3 * ty + tx] for ty in near[py][dy + py] for tx in near[px][dx]]
                    if not hit:
                        continue
                    total = functools.reduce(lambda a, b: a + b, hit)
                    high = total.astype(BF16).astype(F32)
                    col = (3 * dy + dx) * PAD
                    plane_scr[py, pl.ds(px * PAD, hidden), pl.ds(col, hidden)] = high
                    plane_scr[py, pl.ds((2 + px) * PAD, hidden), pl.ds(col, hidden)] = total - high
    plane_ref[...] = plane_scr[...].astype(BF16)

    depth_scr[...] = jnp.zeros_like(depth_scr)
    for t in range(3):
        tap = w_depth_ref[t].astype(F32)
        for z in range(depth):
            if 0 <= z + t - 1 < depth:
                depth_scr[pl.ds(z * PAD, hidden), pl.ds((z + t - 1) * PAD, hidden)] = tap
    depth_ref[...] = depth_scr[...].astype(BF16)

    rows, cols = head_ref.shape
    pick = (iota((rows, maps), 0) % maps == iota((rows, maps), 1)).astype(BF16)
    tall = jnp.dot(pick, w_head_ref[...], preferred_element_type=F32).astype(BF16)
    gather = (iota((hidden, cols), 1) % PAD == iota((hidden, cols), 0)).astype(BF16)
    wide = jnp.dot(tall, gather, preferred_element_type=F32)
    at = iota((rows, cols), 0) // maps
    came = iota((rows, cols), 1) // PAD
    flip = (2 * yf + xf) * depth + (depth - 1) * zf
    head_ref[...] = jnp.where(at == (came ^ flip), wide, 0.0).astype(BF16)

    channels, depth, cells = x_ref.shape
    zeros = jnp.zeros((depth * PAD, LANES), BF16)
    xs_ref[:, pl.ds(0, LANES)] = zeros
    xs_ref[:, pl.ds(LANES + cells, LANES)] = zeros
    for c, copy in enumerate(feats):
        part = pl.ds(c * size, size)
        copy.wait()
        x = x_ref[:, :, part].reshape(channels * depth, size)
        xs_ref[:, pl.ds(LANES + c * size, size)] = jnp.dot(big_ref[...], x, preferred_element_type=F32).astype(BF16)


def front(aug_code, w_in, w_plane, w_depth, w_head, feat):
    _, channels = w_in.shape
    maps = w_head.shape[0]
    _, depth, cells = feat.shape
    plane = (2, 4 * PAD, 6 * PAD)
    depth_w = (depth * PAD, depth * PAD)
    head = (4 * depth * maps, 4 * depth * PAD)
    padded = (depth * PAD, cells + 2 * LANES)
    return pl.pallas_call(
        front_kernel,
        out_shape=[jax.ShapeDtypeStruct(s, BF16) for s in (plane, depth_w, head, padded)],
        in_specs=[smem()] + [hbm()] * 5,
        out_specs=[vmem()] * 4,
        scratch_shapes=[
            pltpu.VMEM(w_in.shape, BF16),
            pltpu.VMEM(w_plane.shape, BF16),
            pltpu.VMEM(w_depth.shape, BF16),
            pltpu.VMEM(w_head.shape, BF16),
            pltpu.VMEM(feat.shape, BF16),
            pltpu.VMEM((depth * PAD, channels * depth), BF16),
            pltpu.VMEM(plane, F32),
            pltpu.VMEM(depth_w, F32),
            pltpu.SemaphoreType.DMA((4 + CHUNKS,)),
        ],
        compiler_params=params(),
        cost_estimate=cost(10**8),
        name="front",
    )(aug_code, *stay(w_in, w_plane, w_depth, w_head, feat))


def patch_kernel(half, tiles, brick_rows, keep_from, last, aug_ref, xs_ref, plane_ref, depth_ref, head_ref, *refs):
    if last:
        carry_in, _, anchor_ref, out_ref, anchor_out, a_ref = refs
        anchor_out[...] = jnp.full(anchor_out.shape, anchor_ref[0], I32)
    else:
        out_ref, carry_out, a_ref = refs
    rows, _ = xs_ref.shape
    depth = rows // PAD
    step = 2 * LANES
    margin = LANES
    carried = carry_in.shape[0] if last else 0
    first_tile = tiles[0] * (step // LANES) - carried
    if last:
        a_ref[pl.ds(0, carried)] = carry_in[...]

    def window_stage(t):
        column = (iota((rows, step), 1) + t * step) % half
        block = xs_ref[:, pl.ds(t * step, step + 2 * margin)]
        near = []
        for d in (-1, 0, 1):
            near.append([])
            for e in (-1, 0, 1):
                at = margin + half * e + d
                one = lax.slice_in_dim(block, at, at + step, axis=1)
                if d:
                    one = jnp.where(column == (0 if d < 0 else half - 1), jnp.zeros_like(one), one)
                near[-1].append(one)
        return near

    def plane_stage(near, z):
        cut = slice(z * PAD, (z + 1) * PAD)
        centre = near[1][1][cut].astype(F32)
        first = []
        for py in range(2):
            around = jnp.concatenate([near[d][py + e][cut] for e in range(2) for d in range(3)], axis=0)
            mix = jnp.dot(plane_ref[py], around, preferred_element_type=F32)
            for px in range(2):
                total = mix[px * PAD : (px + 1) * PAD] + mix[(2 + px) * PAD : (3 + px) * PAD]
                first.append((centre + jnp.maximum(total, 0.0)).astype(BF16))
        return first

    def depth_stage(first, p):
        one = jnp.concatenate([first[z][p] for z in range(depth)], axis=0)
        mix = jnp.dot(depth_ref[...], one, preferred_element_type=F32)
        return (one.astype(F32) + jnp.maximum(mix, 0.0)).astype(BF16)

    def head_stage(t, second):
        logits = jnp.zeros((head_ref.shape[0], step), F32)
        for q in range(2):
            pair = jnp.concatenate(second[2 * q : 2 * q + 2], axis=0)
            logits = logits + jnp.dot(head_ref[:, 2 * q * rows : 2 * (q + 1) * rows], pair, preferred_element_type=F32)
        affinity = jax.nn.sigmoid(logits)
        for u in range(step // LANES):
            a_ref[t * (step // LANES) + u - first_tile] = affinity[:, u * LANES : (u + 1) * LANES]

    aug = aug_ref[0]
    yf, xf = (aug >> 1) & 1, (aug >> 2) & 1
    side = half // 4
    tail = side * side - LANES
    row_tiles = head_ref.shape[0] // 8
    lane = iota((8, LANES), 1)
    group = lane // tail
    span = -(-side * half // LANES)
    near_tiles = span - 2

    def source(cell, j, odd):
        y = cell // side
        x = cell - y * side
        y = jnp.where(yf == 1, side - 1 - y, y)
        x = jnp.where(xf == 1, side - 1 - x, x)
        return y * half + side * j + x + odd * (LANES // 2)

    def cut_stage(i, j):
        odd = i % 2
        owned = []
        for k in range(span):
            x = (lane + k * LANES + half - odd * (LANES // 2) % half) % half
            owned.append((x >= side * j) & (x < side * (j + 1)))
        src = source(lane, j, odd)
        main_lane, main_near = src % LANES, src < near_tiles * LANES
        rest_lane = source(LANES + lane % tail, j, odd) % LANES
        base = side * half * i // LANES - first_tile
        brick = (i ^ (3 * yf)) * 4 + (j ^ (3 * xf))
        packed = jnp.zeros((8, LANES), F32)
        for r in range(row_tiles):
            cut = pl.ds(8 * r, 8)
            merged = []
            for tiles_of in (range(near_tiles), range(near_tiles, span)):
                one = a_ref[base + tiles_of[0], cut]
                for k in tiles_of[1:]:
                    one = jnp.where(owned[k], a_ref[base + k, cut], one)
                merged.append(one)
            low = jnp.take_along_axis(merged[0], main_lane, axis=1)
            high = jnp.take_along_axis(merged[1], main_lane, axis=1)
            out_ref[brick, cut] = jnp.where(main_near, low, high)
            rest = jnp.take_along_axis(jnp.where(yf == 1, merged[0], merged[1]), rest_lane, axis=1)
            packed = jnp.where(group == r, rest, packed)
        out_ref[brick, pl.ds(8 * row_tiles, 8)] = packed

    first, second = {}, {}
    waiting = [(i, j) for i in brick_rows for j in range(4)]
    done = first_tile + carried
    for k in range(len(tiles) + 2):
        if k < len(tiles):
            near = window_stage(tiles[k])
            first[k] = []
        second[k - 1] = []
        for q in range(4):
            if k < len(tiles) and q < depth:
                first[k].append(plane_stage(near, q))
            if 0 <= k - 1 < len(tiles):
                second[k - 1].append(depth_stage(first[k - 1], q))
            if waiting and done >= side * half * waiting[0][0] // LANES + span:
                cut_stage(*waiting.pop(0))
        if 0 <= k - 2 < len(tiles):
            head_stage(tiles[k - 2], second[k - 2])
            done += step // LANES
    for left in waiting:
        cut_stage(*left)
    if not last:
        carry_out[...] = a_ref[pl.ds(keep_from - first_tile, done - keep_from)]


def patch_half(half, tiles, brick_rows, keep_from, last, aug_code, shifted, plane, depth_w, head, extra=()):
    kept = head.shape[0]
    carried = extra[0].shape[0] if last else 0
    bricks = jax.ShapeDtypeStruct((16, kept + 8, LANES), F32)
    beside = jax.ShapeDtypeStruct((1, LANES), I32) if last else jax.ShapeDtypeStruct((2 * len(tiles) - keep_from, kept, LANES), F32)
    spaces = [vmem(), vmem(), smem()] if last else []
    return pl.pallas_call(
        functools.partial(patch_kernel, half, tiles, brick_rows, keep_from, last),
        out_shape=[bricks, beside],
        in_specs=[smem()] + [vmem()] * 4 + spaces,
        out_specs=[vmem()] * 2,
        scratch_shapes=[pltpu.VMEM((2 * len(tiles) + carried, kept, LANES), F32)],
        input_output_aliases={6: 0} if last else {},
        compiler_params=params(),
        cost_estimate=cost(10**9),
    )(aug_code, shifted, plane, depth_w, head, *extra)


def seed_kernel(owner_ref, out_ref):
    here = iota(out_ref.shape, 1) == lax.axis_index("patch")
    out_ref[...] = jnp.where(here, owner_ref[0], 0)


def seed_table(owner, devices):
    width = -(-devices // LANES) * LANES
    return pl.pallas_call(
        seed_kernel,
        out_shape=jax.ShapeDtypeStruct((1, width), I32),
        in_specs=[smem()],
        out_specs=vmem(),
        compiler_params=params(),
        name="seed",
    )(owner)


def partner(devices, bit):
    return [(d, d ^ bit) for d in range(devices)]


def slots_kernel(devices, masks, table_ref, anchor_ref, mine_ref, other_ref, window_ref, *outs):
    me = lax.axis_index("patch")
    brick_rows = devices // 4
    brick = iota(table_ref.shape, 1)
    row = lax.rem(brick // 4 - anchor_ref[:, :1] + brick_rows, jnp.full_like(brick, brick_rows))
    place = row * 4 + brick % 4
    owner = jnp.where(brick < devices, table_ref[...], -1)
    _, rows, lanes = mine_ref.shape
    spare = iota((rows, lanes), 1) - jnp.where(iota((rows, lanes), 0) == rows - 8, SPARE, lanes)
    places = [jnp.sum(jnp.where(owner == (me ^ mask), place, 0)) for mask in masks]
    size = outs[0].shape[0]
    for s, at in enumerate(places):
        covered = at < 16
        slot = at if brick_rows <= 4 else jnp.where(covered, at, 0)
        value = (mine_ref[slot] + other_ref[slot]) * window_ref[slot]
        value = jnp.where(spare == at // 4, 2.0, value)
        value = jnp.where(spare == 4, 2.0 * (at % 4).astype(F32), value)
        if brick_rows > 4:
            value = jnp.where(covered, value, 0.0)
        outs[s // size][s % size] = value


def fill_slots(devices, masks, pieces, table, anchor, mine, other, window):
    shape = jax.ShapeDtypeStruct((len(masks) // pieces,) + mine.shape[1:], F32)
    return pl.pallas_call(
        functools.partial(slots_kernel, devices, masks),
        out_shape=[shape] * pieces,
        in_specs=[vmem()] * 5,
        out_specs=[vmem()] * pieces,
        compiler_params=params(),
        name="slots",
    )(table, anchor, mine, other, window)


def brick_kernel(side, maps, depth_curve, mine_ref, *refs):
    *others, rows_ref, cols_ref, out_ref = refs
    depth = len(depth_curve)
    wide = 2 * side
    plane = wide * wide
    tail = side * side - LANES
    per = depth * maps
    brick = mine_ref[0]
    for other in others:
        brick = brick + other[0]
    kept = 4 * per
    main, packed = brick[:kept], brick[kept:]
    rest = jnp.concatenate([packed if k == 0 else pltpu.roll(packed, LANES - tail * k, 1) for k in range(kept // 8)], axis=0)
    fill = jnp.zeros((16 - per, LANES), F32)
    mains = [jnp.concatenate([main[per * p : per * (p + 1)], fill], axis=0) for p in range(4)]
    rests = [jnp.concatenate([rest[per * p : per * (p + 1)], fill], axis=0) for p in range(4)]
    columns = []
    for d in range(-(-plane // LANES)):
        n = iota((8, LANES), 1) + d * LANES
        y = n // wide
        x = n - y * wide
        cell = (y // 2) * side + x // 2
        quarter = 2 * (y % 2) + x % 2
        lane_of = cell % LANES
        top = min((d + 1) * LANES, plane) - 1
        tiles = []
        for r in range(2):
            cut = slice(8 * r, 8 * r + 8)
            value = None
            for p in range(4):
                one = jnp.take_along_axis(mains[p][cut], lane_of, axis=1)
                if (top // wide // 2 + 1) * side > LANES:
                    one = jnp.where(cell >= LANES, jnp.take_along_axis(rests[p][cut], lane_of, axis=1), one)
                value = one if value is None else jnp.where(quarter == p, one, value)
            tiles.append(value)
        columns.append(jnp.concatenate(tiles, axis=0))
    cells = jnp.concatenate(columns, axis=1)[:, :plane]
    for z in range(depth):
        out_ref[0, pl.ds(0, maps), pl.ds(z * plane, plane)] = cells[z * maps : (z + 1) * maps]

    def noted(k):
        lane = jnp.take_along_axis(packed, jnp.full((8, LANES), SPARE + k, I32), axis=1)[0:1]
        return jnp.concatenate([lane] * (rows_ref.shape[1] // LANES), axis=1)

    counts = [noted(i) for i in range(4)]
    added = counts[0] + counts[1] + counts[2] + counts[3]
    column = noted(4)
    down = sum(counts[i] * rows_ref[pl.ds(i, 1), :] for i in range(4))
    across = sum(jnp.where(column == j * added, cols_ref[pl.ds(j, 1), :], 0.0) for j in range(4))
    window = (down * across)[:, :plane]
    for z in range(depth):
        out_ref[0, pl.ds(maps, 1), pl.ds(z * plane, plane)] = window * depth_curve[z]


def finish(side, maps, depth, mine, others):
    plane = 4 * side * side
    width = -(-plane // LANES) * LANES
    curve = bump(8 * side)
    n = np.arange(width)
    y, x = np.minimum(n // (2 * side), 2 * side - 1), n % (2 * side)
    rows = np.stack([curve[2 * side * i + y] for i in range(4)]).astype(np.float32)
    cols = np.stack([curve[2 * side * i + x] for i in range(4)]).astype(np.float32)
    depth_curve = [float(np.float32(v)) for v in bump(depth)]
    return pl.pallas_call(
        functools.partial(brick_kernel, side, maps, depth_curve),
        out_shape=jax.ShapeDtypeStruct((1, maps + 1, depth * plane), F32),
        in_specs=[vmem()] * (len(others) + 3),
        out_specs=vmem(),
        compiler_params=params(),
        name="brick",
    )(mine, *others, rows, cols)


def wire_window(side, maps, depth):
    curve_y, curve_z = bump(8 * side), bump(depth)
    cell = np.arange(side * side)
    out = np.zeros((16, 4 * depth * maps, side * side))
    for i in range(4):
        for j in range(4):
            for p in range(4):
                y = curve_y[2 * side * i + 2 * (cell // side) + p // 2]
                x = curve_y[2 * side * j + 2 * (cell % side) + p % 2]
                for z in range(depth):
                    for m in range(maps):
                        out[4 * i + j, (p * depth + z) * maps + m] = curve_z[z] * y * x
    kept = out.shape[1]
    tail = side * side - LANES
    packed = np.zeros((16, 8, LANES))
    for k in range(kept // 8):
        packed[:, :, tail * k : tail * (k + 1)] = out[:, 8 * k : 8 * k + 8, LANES:]
    return np.concatenate([out[:, :, :LANES], packed], axis=1).astype(np.float32)


def on_device(features, w_in, w_plane, w_depth, w_head, brick_owner, patch_anchor, aug_code):
    devices = lax.axis_size("patch")
    _, _, depth, cells = features.shape
    side = math.isqrt(cells) // 4
    maps = w_head.shape[0]
    levels = [1 << k for k in range(devices.bit_length() - 1)]
    paired = levels[:1] + [bit | 1 for bit in levels[1:]]
    halved = paired[1 + DIRECT :]
    direct = [sum(bit for k, bit in enumerate(levels[1 : 1 + DIRECT]) if q >> k & 1) | min(q, 1) for q in range(1 << DIRECT)]
    masks = [0]
    for bit in reversed(halved):
        masks = masks + [bit ^ mask for mask in masks]
    masks = [first ^ mask for first in direct for mask in masks]

    def table_round(k, table):
        return table + lax.ppermute(table, "patch", partner(devices, rounds[k]))

    rounds = paired
    table = seed_table(brick_owner, devices)
    for k in range(len(rounds)):
        table = table_round(k, table)
    plane, depth_w, head, shifted = front(aug_code, w_in, w_plane, w_depth, w_head, features[0])
    half = math.isqrt(cells)
    steps = cells // (2 * LANES)
    ready = -(-half * half // 2 // (2 * LANES)) + LEAD
    starts = [half * half * i // 4 // LANES for i in range(4)]
    span = -(-half * half // 4 // LANES)
    early = [i for i in range(4) if starts[i] + span < 2 * ready]
    late = [i for i in range(4) if i not in early]
    bricks, carry = patch_half(half, range(ready), early, starts[late[0]], False, aug_code, shifted, plane, depth_w, head)
    bricks, anchor = patch_half(
        half, range(ready, steps), late, 0, True, aug_code, shifted, plane, depth_w, head, (carry, bricks, patch_anchor)
    )
    other = lax.ppermute(bricks, "patch", partner(devices, 1))
    parts = fill_slots(devices, masks, len(direct), table, anchor, bricks, other, wire_window(side, maps, depth))
    sums = [parts[0]] + [lax.ppermute(parts[q], "patch", partner(devices, direct[q])) for q in FAR_FIRST]
    for bit in halved:
        size = sums[0].shape[0] // 2
        keep, send = (functools.reduce(lambda a, b: a + b, [one[k : k + size] for one in sums]) for k in (0, size))
        sums = [keep, lax.ppermute(send, "patch", partner(devices, bit))]
    return finish(side, maps, depth, sums[0], sums[1:])


def solution(mesh):
    one = P(("group", "patch"))
    in_specs = (P(("group", "patch"), None, None, None), P(), P(), P(), P(), one, one, one)
    return jax.shard_map(
        on_device, mesh=mesh, in_specs=in_specs, out_specs=P(("group", "patch"), None, None), check_vma=False
    )
```

```python
import functools
import math

import numpy as np

import jax
import jax.numpy as jnp
from jax import lax
from jax.experimental import pallas as pl
from jax.experimental.pallas import tpu as pltpu
from jax.sharding import PartitionSpec as P


F32 = jnp.float32
BF16 = jnp.bfloat16
I32 = jnp.int32
PAD = 32
LANES = 128
CHUNKS = 2
START_ORDER = (1, 3, 2)
DIRECT = 2
LEAD = 1
SPARE = 96


def iota(shape, axis):
    return lax.broadcasted_iota(I32, shape, axis)


def vmem():
    return pl.BlockSpec(memory_space=pltpu.VMEM)


def smem():
    return pl.BlockSpec(memory_space=pltpu.SMEM)


def hbm():
    return pl.BlockSpec(memory_space=pltpu.HBM)


def stay(*arrays):
    return [pltpu.with_memory_space_constraint(a, pltpu.HBM) for a in arrays]


def params():
    return pltpu.CompilerParams(vmem_limit_bytes=16 * 2**20)


def cost(flops):
    return pl.CostEstimate(flops=flops, bytes_accessed=2**20, transcendentals=0)


def bump(length):
    position = (np.arange(length, dtype=np.float64) + 0.5) / length
    return 0.1 + np.sin(np.pi * position) ** 2


def front_kernel(aug_ref, w_in_hbm, w_plane_hbm, w_depth_hbm, w_head_hbm, x_hbm, plane_ref, depth_ref, head_ref, xs_ref, w_in_ref, w_plane_ref, w_depth_ref, w_head_ref, x_ref, big_ref, plane_scr, depth_scr, sems):
    size = x_hbm.shape[2] // CHUNKS
    feats = [
        pltpu.make_async_copy(x_hbm.at[:, :, pl.ds(c * size, size)], x_ref.at[:, :, pl.ds(c * size, size)], sems.at[4 + c])
        for c in range(CHUNKS)
    ]
    pairs = ((w_plane_hbm, w_plane_ref), (w_in_hbm, w_in_ref), (w_depth_hbm, w_depth_ref), (w_head_hbm, w_head_ref))
    copies = [pltpu.make_async_copy(src, dst, sems.at[k]) for k, (src, dst) in enumerate(pairs)]
    for copy in copies + feats:
        copy.start()
    for copy in copies:
        copy.wait()
    hidden, _ = w_in_ref.shape
    depth = depth_ref.shape[0] // PAD
    maps = w_head_ref.shape[0]
    aug = aug_ref[0]
    zf, yf, xf = aug & 1, (aug >> 1) & 1, (aug >> 2) & 1

    rows, cols = big_ref.shape
    spread = (iota((rows, hidden), 0) % PAD == iota((rows, hidden), 1)).astype(BF16)
    gather = (iota((w_in_ref.shape[1], cols), 1) // depth == iota((w_in_ref.shape[1], cols), 0)).astype(BF16)
    tall = jnp.dot(spread, w_in_ref[...], preferred_element_type=F32).astype(BF16)
    wide = jnp.dot(tall, gather, preferred_element_type=F32)
    same = iota((rows, cols), 1) % depth == iota((rows, cols), 0) // PAD
    big_ref[...] = jnp.where(same, wide, 0.0).astype(BF16)

    plane_scr[...] = jnp.zeros_like(plane_scr)
    taps = [w_plane_ref[t].astype(F32) for t in range(9)]
    near = (((0,), (1, 2), ()), ((), (0, 1), (2,)))
    for py in range(2):
        for px in range(2):
            for dy in range(2):
                for dx in range(3):
                    hit = [taps[3 * ty + tx] for ty in near[py][dy + py] for tx in near[px][dx]]
                    if not hit:
                        continue
                    total = functools.reduce(lambda a, b: a + b, hit)
                    high = total.astype(BF16).astype(F32)
                    col = (3 * dy + dx) * PAD
                    plane_scr[py, pl.ds(px * PAD, hidden), pl.ds(col, hidden)] = high
                    plane_scr[py, pl.ds((2 + px) * PAD, hidden), pl.ds(col, hidden)] = total - high
    plane_ref[...] = plane_scr[...].astype(BF16)

    depth_scr[...] = jnp.zeros_like(depth_scr)
    for t in range(3):
        tap = w_depth_ref[t].astype(F32)
        for z in range(depth):
            if 0 <= z + t - 1 < depth:
                depth_scr[pl.ds(z * PAD, hidden), pl.ds((z + t - 1) * PAD, hidden)] = tap
    depth_ref[...] = depth_scr[...].astype(BF16)

    rows, cols = head_ref.shape
    pick = (iota((rows, maps), 0) % maps == iota((rows, maps), 1)).astype(BF16)
    tall = jnp.dot(pick, w_head_ref[...], preferred_element_type=F32).astype(BF16)
    gather = (iota((hidden, cols), 1) % PAD == iota((hidden, cols), 0)).astype(BF16)
    wide = jnp.dot(tall, gather, preferred_element_type=F32)
    at = iota((rows, cols), 0) // maps
    came = iota((rows, cols), 1) // PAD
    flip = (2 * yf + xf) * depth + (depth - 1) * zf
    head_ref[...] = jnp.where(at == (came ^ flip), wide, 0.0).astype(BF16)

    channels, depth, cells = x_ref.shape
    zeros = jnp.zeros((depth * PAD, LANES), BF16)
    xs_ref[:, pl.ds(0, LANES)] = zeros
    xs_ref[:, pl.ds(LANES + cells, LANES)] = zeros
    for c, copy in enumerate(feats):
        part = pl.ds(c * size, size)
        copy.wait()
        x = x_ref[:, :, part].reshape(channels * depth, size)
        xs_ref[:, pl.ds(LANES + c * size, size)] = jnp.dot(big_ref[...], x, preferred_element_type=F32).astype(BF16)


def front(aug_code, w_in, w_plane, w_depth, w_head, feat):
    _, channels = w_in.shape
    maps = w_head.shape[0]
    _, depth, cells = feat.shape
    plane = (2, 4 * PAD, 6 * PAD)
    depth_w = (depth * PAD, depth * PAD)
    head = (4 * depth * maps, 4 * depth * PAD)
    padded = (depth * PAD, cells + 2 * LANES)
    return pl.pallas_call(
        front_kernel,
        out_shape=[jax.ShapeDtypeStruct(s, BF16) for s in (plane, depth_w, head, padded)],
        in_specs=[smem()] + [hbm()] * 5,
        out_specs=[vmem()] * 4,
        scratch_shapes=[
            pltpu.VMEM(w_in.shape, BF16),
            pltpu.VMEM(w_plane.shape, BF16),
            pltpu.VMEM(w_depth.shape, BF16),
            pltpu.VMEM(w_head.shape, BF16),
            pltpu.VMEM(feat.shape, BF16),
            pltpu.VMEM((depth * PAD, channels * depth), BF16),
            pltpu.VMEM(plane, F32),
            pltpu.VMEM(depth_w, F32),
            pltpu.SemaphoreType.DMA((4 + CHUNKS,)),
        ],
        compiler_params=params(),
        cost_estimate=cost(10**8),
        name="front",
    )(aug_code, *stay(w_in, w_plane, w_depth, w_head, feat))


def patch_kernel(half, tiles, brick_rows, keep_from, last, aug_ref, xs_ref, plane_ref, depth_ref, head_ref, *refs):
    if last:
        carry_in, _, out_ref, a_ref = refs
    else:
        out_ref, carry_out, a_ref = refs
    rows, _ = xs_ref.shape
    depth = rows // PAD
    step = 2 * LANES
    margin = LANES
    carried = carry_in.shape[0] if last else 0
    first_tile = tiles[0] * (step // LANES) - carried
    if last:
        a_ref[pl.ds(0, carried)] = carry_in[...]

    def window_stage(t):
        column = (iota((rows, step), 1) + t * step) % half
        block = xs_ref[:, pl.ds(t * step, step + 2 * margin)]
        near = []
        for d in (-1, 0, 1):
            near.append([])
            for e in (-1, 0, 1):
                at = margin + half * e + d
                one = lax.slice_in_dim(block, at, at + step, axis=1)
                if d:
                    one = jnp.where(column == (0 if d < 0 else half - 1), jnp.zeros_like(one), one)
                near[-1].append(one)
        return near

    def plane_stage(near, z):
        cut = slice(z * PAD, (z + 1) * PAD)
        centre = near[1][1][cut].astype(F32)
        first = []
        for py in range(2):
            around = jnp.concatenate([near[d][py + e][cut] for e in range(2) for d in range(3)], axis=0)
            mix = jnp.dot(plane_ref[py], around, preferred_element_type=F32)
            for px in range(2):
                total = mix[px * PAD : (px + 1) * PAD] + mix[(2 + px) * PAD : (3 + px) * PAD]
                first.append((centre + jnp.maximum(total, 0.0)).astype(BF16))
        return first

    def depth_stage(first, p):
        one = jnp.concatenate([first[z][p] for z in range(depth)], axis=0)
        mix = jnp.dot(depth_ref[...], one, preferred_element_type=F32)
        return (one.astype(F32) + jnp.maximum(mix, 0.0)).astype(BF16)

    def head_stage(t, second):
        logits = jnp.zeros((head_ref.shape[0], step), F32)
        for q in range(2):
            pair = jnp.concatenate(second[2 * q : 2 * q + 2], axis=0)
            logits = logits + jnp.dot(head_ref[:, 2 * q * rows : 2 * (q + 1) * rows], pair, preferred_element_type=F32)
        affinity = jax.nn.sigmoid(logits)
        for u in range(step // LANES):
            a_ref[t * (step // LANES) + u - first_tile] = affinity[:, u * LANES : (u + 1) * LANES]

    aug = aug_ref[0]
    yf, xf = (aug >> 1) & 1, (aug >> 2) & 1
    side = half // 4
    tail = side * side - LANES
    row_tiles = head_ref.shape[0] // 8
    lane = iota((8, LANES), 1)
    group = lane // tail
    span = -(-side * half // LANES)
    near_tiles = span - 2

    def source(cell, j, odd):
        y = cell // side
        x = cell - y * side
        y = jnp.where(yf == 1, side - 1 - y, y)
        x = jnp.where(xf == 1, side - 1 - x, x)
        return y * half + side * j + x + odd * (LANES // 2)

    def cut_stage(i, j):
        odd = i % 2
        owned = []
        for k in range(span):
            x = (lane + k * LANES + half - odd * (LANES // 2) % half) % half
            owned.append((x >= side * j) & (x < side * (j + 1)))
        src = source(lane, j, odd)
        main_lane, main_near = src % LANES, src < near_tiles * LANES
        rest_lane = source(LANES + lane % tail, j, odd) % LANES
        base = side * half * i // LANES - first_tile
        brick = (i ^ (3 * yf)) * 4 + (j ^ (3 * xf))
        packed = jnp.zeros((8, LANES), F32)
        for r in range(row_tiles):
            cut = pl.ds(8 * r, 8)
            merged = []
            for tiles_of in (range(near_tiles), range(near_tiles, span)):
                one = a_ref[base + tiles_of[0], cut]
                for k in tiles_of[1:]:
                    one = jnp.where(owned[k], a_ref[base + k, cut], one)
                merged.append(one)
            low = jnp.take_along_axis(merged[0], main_lane, axis=1)
            high = jnp.take_along_axis(merged[1], main_lane, axis=1)
            out_ref[brick, cut] = jnp.where(main_near, low, high)
            rest = jnp.take_along_axis(jnp.where(yf == 1, merged[0], merged[1]), rest_lane, axis=1)
            packed = jnp.where(group == r, rest, packed)
        out_ref[brick, pl.ds(8 * row_tiles, 8)] = packed

    first, second = {}, {}
    waiting = [(i, j) for i in brick_rows for j in range(4)]
    done = first_tile + carried
    for k in range(len(tiles) + 2):
        if k < len(tiles):
            near = window_stage(tiles[k])
            first[k] = []
        second[k - 1] = []
        for q in range(4):
            if k < len(tiles) and q < depth:
                first[k].append(plane_stage(near, q))
            if 0 <= k - 1 < len(tiles):
                second[k - 1].append(depth_stage(first[k - 1], q))
            if waiting and done >= side * half * waiting[0][0] // LANES + span:
                cut_stage(*waiting.pop(0))
        if 0 <= k - 2 < len(tiles):
            head_stage(tiles[k - 2], second[k - 2])
            done += step // LANES
    for left in waiting:
        cut_stage(*left)
    if not last:
        carry_out[...] = a_ref[pl.ds(keep_from - first_tile, done - keep_from)]


def patch_half(half, tiles, brick_rows, keep_from, last, aug_code, shifted, plane, depth_w, head, extra=()):
    kept = head.shape[0]
    carried = extra[0].shape[0] if last else 0
    bricks = jax.ShapeDtypeStruct((16, kept + 8, LANES), F32)
    beside = jax.ShapeDtypeStruct((2 * len(tiles) - keep_from, kept, LANES), F32)
    return pl.pallas_call(
        functools.partial(patch_kernel, half, tiles, brick_rows, keep_from, last),
        out_shape=[bricks] if last else [bricks, beside],
        in_specs=[smem()] + [vmem()] * (4 + len(extra)),
        out_specs=[vmem()] * (1 if last else 2),
        scratch_shapes=[pltpu.VMEM((2 * len(tiles) + carried, kept, LANES), F32)],
        input_output_aliases={6: 0} if last else {},
        compiler_params=params(),
        cost_estimate=cost(10**9),
    )(aug_code, shifted, plane, depth_w, head, *extra)


def seed_kernel(owner_ref, out_ref):
    here = iota(out_ref.shape, 1) == lax.axis_index("patch")
    out_ref[...] = jnp.where(here, owner_ref[0], 0)


def seed_table(owner, devices):
    width = -(-devices // LANES) * LANES
    return pl.pallas_call(
        seed_kernel,
        out_shape=jax.ShapeDtypeStruct((1, width), I32),
        in_specs=[smem()],
        out_specs=vmem(),
        compiler_params=params(),
        name="seed",
    )(owner)


def partner(devices, bit):
    return [(d, d ^ bit) for d in range(devices)]


def slots_kernel(devices, masks, table_ref, anchor_ref, mine_ref, other_ref, window_ref, *outs):
    me = lax.axis_index("patch")
    brick_rows = devices // 4
    brick = iota(table_ref.shape, 1)
    row = lax.rem(brick // 4 - anchor_ref[0] + brick_rows, jnp.full_like(brick, brick_rows))
    place = row * 4 + brick % 4
    owner = jnp.where(brick < devices, table_ref[...], -1)
    _, rows, lanes = mine_ref.shape
    spare = iota((rows, lanes), 1) - jnp.where(iota((rows, lanes), 0) == rows - 8, SPARE, lanes)
    places = [jnp.sum(jnp.where(owner == (me ^ mask), place, 0)) for mask in masks]
    size = outs[0].shape[0]
    for s, at in enumerate(places):
        covered = at < 16
        slot = at if brick_rows <= 4 else jnp.where(covered, at, 0)
        value = (mine_ref[slot] + other_ref[slot]) * window_ref[slot]
        value = jnp.where(spare == at // 4, 2.0, value)
        value = jnp.where(spare == 4, 2.0 * (at % 4).astype(F32), value)
        if brick_rows > 4:
            value = jnp.where(covered, value, 0.0)
        outs[s // size][s % size] = value


def fill_slots(devices, masks, pieces, table, anchor, mine, other, window):
    shape = jax.ShapeDtypeStruct((len(masks) // pieces,) + mine.shape[1:], F32)
    return pl.pallas_call(
        functools.partial(slots_kernel, devices, masks),
        out_shape=[shape] * pieces,
        in_specs=[vmem(), smem()] + [vmem()] * 3,
        out_specs=[vmem()] * pieces,
        compiler_params=params(),
        name="slots",
    )(table, anchor, mine, other, window)


def brick_kernel(side, maps, depth_curve, mine_ref, *refs):
    *others, rows_ref, cols_ref, out_ref = refs
    depth = len(depth_curve)
    wide = 2 * side
    plane = wide * wide
    tail = side * side - LANES
    per = depth * maps
    brick = mine_ref[0]
    for other in others:
        brick = brick + other[0]
    kept = 4 * per
    main, packed = brick[:kept], brick[kept:]
    rest = jnp.concatenate([packed if k == 0 else pltpu.roll(packed, LANES - tail * k, 1) for k in range(kept // 8)], axis=0)
    fill = jnp.zeros((16 - per, LANES), F32)
    mains = [jnp.concatenate([main[per * p : per * (p + 1)], fill], axis=0) for p in range(4)]
    rests = [jnp.concatenate([rest[per * p : per * (p + 1)], fill], axis=0) for p in range(4)]
    columns = []
    for d in range(-(-plane // LANES)):
        n = iota((8, LANES), 1) + d * LANES
        y = n // wide
        x = n - y * wide
        cell = (y // 2) * side + x // 2
        quarter = 2 * (y % 2) + x % 2
        lane_of = cell % LANES
        top = min((d + 1) * LANES, plane) - 1
        tiles = []
        for r in range(2):
            cut = slice(8 * r, 8 * r + 8)
            value = None
            for p in range(4):
                one = jnp.take_along_axis(mains[p][cut], lane_of, axis=1)
                if (top // wide // 2 + 1) * side > LANES:
                    one = jnp.where(cell >= LANES, jnp.take_along_axis(rests[p][cut], lane_of, axis=1), one)
                value = one if value is None else jnp.where(quarter == p, one, value)
            tiles.append(value)
        columns.append(jnp.concatenate(tiles, axis=0))
    cells = jnp.concatenate(columns, axis=1)[:, :plane]
    for z in range(depth):
        out_ref[0, pl.ds(0, maps), pl.ds(z * plane, plane)] = cells[z * maps : (z + 1) * maps]

    def noted(k):
        lane = jnp.take_along_axis(packed, jnp.full((8, LANES), SPARE + k, I32), axis=1)[0:1]
        return jnp.concatenate([lane] * (rows_ref.shape[1] // LANES), axis=1)

    counts = [noted(i) for i in range(4)]
    added = counts[0] + counts[1] + counts[2] + counts[3]
    column = noted(4)
    down = sum(counts[i] * rows_ref[pl.ds(i, 1), :] for i in range(4))
    across = sum(jnp.where(column == j * added, cols_ref[pl.ds(j, 1), :], 0.0) for j in range(4))
    window = (down * across)[:, :plane]
    for z in range(depth):
        out_ref[0, pl.ds(maps, 1), pl.ds(z * plane, plane)] = window * depth_curve[z]


def finish(side, maps, depth, mine, others):
    plane = 4 * side * side
    width = -(-plane // LANES) * LANES
    curve = bump(8 * side)
    n = np.arange(width)
    y, x = np.minimum(n // (2 * side), 2 * side - 1), n % (2 * side)
    rows = np.stack([curve[2 * side * i + y] for i in range(4)]).astype(np.float32)
    cols = np.stack([curve[2 * side * i + x] for i in range(4)]).astype(np.float32)
    depth_curve = [float(np.float32(v)) for v in bump(depth)]
    return pl.pallas_call(
        functools.partial(brick_kernel, side, maps, depth_curve),
        out_shape=jax.ShapeDtypeStruct((1, maps + 1, depth * plane), F32),
        in_specs=[vmem()] * (len(others) + 3),
        out_specs=vmem(),
        compiler_params=params(),
        name="brick",
    )(mine, *others, rows, cols)


def wire_window(side, maps, depth):
    curve_y, curve_z = bump(8 * side), bump(depth)
    cell = np.arange(side * side)
    out = np.zeros((16, 4 * depth * maps, side * side))
    for i in range(4):
        for j in range(4):
            for p in range(4):
                y = curve_y[2 * side * i + 2 * (cell // side) + p // 2]
                x = curve_y[2 * side * j + 2 * (cell % side) + p % 2]
                for z in range(depth):
                    for m in range(maps):
                        out[4 * i + j, (p * depth + z) * maps + m] = curve_z[z] * y * x
    kept = out.shape[1]
    tail = side * side - LANES
    packed = np.zeros((16, 8, LANES))
    for k in range(kept // 8):
        packed[:, :, tail * k : tail * (k + 1)] = out[:, 8 * k : 8 * k + 8, LANES:]
    return np.concatenate([out[:, :, :LANES], packed], axis=1).astype(np.float32)


def on_device(features, w_in, w_plane, w_depth, w_head, brick_owner, patch_anchor, aug_code):
    devices = lax.axis_size("patch")
    _, _, depth, cells = features.shape
    side = math.isqrt(cells) // 4
    maps = w_head.shape[0]
    levels = [1 << k for k in range(devices.bit_length() - 1)]
    paired = levels[:1] + [bit | 1 for bit in levels[1:]]
    halved = paired[1 + DIRECT :]
    direct = [sum(bit for k, bit in enumerate(levels[1 : 1 + DIRECT]) if q >> k & 1) | min(q, 1) for q in range(1 << DIRECT)]
    masks = [0]
    for bit in reversed(halved):
        masks = masks + [bit ^ mask for mask in masks]
    masks = [first ^ mask for first in direct for mask in masks]

    table = seed_table(brick_owner, devices)
    near = []
    for mask in (1, 3, 2):
        near.append(lax.ppermute(table, "patch", partner(devices, mask)))
    table = functools.reduce(lambda a, b: a + b, near, table)
    for bit in paired[2:]:
        table = table + lax.ppermute(table, "patch", partner(devices, bit))
    plane, depth_w, head, shifted = front(aug_code, w_in, w_plane, w_depth, w_head, features[0])
    half = math.isqrt(cells)
    steps = cells // (2 * LANES)
    ready = -(-half * half // 2 // (2 * LANES)) + LEAD
    starts = [half * half * i // 4 // LANES for i in range(4)]
    span = -(-half * half // 4 // LANES)
    early = [i for i in range(4) if starts[i] + span < 2 * ready]
    late = [i for i in range(4) if i not in early]
    bricks, carry = patch_half(half, range(ready), early, starts[late[0]], False, aug_code, shifted, plane, depth_w, head)
    (bricks,) = patch_half(
        half, range(ready, steps), late, 0, True, aug_code, shifted, plane, depth_w, head, (carry, bricks)
    )
    other = lax.ppermute(bricks, "patch", partner(devices, 1))
    parts = fill_slots(devices, masks, len(direct), table, patch_anchor, bricks, other, wire_window(side, maps, depth))
    sums = [parts[0]] + [lax.ppermute(parts[q], "patch", partner(devices, direct[q])) for q in START_ORDER]
    for bit in halved:
        size = sums[0].shape[0] // 2
        keep, send = (functools.reduce(lambda a, b: a + b, [one[k : k + size] for one in sums]) for k in (0, size))
        sums = [keep, lax.ppermute(send, "patch", partner(devices, bit))]
    return finish(side, maps, depth, sums[0], sums[1:])


def solution(mesh):
    one = P(("group", "patch"))
    in_specs = (P(("group", "patch"), None, None, None), P(), P(), P(), P(), one, one, one)
    return jax.shard_map(
        on_device, mesh=mesh, in_specs=in_specs, out_specs=P(("group", "patch"), None, None), check_vma=False
    )
```

```python
import functools
import math

import numpy as np

import jax
import jax.numpy as jnp
from jax import lax
from jax.experimental import pallas as pl
from jax.experimental.pallas import tpu as pltpu
from jax.sharding import PartitionSpec as P


F32 = jnp.float32
BF16 = jnp.bfloat16
I32 = jnp.int32
PAD = 32
LANES = 128
CHUNKS = 2
START_ORDER = (1, 3, 2)
DIRECT = 2
LEAD = 2
SPARE = 96


def iota(shape, axis):
    return lax.broadcasted_iota(I32, shape, axis)


def vmem():
    return pl.BlockSpec(memory_space=pltpu.VMEM)


def smem():
    return pl.BlockSpec(memory_space=pltpu.SMEM)


def hbm():
    return pl.BlockSpec(memory_space=pltpu.HBM)


def stay(*arrays):
    return [pltpu.with_memory_space_constraint(a, pltpu.HBM) for a in arrays]


def params():
    return pltpu.CompilerParams(vmem_limit_bytes=16 * 2**20)


def cost(flops):
    return pl.CostEstimate(flops=flops, bytes_accessed=2**20, transcendentals=0)


def bump(length):
    position = (np.arange(length, dtype=np.float64) + 0.5) / length
    return 0.1 + np.sin(np.pi * position) ** 2


def front_kernel(aug_ref, w_in_hbm, w_plane_hbm, w_depth_hbm, w_head_hbm, x_hbm, plane_ref, depth_ref, head_ref, xs_ref, w_in_ref, w_plane_ref, w_depth_ref, w_head_ref, x_ref, big_ref, plane_scr, depth_scr, sems):
    size = x_hbm.shape[2] // CHUNKS
    feats = [
        pltpu.make_async_copy(x_hbm.at[:, :, pl.ds(c * size, size)], x_ref.at[:, :, pl.ds(c * size, size)], sems.at[4 + c])
        for c in range(CHUNKS)
    ]
    pairs = ((w_plane_hbm, w_plane_ref), (w_in_hbm, w_in_ref), (w_depth_hbm, w_depth_ref), (w_head_hbm, w_head_ref))
    copies = [pltpu.make_async_copy(src, dst, sems.at[k]) for k, (src, dst) in enumerate(pairs)]
    for copy in copies + feats:
        copy.start()
    for copy in copies:
        copy.wait()
    hidden, _ = w_in_ref.shape
    depth = depth_ref.shape[0] // PAD
    maps = w_head_ref.shape[0]
    aug = aug_ref[0]
    zf, yf, xf = aug & 1, (aug >> 1) & 1, (aug >> 2) & 1

    rows, cols = big_ref.shape
    spread = (iota((rows, hidden), 0) % PAD == iota((rows, hidden), 1)).astype(BF16)
    gather = (iota((w_in_ref.shape[1], cols), 1) // depth == iota((w_in_ref.shape[1], cols), 0)).astype(BF16)
    tall = jnp.dot(spread, w_in_ref[...], preferred_element_type=F32).astype(BF16)
    wide = jnp.dot(tall, gather, preferred_element_type=F32)
    same = iota((rows, cols), 1) % depth == iota((rows, cols), 0) // PAD
    big_ref[...] = jnp.where(same, wide, 0.0).astype(BF16)

    plane_scr[...] = jnp.zeros_like(plane_scr)
    taps = [w_plane_ref[t].astype(F32) for t in range(9)]
    near = (((0,), (1, 2), ()), ((), (0, 1), (2,)))
    for py in range(2):
        for px in range(2):
            for dy in range(2):
                for dx in range(3):
                    hit = [taps[3 * ty + tx] for ty in near[py][dy + py] for tx in near[px][dx]]
                    if not hit:
                        continue
                    total = functools.reduce(lambda a, b: a + b, hit)
                    high = total.astype(BF16).astype(F32)
                    col = (3 * dy + dx) * PAD
                    plane_scr[py, pl.ds(px * PAD, hidden), pl.ds(col, hidden)] = high
                    plane_scr[py, pl.ds((2 + px) * PAD, hidden), pl.ds(col, hidden)] = total - high
    plane_ref[...] = plane_scr[...].astype(BF16)

    depth_scr[...] = jnp.zeros_like(depth_scr)
    for t in range(3):
        tap = w_depth_ref[t].astype(F32)
        for z in range(depth):
            if 0 <= z + t - 1 < depth:
                depth_scr[pl.ds(z * PAD, hidden), pl.ds((z + t - 1) * PAD, hidden)] = tap
    depth_ref[...] = depth_scr[...].astype(BF16)

    rows, cols = head_ref.shape
    pick = (iota((rows, maps), 0) % maps == iota((rows, maps), 1)).astype(BF16)
    tall = jnp.dot(pick, w_head_ref[...], preferred_element_type=F32).astype(BF16)
    gather = (iota((hidden, cols), 1) % PAD == iota((hidden, cols), 0)).astype(BF16)
    wide = jnp.dot(tall, gather, preferred_element_type=F32)
    at = iota((rows, cols), 0) // maps
    came = iota((rows, cols), 1) // PAD
    flip = (2 * yf + xf) * depth + (depth - 1) * zf
    head_ref[...] = jnp.where(at == (came ^ flip), wide, 0.0).astype(BF16)

    channels, depth, cells = x_ref.shape
    zeros = jnp.zeros((depth * PAD, LANES), BF16)
    xs_ref[:, pl.ds(0, LANES)] = zeros
    xs_ref[:, pl.ds(LANES + cells, LANES)] = zeros
    for c, copy in enumerate(feats):
        part = pl.ds(c * size, size)
        copy.wait()
        x = x_ref[:, :, part].reshape(channels * depth, size)
        xs_ref[:, pl.ds(LANES + c * size, size)] = jnp.dot(big_ref[...], x, preferred_element_type=F32).astype(BF16)


def front(aug_code, w_in, w_plane, w_depth, w_head, feat):
    _, channels = w_in.shape
    maps = w_head.shape[0]
    _, depth, cells = feat.shape
    plane = (2, 4 * PAD, 6 * PAD)
    depth_w = (depth * PAD, depth * PAD)
    head = (4 * depth * maps, 4 * depth * PAD)
    padded = (depth * PAD, cells + 2 * LANES)
    return pl.pallas_call(
        front_kernel,
        out_shape=[jax.ShapeDtypeStruct(s, BF16) for s in (plane, depth_w, head, padded)],
        in_specs=[smem()] + [hbm()] * 5,
        out_specs=[vmem()] * 4,
        scratch_shapes=[
            pltpu.VMEM(w_in.shape, BF16),
            pltpu.VMEM(w_plane.shape, BF16),
            pltpu.VMEM(w_depth.shape, BF16),
            pltpu.VMEM(w_head.shape, BF16),
            pltpu.VMEM(feat.shape, BF16),
            pltpu.VMEM((depth * PAD, channels * depth), BF16),
            pltpu.VMEM(plane, F32),
            pltpu.VMEM(depth_w, F32),
            pltpu.SemaphoreType.DMA((4 + CHUNKS,)),
        ],
        compiler_params=params(),
        cost_estimate=cost(10**8),
        name="front",
    )(aug_code, *stay(w_in, w_plane, w_depth, w_head, feat))


def patch_kernel(half, tiles, brick_rows, keep_from, last, aug_ref, xs_ref, plane_ref, depth_ref, head_ref, *refs):
    if last:
        carry_in, _, out_ref, a_ref = refs
    else:
        out_ref, carry_out, a_ref = refs
    rows, _ = xs_ref.shape
    depth = rows // PAD
    step = 2 * LANES
    margin = LANES
    carried = carry_in.shape[0] if last else 0
    first_tile = tiles[0] * (step // LANES) - carried
    if last:
        a_ref[pl.ds(0, carried)] = carry_in[...]

    def window_stage(t):
        column = (iota((rows, step), 1) + t * step) % half
        block = xs_ref[:, pl.ds(t * step, step + 2 * margin)]
        near = []
        for d in (-1, 0, 1):
            near.append([])
            for e in (-1, 0, 1):
                at = margin + half * e + d
                one = lax.slice_in_dim(block, at, at + step, axis=1)
                if d:
                    one = jnp.where(column == (0 if d < 0 else half - 1), jnp.zeros_like(one), one)
                near[-1].append(one)
        return near

    def plane_stage(near, z):
        cut = slice(z * PAD, (z + 1) * PAD)
        centre = near[1][1][cut].astype(F32)
        first = []
        for py in range(2):
            around = jnp.concatenate([near[d][py + e][cut] for e in range(2) for d in range(3)], axis=0)
            mix = jnp.dot(plane_ref[py], around, preferred_element_type=F32)
            for px in range(2):
                total = mix[px * PAD : (px + 1) * PAD] + mix[(2 + px) * PAD : (3 + px) * PAD]
                first.append((centre + jnp.maximum(total, 0.0)).astype(BF16))
        return first

    def depth_stage(first, p):
        one = jnp.concatenate([first[z][p] for z in range(depth)], axis=0)
        mix = jnp.dot(depth_ref[...], one, preferred_element_type=F32)
        return (one.astype(F32) + jnp.maximum(mix, 0.0)).astype(BF16)

    def head_stage(t, second):
        logits = jnp.zeros((head_ref.shape[0], step), F32)
        for q in range(2):
            pair = jnp.concatenate(second[2 * q : 2 * q + 2], axis=0)
            logits = logits + jnp.dot(head_ref[:, 2 * q * rows : 2 * (q + 1) * rows], pair, preferred_element_type=F32)
        affinity = jax.nn.sigmoid(logits)
        for u in range(step // LANES):
            a_ref[t * (step // LANES) + u - first_tile] = affinity[:, u * LANES : (u + 1) * LANES]

    aug = aug_ref[0]
    yf, xf = (aug >> 1) & 1, (aug >> 2) & 1
    side = half // 4
    tail = side * side - LANES
    row_tiles = head_ref.shape[0] // 8
    lane = iota((8, LANES), 1)
    group = lane // tail
    span = -(-side * half // LANES)
    near_tiles = span - 2

    def source(cell, j, odd):
        y = cell // side
        x = cell - y * side
        y = jnp.where(yf == 1, side - 1 - y, y)
        x = jnp.where(xf == 1, side - 1 - x, x)
        return y * half + side * j + x + odd * (LANES // 2)

    def cut_stage(i, j):
        odd = i % 2
        owned = []
        for k in range(span):
            x = (lane + k * LANES + half - odd * (LANES // 2) % half) % half
            owned.append((x >= side * j) & (x < side * (j + 1)))
        src = source(lane, j, odd)
        main_lane, main_near = src % LANES, src < near_tiles * LANES
        rest_lane = source(LANES + lane % tail, j, odd) % LANES
        base = side * half * i // LANES - first_tile
        brick = (i ^ (3 * yf)) * 4 + (j ^ (3 * xf))
        packed = jnp.zeros((8, LANES), F32)
        for r in range(row_tiles):
            cut = pl.ds(8 * r, 8)
            merged = []
            for tiles_of in (range(near_tiles), range(near_tiles, span)):
                one = a_ref[base + tiles_of[0], cut]
                for k in tiles_of[1:]:
                    one = jnp.where(owned[k], a_ref[base + k, cut], one)
                merged.append(one)
            low = jnp.take_along_axis(merged[0], main_lane, axis=1)
            high = jnp.take_along_axis(merged[1], main_lane, axis=1)
            out_ref[brick, cut] = jnp.where(main_near, low, high)
            rest = jnp.take_along_axis(jnp.where(yf == 1, merged[0], merged[1]), rest_lane, axis=1)
            packed = jnp.where(group == r, rest, packed)
        out_ref[brick, pl.ds(8 * row_tiles, 8)] = packed

    first, second = {}, {}
    waiting = [(i, j) for i in brick_rows for j in range(4)]
    done = first_tile + carried
    for k in range(len(tiles) + 2):
        if k < len(tiles):
            near = window_stage(tiles[k])
            first[k] = []
        second[k - 1] = []
        for q in range(4):
            if k < len(tiles) and q < depth:
                first[k].append(plane_stage(near, q))
            if 0 <= k - 1 < len(tiles):
                second[k - 1].append(depth_stage(first[k - 1], q))
            if waiting and done >= side * half * waiting[0][0] // LANES + span:
                cut_stage(*waiting.pop(0))
        if 0 <= k - 2 < len(tiles):
            head_stage(tiles[k - 2], second[k - 2])
            done += step // LANES
    for left in waiting:
        cut_stage(*left)
    if not last:
        carry_out[...] = a_ref[pl.ds(keep_from - first_tile, done - keep_from)]


def patch_half(half, tiles, brick_rows, keep_from, last, aug_code, shifted, plane, depth_w, head, extra=()):
    kept = head.shape[0]
    carried = extra[0].shape[0] if last else 0
    bricks = jax.ShapeDtypeStruct((16, kept + 8, LANES), F32)
    beside = jax.ShapeDtypeStruct((2 * len(tiles) - keep_from, kept, LANES), F32)
    return pl.pallas_call(
        functools.partial(patch_kernel, half, tiles, brick_rows, keep_from, last),
        out_shape=[bricks] if last else [bricks, beside],
        in_specs=[smem()] + [vmem()] * (4 + len(extra)),
        out_specs=[vmem()] * (1 if last else 2),
        scratch_shapes=[pltpu.VMEM((2 * len(tiles) + carried, kept, LANES), F32)],
        input_output_aliases={6: 0} if last else {},
        compiler_params=params(),
        cost_estimate=cost(10**9),
    )(aug_code, shifted, plane, depth_w, head, *extra)


def seed_kernel(owner_ref, out_ref):
    here = iota(out_ref.shape, 1) == lax.axis_index("patch")
    out_ref[...] = jnp.where(here, owner_ref[0], 0)


def seed_table(owner, devices):
    width = -(-devices // LANES) * LANES
    return pl.pallas_call(
        seed_kernel,
        out_shape=jax.ShapeDtypeStruct((1, width), I32),
        in_specs=[smem()],
        out_specs=vmem(),
        compiler_params=params(),
        name="seed",
    )(owner)


def partner(devices, bit):
    return [(d, d ^ bit) for d in range(devices)]


def slots_kernel(devices, masks, table_ref, anchor_ref, mine_ref, other_ref, window_ref, *outs):
    me = lax.axis_index("patch")
    brick_rows = devices // 4
    brick = iota(table_ref.shape, 1)
    row = lax.rem(brick // 4 - anchor_ref[0] + brick_rows, jnp.full_like(brick, brick_rows))
    place = row * 4 + brick % 4
    owner = jnp.where(brick < devices, table_ref[...], -1)
    _, rows, lanes = mine_ref.shape
    spare = iota((rows, lanes), 1) - jnp.where(iota((rows, lanes), 0) == rows - 8, SPARE, lanes)
    places = [jnp.sum(jnp.where(owner == (me ^ mask), place, 0)) for mask in masks]
    size = outs[0].shape[0]
    for s, at in enumerate(places):
        covered = at < 16
        slot = at if brick_rows <= 4 else jnp.where(covered, at, 0)
        value = (mine_ref[slot] + other_ref[slot]) * window_ref[slot]
        value = jnp.where(spare == at // 4, 2.0, value)
        value = jnp.where(spare == 4, 2.0 * (at % 4).astype(F32), value)
        if brick_rows > 4:
            value = jnp.where(covered, value, 0.0)
        outs[s // size][s % size] = value


def fill_slots(devices, masks, pieces, table, anchor, mine, other, window):
    shape = jax.ShapeDtypeStruct((len(masks) // pieces,) + mine.shape[1:], F32)
    return pl.pallas_call(
        functools.partial(slots_kernel, devices, masks),
        out_shape=[shape] * pieces,
        in_specs=[vmem(), smem()] + [vmem()] * 3,
        out_specs=[vmem()] * pieces,
        compiler_params=params(),
        name="slots",
    )(table, anchor, mine, other, window)


def brick_kernel(side, maps, depth_curve, mine_ref, *refs):
    *others, rows_ref, cols_ref, out_ref = refs
    depth = len(depth_curve)
    wide = 2 * side
    plane = wide * wide
    tail = side * side - LANES
    per = depth * maps
    brick = mine_ref[0]
    for other in others:
        brick = brick + other[0]
    kept = 4 * per
    main, packed = brick[:kept], brick[kept:]
    rest = jnp.concatenate([packed if k == 0 else pltpu.roll(packed, LANES - tail * k, 1) for k in range(kept // 8)], axis=0)
    fill = jnp.zeros((16 - per, LANES), F32)
    mains = [jnp.concatenate([main[per * p : per * (p + 1)], fill], axis=0) for p in range(4)]
    rests = [jnp.concatenate([rest[per * p : per * (p + 1)], fill], axis=0) for p in range(4)]
    columns = []
    for d in range(-(-plane // LANES)):
        n = iota((8, LANES), 1) + d * LANES
        y = n // wide
        x = n - y * wide
        cell = (y // 2) * side + x // 2
        quarter = 2 * (y % 2) + x % 2
        lane_of = cell % LANES
        top = min((d + 1) * LANES, plane) - 1
        tiles = []
        for r in range(2):
            cut = slice(8 * r, 8 * r + 8)
            value = None
            for p in range(4):
                one = jnp.take_along_axis(mains[p][cut], lane_of, axis=1)
                if (top // wide // 2 + 1) * side > LANES:
                    one = jnp.where(cell >= LANES, jnp.take_along_axis(rests[p][cut], lane_of, axis=1), one)
                value = one if value is None else jnp.where(quarter == p, one, value)
            tiles.append(value)
        columns.append(jnp.concatenate(tiles, axis=0))
    cells = jnp.concatenate(columns, axis=1)[:, :plane]
    for z in range(depth):
        out_ref[0, pl.ds(0, maps), pl.ds(z * plane, plane)] = cells[z * maps : (z + 1) * maps]

    def noted(k):
        lane = jnp.take_along_axis(packed, jnp.full((8, LANES), SPARE + k, I32), axis=1)[0:1]
        return jnp.concatenate([lane] * (rows_ref.shape[1] // LANES), axis=1)

    counts = [noted(i) for i in range(4)]
    added = counts[0] + counts[1] + counts[2] + counts[3]
    column = noted(4)
    down = sum(counts[i] * rows_ref[pl.ds(i, 1), :] for i in range(4))
    across = sum(jnp.where(column == j * added, cols_ref[pl.ds(j, 1), :], 0.0) for j in range(4))
    window = (down * across)[:, :plane]
    for z in range(depth):
        out_ref[0, pl.ds(maps, 1), pl.ds(z * plane, plane)] = window * depth_curve[z]


def finish(side, maps, depth, mine, others):
    plane = 4 * side * side
    width = -(-plane // LANES) * LANES
    curve = bump(8 * side)
    n = np.arange(width)
    y, x = np.minimum(n // (2 * side), 2 * side - 1), n % (2 * side)
    rows = np.stack([curve[2 * side * i + y] for i in range(4)]).astype(np.float32)
    cols = np.stack([curve[2 * side * i + x] for i in range(4)]).astype(np.float32)
    depth_curve = [float(np.float32(v)) for v in bump(depth)]
    return pl.pallas_call(
        functools.partial(brick_kernel, side, maps, depth_curve),
        out_shape=jax.ShapeDtypeStruct((1, maps + 1, depth * plane), F32),
        in_specs=[vmem()] * (len(others) + 3),
        out_specs=vmem(),
        compiler_params=params(),
        name="brick",
    )(mine, *others, rows, cols)


def wire_window(side, maps, depth):
    curve_y, curve_z = bump(8 * side), bump(depth)
    cell = np.arange(side * side)
    out = np.zeros((16, 4 * depth * maps, side * side))
    for i in range(4):
        for j in range(4):
            for p in range(4):
                y = curve_y[2 * side * i + 2 * (cell // side) + p // 2]
                x = curve_y[2 * side * j + 2 * (cell % side) + p % 2]
                for z in range(depth):
                    for m in range(maps):
                        out[4 * i + j, (p * depth + z) * maps + m] = curve_z[z] * y * x
    kept = out.shape[1]
    tail = side * side - LANES
    packed = np.zeros((16, 8, LANES))
    for k in range(kept // 8):
        packed[:, :, tail * k : tail * (k + 1)] = out[:, 8 * k : 8 * k + 8, LANES:]
    return np.concatenate([out[:, :, :LANES], packed], axis=1).astype(np.float32)


def on_device(features, w_in, w_plane, w_depth, w_head, brick_owner, patch_anchor, aug_code):
    devices = lax.axis_size("patch")
    _, _, depth, cells = features.shape
    side = math.isqrt(cells) // 4
    maps = w_head.shape[0]
    levels = [1 << k for k in range(devices.bit_length() - 1)]
    paired = levels[:1] + [bit | 1 for bit in levels[1:]]
    halved = paired[1 + DIRECT :]
    direct = [sum(bit for k, bit in enumerate(levels[1 : 1 + DIRECT]) if q >> k & 1) | min(q, 1) for q in range(1 << DIRECT)]
    masks = [0]
    for bit in reversed(halved):
        masks = masks + [bit ^ mask for mask in masks]
    masks = [first ^ mask for first in direct for mask in masks]

    def table_round(k, table):
        return table + lax.ppermute(table, "patch", partner(devices, rounds[k]))

    rounds = paired
    table = seed_table(brick_owner, devices)
    for k in range(len(rounds)):
        table = table_round(k, table)
    plane, depth_w, head, shifted = front(aug_code, w_in, w_plane, w_depth, w_head, features[0])
    half = math.isqrt(cells)
    steps = cells // (2 * LANES)
    ready = -(-half * half // 2 // (2 * LANES)) + LEAD
    starts = [half * half * i // 4 // LANES for i in range(4)]
    span = -(-half * half // 4 // LANES)
    early = [i for i in range(4) if starts[i] + span < 2 * ready]
    late = [i for i in range(4) if i not in early]
    bricks, carry = patch_half(half, range(ready), early, starts[late[0]], False, aug_code, shifted, plane, depth_w, head)
    (bricks,) = patch_half(
        half, range(ready, steps), late, 0, True, aug_code, shifted, plane, depth_w, head, (carry, bricks)
    )
    other = lax.ppermute(bricks, "patch", partner(devices, 1))
    parts = fill_slots(devices, masks, len(direct), table, patch_anchor, bricks, other, wire_window(side, maps, depth))
    sums = [parts[0]] + [lax.ppermute(parts[q], "patch", partner(devices, direct[q])) for q in START_ORDER]
    for bit in halved:
        size = sums[0].shape[0] // 2
        keep, send = (functools.reduce(lambda a, b: a + b, [one[k : k + size] for one in sums]) for k in (0, size))
        sums = [keep, lax.ppermute(send, "patch", partner(devices, bit))]
    return finish(side, maps, depth, sums[0], sums[1:])


def solution(mesh):
    one = P(("group", "patch"))
    in_specs = (P(("group", "patch"), None, None, None), P(), P(), P(), P(), one, one, one)
    return jax.shard_map(
        on_device, mesh=mesh, in_specs=in_specs, out_specs=P(("group", "patch"), None, None), check_vma=False
    )
```
